128 devices in a mesh: dp: 16 (over z, y), tp: 8 (over x, core).
Axes of the slice: x: 4, y: 4, z: 4, core: 2. Of those that a mesh axis runs over, the one named last changes fastest.
Arguments:
- hidden: bfloat16 [1024, 640], P('dp')
- w_final: float32 [640], replicated
- emb_table: bfloat16 [262144, 640], P('tp')
- teacher: bfloat16 [1024, 262144], P('dp', 'tp')
- tok_mask: float32 [1024], P('dp')
Outputs:
- output 1: float32 [], replicated
- output 2: bfloat16 [1024, 640], P('dp')
- output 3: float32 [640], replicated
- output 4: float32 [262144, 640], P('tp')
All inputs are finite; a program needn't handle non-finite values.
Results may differ from the reference program's by a relative error of at most 0.001.
Values sent between devices are 32-bit elements.
A program may use at most 1 GiB of HBM per device.

```python
import math
import jax
import jax.numpy as jnp
from jax import lax

MODEL_DIM = 640
VOCAB_SIZE = 262144
NUM_TOKENS = 1024
SEQ_LEN = 16
ROW_BLOCK = math.gcd(NUM_TOKENS, 64)
SOFT_CAP = 30.0
NORM_EPS = 1e-6


def setup_inputs(seed: int = 0) -> dict:
    root_key = jax.random.key(seed)
    k_hid, k_gain, k_dir, k_tab, k_off, k_tea, k_seq, k_tok = jax.random.split(root_key, 8)
    fan_scale = 1.0 / math.sqrt(MODEL_DIM)
    hidden = 3.0 * jax.random.normal(k_hid, (NUM_TOKENS, MODEL_DIM), jnp.float32)
    w_final = 0.3 * jax.random.normal(k_gain, (MODEL_DIM,), jnp.float32)
    direction = 15.0 * fan_scale * jax.random.normal(k_dir, (MODEL_DIM,), jnp.float32)
    emb_table = direction[None, :] + 2.0 * fan_scale * jax.random.normal(k_tab, (VOCAB_SIZE, MODEL_DIM), jnp.float32)
    offset = 15.0 * jax.random.normal(k_off, (NUM_TOKENS, 1), jnp.float32)
    teacher = offset + 3.0 * jax.random.normal(k_tea, (NUM_TOKENS, VOCAB_SIZE), jnp.float32)
    seq_keep = (jax.random.randint(k_seq, (NUM_TOKENS // SEQ_LEN,), 0, 4) > 0).at[0].set(True)
    tok_keep = (jax.random.randint(k_tok, (NUM_TOKENS,), 0, 8) > 0).at[0].set(True)
    tok_mask = jnp.logical_and(jnp.repeat(seq_keep, SEQ_LEN), tok_keep).astype(jnp.float32)
    return {'hidden': hidden.astype(jnp.bfloat16), 'w_final': w_final, 'emb_table': emb_table.astype(jnp.bfloat16), 'teacher': teacher.astype(jnp.bfloat16), 'tok_mask': tok_mask}


def final_norm(hid_rows, w_final):
    hid_f = hid_rows.astype(jnp.float32)
    inv_rms = lax.rsqrt(jnp.mean(hid_f * hid_f, axis=-1, keepdims=True) + NORM_EPS)
    normed = hid_f * inv_rms
    return inv_rms, normed, (normed * (1.0 + w_final)).astype(jnp.bfloat16)


def reference(hidden, w_final, emb_table, teacher, tok_mask):
    mask_sum = jnp.sum(tok_mask)
    num_blocks = NUM_TOKENS // ROW_BLOCK
    hid_blocks = hidden.reshape(num_blocks, ROW_BLOCK, MODEL_DIM)
    tea_blocks = teacher.reshape(num_blocks, ROW_BLOCK, VOCAB_SIZE)
    mask_blocks = tok_mask.reshape(num_blocks, ROW_BLOCK)

    def block_step(scan_carry, block_in):
        loss_acc, gain_acc, table_acc = scan_carry
        hid_rows, tea_rows, mask_rows = block_in
        inv_rms, normed, x_rows = final_norm(hid_rows, w_final)
        logits = jnp.dot(x_rows, emb_table.T, preferred_element_type=jnp.float32)
        stu_cap = SOFT_CAP * jnp.tanh(logits / SOFT_CAP)
        tea_cap = SOFT_CAP * jnp.tanh(tea_rows.astype(jnp.float32) / SOFT_CAP)
        stu_logp = stu_cap - jax.nn.logsumexp(stu_cap, axis=-1, keepdims=True)
        tea_logp = tea_cap - jax.nn.logsumexp(tea_cap, axis=-1, keepdims=True)
        tea_prob = jnp.exp(tea_logp)
        kl_rows = jnp.sum(tea_prob * (tea_logp - stu_logp), axis=-1)
        weight = (mask_rows / mask_sum)[:, None]
        cap_ratio = stu_cap / SOFT_CAP
        grad_z = ((jnp.exp(stu_logp) - tea_prob) * weight * (1.0 - cap_ratio * cap_ratio)).astype(jnp.bfloat16)
        grad_x = jnp.dot(grad_z, emb_table, preferred_element_type=jnp.float32)
        grad_n = grad_x * (1.0 + w_final)
        grad_h = inv_rms * (grad_n - normed * jnp.mean(grad_n * normed, axis=-1, keepdims=True))
        loss_acc = loss_acc + jnp.sum(mask_rows * kl_rows)
        gain_acc = gain_acc + jnp.sum(grad_x * normed, axis=0)
        table_acc = table_acc + jnp.dot(grad_z.T, x_rows, preferred_element_type=jnp.float32)
        return (loss_acc, gain_acc, table_acc), grad_h.astype(jnp.bfloat16)

    init_carry = (jnp.zeros((), jnp.float32), jnp.zeros((MODEL_DIM,), jnp.float32), jnp.zeros((VOCAB_SIZE, MODEL_DIM), jnp.float32))
    (loss_acc, gain_acc, table_acc), grad_blocks = lax.scan(block_step, init_carry, (hid_blocks, tea_blocks, mask_blocks))
    return loss_acc / mask_sum, grad_blocks.reshape(NUM_TOKENS, MODEL_DIM), gain_acc, table_acc
```

```python
import jax
import jax.numpy as jnp
from jax import lax
from jax.sharding import PartitionSpec as P

SOFT_CAP = 30.0
NORM_EPS = 1e-6
CHUNKS = (4096, 8192, 12288, 6144, 2048)


def final_norm(hid_rows, w_final):
    hid_f = hid_rows.astype(jnp.float32)
    inv_rms = lax.rsqrt(jnp.mean(hid_f * hid_f, axis=-1, keepdims=True) + NORM_EPS)
    normed = hid_f * inv_rms
    return inv_rms, normed, (normed * (1.0 + w_final)).astype(jnp.bfloat16)


def solution(mesh):
    n_dp = mesh.shape['dp']

    def local_step(hid_rows, w_final, tab_rows, tea_rows, mask_rows):
        tokens, dim = hid_rows.shape
        vocab = tab_rows.shape[0]
        me = lax.axis_index('dp')
        inv_rms, normed, x_rows = final_norm(hid_rows, w_final)
        x_all = (lax.all_gather(normed, 'dp', axis=0, tiled=True) * (1.0 + w_final)).astype(jnp.bfloat16)
        logits = lax.dot_general(x_rows, tab_rows, (((1,), (1,)), ((), ())), preferred_element_type=jnp.float32)
        stu_cap = SOFT_CAP * jnp.tanh(logits / SOFT_CAP)
        tea_cap = SOFT_CAP * jnp.tanh(tea_rows.astype(jnp.float32) / SOFT_CAP)
        stu_exp = jnp.exp(stu_cap - SOFT_CAP)
        tea_exp = jnp.exp(tea_cap - SOFT_CAP)
        own = jnp.stack([jnp.sum(stu_exp, axis=-1), jnp.sum(tea_exp, axis=-1), jnp.sum(tea_exp * (tea_cap - stu_cap), axis=-1), jnp.where(lax.axis_index('tp') == 0, mask_rows, 0.0)], axis=0)
        slots = jnp.where(lax.broadcasted_iota(jnp.int32, (n_dp, 4, tokens), 0) == me, own[None], 0.0)
        stats = lax.psum(slots, ('dp', 'tp'))
        all_kl = stats[:, 2] / stats[:, 1] + jnp.log(stats[:, 0]) - jnp.log(stats[:, 1])
        mask_sum = jnp.sum(stats[:, 3])
        loss_val = jnp.sum(stats[:, 3] * all_kl) / mask_sum
        mine = lax.dynamic_index_in_dim(stats, me, 0, keepdims=False)
        weight = (mask_rows / mask_sum)[:, None]
        cap_ratio = stu_cap / SOFT_CAP
        raw_z = (stu_exp / mine[0][:, None] - tea_exp / mine[1][:, None]) * (1.0 - cap_ratio * cap_ratio)
        grad_z = (raw_z * weight).astype(jnp.bfloat16)
        weights = (stats[:, 3] / mask_sum)[:, :, None]
        table = jnp.zeros((vocab, dim), jnp.float32)
        x_blocks = x_all.reshape(n_dp, tokens, dim)
        sends = []
        start = 0
        for rows in CHUNKS:
            sends.append(raw_z[:, start:start + rows].reshape(tokens, n_dp, rows // n_dp).transpose(1, 0, 2))
            start += rows
        got_all = lax.all_to_all(jnp.concatenate(sends, axis=2), 'dp', 0, 0)
        start = 0
        for rows in CHUNKS:
            part = rows // n_dp
            got = got_all[:, :, start // n_dp:start // n_dp + part]
            piece = lax.dot_general((got * weights).astype(jnp.bfloat16), x_blocks, (((0, 1), (0, 1)), ((), ())), preferred_element_type=jnp.float32)
            full = lax.all_gather(piece, 'dp', axis=0, tiled=True)
            table = lax.dynamic_update_slice(table, full, (start, 0))
            start += rows
        part_x = jnp.dot(grad_z, tab_rows, preferred_element_type=jnp.float32)
        grad_x = lax.psum(part_x, 'tp')
        grad_gain = lax.psum(jnp.sum(part_x * normed, axis=0), ('dp', 'tp'))
        grad_n = grad_x * (1.0 + w_final)
        grad_h = inv_rms * (grad_n - normed * jnp.mean(grad_n * normed, axis=-1, keepdims=True))
        return loss_val, grad_h.astype(jnp.bfloat16), grad_gain, table

    return jax.shard_map(local_step, mesh=mesh, in_specs=(P('dp', None), P(None), P('tp', None), P('dp', 'tp'), P('dp')), out_specs=(P(), P('dp', None), P(None), P('tp', None)), check_vma=False)
```

```python
import jax
import jax.numpy as jnp
from jax import lax
from jax.experimental import pallas as pl
from jax.experimental.pallas import tpu as pltpu
from jax.sharding import PartitionSpec as P

SOFT_CAP = 30.0
NORM_EPS = 1e-6
SPLIT = 2


def pos_of(cyc, dp):
    z, y = dp // 4, dp % 4
    if cyc == 0:
        return z * 4 + (y + z) % 4
    return y * 4 + (z + y) % 4

def dp_of(cyc, pos):
    a = pos // 4
    b = (pos % 4 - a + 4) % 4
    if cyc == 0:
        return a * 4 + b
    return b * 4 + a

def place(table, pieces, group, step, rows, vocab):
    part, dim = pieces[0].shape

    def kern(*refs):
        srcs, dst, sem = refs[:4], refs[-2], refs[-1]
        me = lax.axis_index('dp')
        copies = []
        for ring in range(4):
            sgn = 1 if ring % 2 == 0 else -1
            owner = dp_of(ring // 2, (pos_of(ring // 2, me) - sgn * step + 32) % 16)
            start = pl.multiple_of(owner * rows + ring * (rows // 4) + group * part, 8)
            copies.append(pltpu.make_async_copy(srcs[ring], dst.at[pl.ds(start, part)], sem.at[ring]))
        for cp in copies:
            cp.start()
        for cp in copies:
            cp.wait()

    vm = pl.BlockSpec(memory_space=pltpu.VMEM)
    hb = pl.BlockSpec(memory_space=pl.ANY)
    args = list(pieces) if table is None else [*pieces, table]
    return pl.pallas_call(kern, out_shape=jax.ShapeDtypeStruct((vocab, dim), jnp.float32), in_specs=[vm] * 4 + [hb] * (len(args) - 4), out_specs=hb,
        scratch_shapes=[pltpu.SemaphoreType.DMA((4,))], input_output_aliases={} if table is None else {4: 0}, name='place',
        compiler_params=pltpu.CompilerParams(vmem_limit_bytes=2 ** 22),
        cost_estimate=pl.CostEstimate(flops=10 ** 7, bytes_accessed=8 * part * dim * 4, transcendentals=0))(*args)


def gather_rings(shard, vocab):
    rows, dim = shard.shape
    part = rows // 4 // SPLIT
    held = []
    for c in range(SPLIT):
        held.append([])
        for ring in range(4):
            off = ring * (rows // 4) + c * part
            held[c].append(shard[off:off + part])
    table = None
    for s in range(1, 16):
        for c in range(SPLIT):
            new = []
            for ring in range(4):
                cyc, sgn = ring // 2, 1 if ring % 2 == 0 else -1
                perm = [(d, dp_of(cyc, (pos_of(cyc, d) + sgn) % 16)) for d in range(16)]
                new.append(lax.ppermute(held[c][ring], 'dp', perm))
            table = place(table, held[c], c, s - 1, rows, vocab)
            table, *held[c] = lax.optimization_barrier((table, *new))
    for c in range(SPLIT):
        table = place(table, held[c], c, 15, rows, vocab)
    return table


def final_norm(hid_rows, w_final):
    hid_f = hid_rows.astype(jnp.float32)
    inv_rms = lax.rsqrt(jnp.mean(hid_f * hid_f, axis=-1, keepdims=True) + NORM_EPS)
    normed = hid_f * inv_rms
    return inv_rms, normed, (normed * (1.0 + w_final)).astype(jnp.bfloat16)


def solution(mesh):
    n_dp = mesh.shape['dp']

    def local_step(hid_rows, w_final, tab_rows, tea_rows, mask_rows):
        tokens, dim = hid_rows.shape
        vocab = tab_rows.shape[0]
        me = lax.axis_index('dp')
        inv_rms, normed, x_rows = final_norm(hid_rows, w_final)
        x_all = (lax.all_gather(normed, 'dp', axis=0, tiled=True) * (1.0 + w_final)).astype(jnp.bfloat16)
        logits = lax.dot_general(x_rows, tab_rows, (((1,), (1,)), ((), ())), preferred_element_type=jnp.float32)
        stu_cap = SOFT_CAP * jnp.tanh(logits / SOFT_CAP)
        tea_cap = SOFT_CAP * jnp.tanh(tea_rows.astype(jnp.float32) / SOFT_CAP)
        stu_exp = jnp.exp(stu_cap - SOFT_CAP)
        tea_exp = jnp.exp(tea_cap - SOFT_CAP)
        own = jnp.stack([jnp.sum(stu_exp, axis=-1), jnp.sum(tea_exp, axis=-1), jnp.sum(tea_exp * (tea_cap - stu_cap), axis=-1), jnp.where(lax.axis_index('tp') == 0, mask_rows, 0.0)], axis=0)
        slots = jnp.where(lax.broadcasted_iota(jnp.int32, (n_dp, 4, tokens), 0) == me, own[None], 0.0)
        stats = lax.psum(slots, ('dp', 'tp'))
        all_kl = stats[:, 2] / stats[:, 1] + jnp.log(stats[:, 0]) - jnp.log(stats[:, 1])
        mask_sum = jnp.sum(stats[:, 3])
        loss_val = jnp.sum(stats[:, 3] * all_kl) / mask_sum
        mine = lax.dynamic_index_in_dim(stats, me, 0, keepdims=False)
        weight = (mask_rows / mask_sum)[:, None]
        cap_ratio = stu_cap / SOFT_CAP
        raw_z = (stu_exp / mine[0][:, None] - tea_exp / mine[1][:, None]) * (1.0 - cap_ratio * cap_ratio)
        grad_z = (raw_z * weight).astype(jnp.bfloat16)
        weights = (stats[:, 3] / mask_sum)[:, :, None]
        part = vocab // n_dp
        sends = raw_z.reshape(tokens, n_dp, part).transpose(1, 0, 2)
        got = lax.all_to_all(sends, 'dp', 0, 0)
        x_blocks = x_all.reshape(n_dp, tokens, dim)
        piece = lax.dot_general((got * weights).astype(jnp.bfloat16), x_blocks, (((0, 1), (0, 1)), ((), ())), preferred_element_type=jnp.float32)
        table = gather_rings(piece, vocab)
        part_x = jnp.dot(grad_z, tab_rows, preferred_element_type=jnp.float32)
        grad_x = lax.psum(part_x, 'tp')
        grad_gain = lax.psum(jnp.sum(part_x * normed, axis=0), ('dp', 'tp'))
        grad_n = grad_x * (1.0 + w_final)
        grad_h = inv_rms * (grad_n - normed * jnp.mean(grad_n * normed, axis=-1, keepdims=True))
        return loss_val, grad_h.astype(jnp.bfloat16), grad_gain, table

    return jax.shard_map(local_step, mesh=mesh, in_specs=(P('dp', None), P(None), P('tp', None), P('dp', 'tp'), P('dp')), out_specs=(P(), P('dp', None), P(None), P('tp', None)), check_vma=False)
```

```python
import jax
import jax.numpy as jnp
from jax import lax
from jax.experimental import pallas as pl
from jax.experimental.pallas import tpu as pltpu
from jax.sharding import PartitionSpec as P


SOFT_CAP = 30.0
NORM_EPS = 1e-6
SPLIT = 2


def pos_of(cyc, dp):
    z, y = dp // 4, dp % 4
    if cyc == 0:
        return z * 4 + (y + z) % 4
    return y * 4 + (z + y) % 4


def dp_of(cyc, pos):
    a = pos // 4
    b = (pos % 4 - a + 4) % 4
    if cyc == 0:
        return a * 4 + b
    return b * 4 + a


def place(table, pieces, group, step, rows, vocab):
    part, dim = pieces[0].shape

    def kern(*refs):
        srcs, dst, sem = refs[:4], refs[-2], refs[-1]
        me = lax.axis_index('dp')
        copies = []
        for ring in range(4):
            sgn = 1 if ring % 2 == 0 else -1
            owner = dp_of(ring // 2, (pos_of(ring // 2, me) - sgn * step + 32) % 16)
            start = pl.multiple_of(owner * rows + (group * 4 + ring) * part, 8)
            copies.append(pltpu.make_async_copy(srcs[ring], dst.at[pl.ds(start, part)], sem.at[ring]))
        for cp in copies:
            cp.start()
        for cp in copies:
            cp.wait()

    vm = pl.BlockSpec(memory_space=pltpu.VMEM)
    hb = pl.BlockSpec(memory_space=pltpu.HBM)
    args = list(pieces) if table is None else [*pieces, table]
    return pl.pallas_call(kern, out_shape=jax.ShapeDtypeStruct((vocab, dim), jnp.float32), in_specs=[vm] * 4 + [hb] * (len(args) - 4), out_specs=hb,
        scratch_shapes=[pltpu.SemaphoreType.DMA((4,))], input_output_aliases={} if table is None else {4: 0}, name='place',
        compiler_params=pltpu.CompilerParams(vmem_limit_bytes=2 ** 22),
        cost_estimate=pl.CostEstimate(flops=10 ** 7, bytes_accessed=8 * part * dim * 4, transcendentals=0))(*args)


def gather_rings(groups, vocab):
    half, _ = groups[0].shape
    part = half // 4
    rows = half * SPLIT
    held = [[g[ring * part:(ring + 1) * part] for ring in range(4)] for g in groups]
    table = None
    for s in range(1, 16):
        for c in range(SPLIT):
            new = []
            for ring in range(4):
                cyc, sgn = ring // 2, 1 if ring % 2 == 0 else -1
                perm = [(d, dp_of(cyc, (pos_of(cyc, d) + sgn) % 16)) for d in range(16)]
                new.append(lax.ppermute(held[c][ring], 'dp', perm))
            table = place(table, held[c], c, s - 1, rows, vocab)
            table, *held[c] = lax.optimization_barrier((table, *new))
    for c in range(SPLIT):
        table = place(table, held[c], c, 15, rows, vocab)
    return table


OFFSETS = tuple((dz, dy) for dz in range(4) for dy in range(4))


def shift(dp, dz, dy):
    return (dp // 4 + dz + 4) % 4 * 4 + (dp % 4 + dy + 4) % 4


def teach(teacher, part, offsets):
    tokens = teacher.shape[0]
    n = len(offsets)

    def kern(tea_ref, *refs):
        outs, buf, sem = refs[:n], refs[-2], refs[-1]
        me = lax.axis_index('dp')
        copies = []
        for k, (dz, dy) in enumerate(offsets):
            start = pl.multiple_of(shift(me, dz, dy) * part, 128)
            copies.append(pltpu.make_async_copy(tea_ref.at[:, pl.ds(start, part)], buf.at[k], sem.at[k]))
        for cp in copies:
            cp.start()
        for k in range(n):
            copies[k].wait()
            for row in range(0, tokens, 8):
                raw = buf[k, row:row + 8].astype(jnp.float32)
                outs[k][row:row + 8] = jnp.exp(SOFT_CAP * jnp.tanh(raw / SOFT_CAP) - SOFT_CAP)

    vm = pl.BlockSpec(memory_space=pltpu.VMEM)
    return pl.pallas_call(kern, out_shape=[jax.ShapeDtypeStruct((tokens, part), jnp.float32)] * n, in_specs=[pl.BlockSpec(memory_space=pltpu.HBM)], out_specs=[vm] * n,
        scratch_shapes=[pltpu.VMEM((n, tokens, part), teacher.dtype), pltpu.SemaphoreType.DMA((n,))], name='teach',
        compiler_params=pltpu.CompilerParams(vmem_limit_bytes=2 ** 22 * n // 4),
        cost_estimate=pl.CostEstimate(flops=2 * 10 ** 7, bytes_accessed=4 * n * tokens * part, transcendentals=0))(teacher)


def finish(teas, x_all, tab_part, coef, group):
    tokens, part = teas[0].shape
    dim = x_all.shape[1]
    n = len(OFFSETS)
    span = part // SPLIT
    tile = span // 4

    def kern(*refs):
        tea, x_ref, tab_ref, coef_ref, out_ref, x_buf, c_buf, g_buf = refs[:n], *refs[n:]
        me = lax.axis_index('dp')
        for k, (dz, dy) in enumerate(OFFSETS):
            src = pl.multiple_of(shift(me, -dz, -dy) * tokens, tokens)
            x_buf[k * tokens:(k + 1) * tokens] = x_ref[pl.ds(src, tokens)]
            c_buf[k * tokens:(k + 1) * tokens] = coef_ref[pl.ds(src, tokens)]
        for t in range(4):
            base = group * span + t * tile
            rows = tab_ref[base:base + tile]
            for k in range(n):
                here = pl.ds(k * tokens, tokens)
                z = lax.dot_general(x_buf[here], rows, (((1,), (1,)), ((), ())), preferred_element_type=jnp.float32)
                ratio = jnp.tanh(z / SOFT_CAP)
                stu = jnp.exp(SOFT_CAP * ratio - SOFT_CAP)
                inv_s, inv_t, wgt = c_buf[here, 0:1], c_buf[here, 1:2], c_buf[here, 2:3]
                diff = (stu * inv_s - tea[k][:, base:base + tile] * inv_t) * wgt
                g_buf[here] = (diff * (1.0 - ratio * ratio)).astype(jnp.bfloat16)
            out_ref[t * tile:(t + 1) * tile] = lax.dot_general(g_buf[...], x_buf[...], (((0,), (0,)), ((), ())), preferred_element_type=jnp.float32)

    vm = pl.BlockSpec(memory_space=pltpu.VMEM)
    return pl.pallas_call(kern, out_shape=jax.ShapeDtypeStruct((span, dim), jnp.float32), in_specs=[vm] * (n + 3), out_specs=vm,
        scratch_shapes=[pltpu.VMEM(x_all.shape, x_all.dtype), pltpu.VMEM(coef.shape, coef.dtype), pltpu.VMEM((n * tokens, tile), jnp.bfloat16)], name='finish',
        compiler_params=pltpu.CompilerParams(vmem_limit_bytes=26 * 2 ** 20),
        cost_estimate=pl.CostEstimate(flops=10 ** 9, bytes_accessed=10 ** 7, transcendentals=0))(*teas, x_all, tab_part, coef)


def spread(value, axis, n):
    return lax.all_to_all(jnp.broadcast_to(value[None], (n, *value.shape)), axis, 0, 0)


def solution(mesh):
    n_dp, n_tp = mesh.shape['dp'], mesh.shape['tp']

    def local_step(hid_rows, w_final, tab_rows, tea_rows, mask_rows):
        tokens, dim = hid_rows.shape
        vocab = tab_rows.shape[0]
        part = vocab // n_dp
        few = tokens // n_tp
        me, col = lax.axis_index('dp'), lax.axis_index('tp')
        gain = 1.0 + w_final
        hid_f = hid_rows.astype(jnp.float32)
        inv_rms = lax.rsqrt(jnp.mean(hid_f * hid_f, axis=-1, keepdims=True) + NORM_EPS)
        normed = hid_f * inv_rms
        x_rows = (normed * gain).astype(jnp.bfloat16)

        my_normed = lax.dynamic_slice_in_dim(normed, col * few, few, 0)
        mask_line = jnp.pad(mask_rows[None], ((0, 7), (0, dim - tokens)))
        first = spread(jnp.concatenate([my_normed, mask_line]), 'dp', n_dp)

        teas = []
        for k in range(0, 16, 4):
            offsets = OFFSETS[k:k + 4]
            blocks = teach(tea_rows, part, offsets)
            if k:
                first, *blocks = lax.optimization_barrier((first, *blocks))
            for (dz, dy), block in zip(offsets, blocks):
                teas.append(block if dz == dy == 0 else lax.ppermute(block, 'dp', [(d, shift(d, dz, dy)) for d in range(n_dp)]))

        masks = first[:, few, :tokens]
        mask_sum = jnp.sum(masks)
        x_tp = spread(first[:, :few], 'tp', n_tp)
        x_all = (x_tp.transpose(1, 0, 2, 3).reshape(n_dp * tokens, dim) * gain).astype(jnp.bfloat16)

        logits = lax.dot_general(x_rows, tab_rows, (((1,), (1,)), ((), ())), preferred_element_type=jnp.float32)
        ratio = jnp.tanh(logits / SOFT_CAP)
        stu_exp = jnp.exp(SOFT_CAP * ratio - SOFT_CAP)
        tea_cap = SOFT_CAP * jnp.tanh(tea_rows.astype(jnp.float32) / SOFT_CAP)
        tea_exp = jnp.exp(tea_cap - SOFT_CAP)
        sums = (jnp.sum(stu_exp, axis=-1), jnp.sum(tea_exp, axis=-1), jnp.sum(tea_exp * (tea_cap - SOFT_CAP * ratio), axis=-1))
        part_stats = jnp.pad(jnp.stack(sums, axis=0), ((0, 5), (0, 128 - tokens)))
        part_stats, x_all = lax.optimization_barrier((part_stats, x_all))
        stats = jnp.sum(spread(part_stats, 'tp', n_tp), axis=0)

        weight = (mask_rows / mask_sum)[:, None]
        grad_z = ((stu_exp / stats[0, :tokens, None] - tea_exp / stats[1, :tokens, None]) * weight * (1.0 - ratio * ratio)).astype(jnp.bfloat16)
        part_x = jnp.dot(grad_z, tab_rows, preferred_element_type=jnp.float32)
        my_x = jnp.sum(lax.all_to_all(part_x.reshape(n_tp, few, dim), 'tp', 0, 0), axis=0)
        grad_n = my_x * gain
        my_inv = lax.dynamic_slice_in_dim(inv_rms, col * few, few, 0)
        my_h = my_inv * (grad_n - my_normed * jnp.mean(grad_n * my_normed, axis=-1, keepdims=True))
        gain_line = jnp.pad(jnp.sum(my_x * my_normed, axis=0)[None], ((0, 7), (0, 0)))
        second = spread(jnp.concatenate([my_h, gain_line]), 'tp', n_tp)
        grad_h = second[:, :few].reshape(tokens, dim)
        gain_tp = jnp.sum(second[:, few:], axis=0)

        third = spread(jnp.concatenate([gain_tp, jnp.pad(stats, ((0, 0), (0, dim - 128)))]), 'dp', n_dp)
        grad_gain = jnp.sum(third[:, 0], axis=0)
        all_stats = third[:, 8:11, :tokens]
        all_kl = all_stats[:, 2] / all_stats[:, 1] + jnp.log(all_stats[:, 0]) - jnp.log(all_stats[:, 1])
        loss_val = jnp.sum(masks * all_kl) / mask_sum

        tab_part = lax.dynamic_slice_in_dim(tab_rows, me * part, part, 0)
        coef = jnp.stack([(1.0 / all_stats[:, 0]).reshape(-1), (1.0 / all_stats[:, 1]).reshape(-1), (masks / mask_sum).reshape(-1)], axis=-1)
        coef = jnp.pad(coef, ((0, 0), (0, 125)))
        groups = [finish(teas, x_all, tab_part, coef, c) for c in range(SPLIT)]

        table = gather_rings(groups, vocab)
        return loss_val, grad_h.astype(jnp.bfloat16), grad_gain, table

    return jax.shard_map(local_step, mesh=mesh, in_specs=(P('dp', None), P(None), P('tp', None), P('dp', 'tp'), P('dp')), out_specs=(P(), P('dp', None), P(None), P('tp', None)), check_vma=False)
```

```python
import jax
import jax.numpy as jnp
from jax import lax
from jax.experimental import pallas as pl
from jax.experimental.pallas import tpu as pltpu
from jax.sharding import PartitionSpec as P

SOFT_CAP = 30.0
NORM_EPS = 1e-6
VMEM_FRONT = 40 * 2 ** 20
SPLIT = 2


def pos_of(cyc, dp):
    z, y = dp // 4, dp % 4
    if cyc == 0:
        return z * 4 + (y + z) % 4
    return y * 4 + (z + y) % 4


def dp_of(cyc, pos):
    a = pos // 4
    b = (pos % 4 - a + 4) % 4
    if cyc == 0:
        return a * 4 + b
    return b * 4 + a


def place(table, pieces, group, step, rows, vocab):
    part, dim = pieces[0].shape

    def kern(*refs):
        srcs, dst, sem = refs[:4], refs[-2], refs[-1]
        me = lax.axis_index('dp')
        copies = []
        for ring in range(4):
            sgn = 1 if ring % 2 == 0 else -1
            owner = dp_of(ring // 2, (pos_of(ring // 2, me) - sgn * step + 32) % 16)
            start = pl.multiple_of(owner * rows + (group * 4 + ring) * part, 8)
            copies.append(pltpu.make_async_copy(srcs[ring], dst.at[pl.ds(start, part)], sem.at[ring]))
        for cp in copies:
            cp.start()
        for cp in copies:
            cp.wait()

    vm = pl.BlockSpec(memory_space=pltpu.VMEM)
    hb = pl.BlockSpec(memory_space=pltpu.HBM)
    args = list(pieces) if table is None else [*pieces, table]
    return pl.pallas_call(kern, out_shape=jax.ShapeDtypeStruct((vocab, dim), jnp.float32), in_specs=[vm] * 4 + [hb] * (len(args) - 4), out_specs=hb,
        scratch_shapes=[pltpu.SemaphoreType.DMA((4,))], input_output_aliases={} if table is None else {4: 0}, name='place',
        compiler_params=pltpu.CompilerParams(vmem_limit_bytes=2 ** 22),
        cost_estimate=pl.CostEstimate(flops=10 ** 7, bytes_accessed=8 * part * dim * 4, transcendentals=0))(*args)


def gather_rings(groups, vocab):
    half, dim = groups[0].shape
    part = half // 4
    rows = half * SPLIT
    held = [[g[ring * part:(ring + 1) * part] for ring in range(4)] for g in groups]
    table = None
    for s in range(1, 16):
        for c in range(SPLIT):
            new = []
            for ring in range(4):
                cyc, sgn = ring // 2, 1 if ring % 2 == 0 else -1
                perm = [(d, dp_of(cyc, (pos_of(cyc, d) + sgn) % 16)) for d in range(16)]
                new.append(lax.ppermute(held[c][ring], 'dp', perm))
            table = place(table, held[c], c, s - 1, rows, vocab)
            table, *held[c] = lax.optimization_barrier((table, *new))
    for c in range(SPLIT):
        table = place(table, held[c], c, 15, rows, vocab)
    return table


OFFSETS = tuple((dz, dy) for dz in range(4) for dy in range(4))


def shift(dp, dz, dy):
    return (dp // 4 + dz + 4) % 4 * 4 + (dp % 4 + dy + 4) % 4


FAR = ((2, 0), (0, 2), (2, 1), (1, 2), (2, 3), (3, 2), (2, 2))


def legs(dz, dy, way):
    if dz == dy:
        return (way, way), (way, way)
    return ((way, 0), (way, dy)) if dz == 2 else ((0, way), (dz, way))


HOPS = tuple((o, *legs(*o, way)) for o in FAR for way in (1, 3))
DIRECT = ((1, 0), (3, 0), (0, 1), (0, 3), (1, 1), (3, 3), (1, 3), (3, 1))
ORDER = (*FAR, *DIRECT, (0, 0))
MESH = pl.DeviceIdType.MESH


def front(hidden, gain_row, mask_row, teacher, table):
    tokens, vocab = teacher.shape
    dim = hidden.shape[1]
    part = vocab // 16
    half = tokens // 2
    few = tokens // 8
    inv_cap = 1.0 / SOFT_CAP
    sub = 512
    f32 = jnp.float32

    def kern(hid_ref, w_ref, mask_ref, tea_ref, tab_ref, got_ref, x_out, tab_out, coef_ref, all_ref, gh_ref, gg_ref,
             raw, sends, stage, tabs, n_buf, x_buf, inv_buf, square, pay, pay_got, x_got, tp_got, own_col, own_row, rel, dx, rs_got, ag_own, ag_got, gn_own, gn_got,
             raw_sem, tab_sem, tabp_sem, out_sem, stage_sem, got_sem, tp_out, tp_in, dp_out, dp_in, pay_out, pay_in, xt_out, xt_in,
             rs_out, rs_in, ag_out, ag_in, gn_out, gn_in):
        me, col = lax.axis_index('dp'), lax.axis_index('tp')
        my_few = pl.ds(pl.multiple_of(col * few, few), few)

        def fetch(k):
            d = shift(me, *ORDER[k])
            return pltpu.make_async_copy(tea_ref.at[:, pl.ds(pl.multiple_of(d * part, 128), part)], raw.at[d], raw_sem.at[k])

        def tab_copy(i):
            start = pl.multiple_of(lax.rem(i, 16) * part, 128)
            return pltpu.make_async_copy(tab_ref.at[pl.ds(start, part)], tabs.at[lax.rem(i, 3)], tab_sem.at[lax.rem(i, 3)])

        own_tab = pltpu.make_async_copy(tab_ref.at[pl.ds(pl.multiple_of(me * part, 128), part)], tab_out, tabp_sem)
        for k in range(16):
            fetch(k).start()
        for i in range(2):
            tab_copy(i).start()
        own_tab.start()
        barrier = pltpu.get_barrier_semaphore()
        for dz, dy in OFFSETS[1:]:
            pl.semaphore_signal(barrier, inc=1, device_id=(shift(me, dz, dy), col), device_id_type=MESH)
        for j in range(1, 8):
            pl.semaphore_signal(barrier, inc=1, device_id=(me, (col + j) % 8), device_id_type=MESH)

        hid = hid_ref[...].astype(f32)
        inv = lax.rsqrt(jnp.mean(hid * hid, axis=1, keepdims=True) + NORM_EPS)
        n_buf[...] = hid * inv
        x_buf[...] = (n_buf[...] * w_ref[...]).astype(jnp.bfloat16)
        inv_buf[...] = jnp.broadcast_to(inv, (tokens, 128))
        pay[...] = jnp.zeros((16, dim), f32)
        pay[0:few] = n_buf[my_few]
        pay[8:9, 0:tokens] = mask_ref[...]
        square[...] = jnp.zeros((128, 128), f32)
        square[0:1, 0:tokens] = mask_ref[...]
        mask_col = jnp.transpose(square[...])[0:tokens, 0:1]
        pl.semaphore_wait(barrier, 22)

        def remote(src, dst, out, into, dp, tp):
            return pltpu.make_async_remote_copy(src_ref=src, dst_ref=dst, send_sem=out, recv_sem=into, device_id=(dp, tp), device_id_type=MESH)

        def to_dp(src, dst, out, into):
            def send(k):
                return remote(src, dst.at[me], out.at[k], into.at[me], shift(me, *OFFSETS[k]), col)

            def came(k):
                d = shift(me, *OFFSETS[k])
                return remote(src, dst.at[d], out.at[k], into.at[d], d, col)

            return [send(k) for k in range(1, 16)], [came(k) for k in range(1, 16)]

        def to_tp(srcs, dst, out, into):
            def send(j):
                c = (col + j) % 8
                return remote(srcs(c), dst.at[col], out.at[j], into.at[col], me, c)

            def came(j):
                c = (col + j) % 8
                return remote(srcs(c), dst.at[c], out.at[j], into.at[c], me, c)

            return [send(j) for j in range(1, 8)], [came(j) for j in range(1, 8)]

        def leg_one(j):
            (dz, dy), (az, ay), _ = HOPS[j]
            src = sends.at[shift(me, dz, dy), pl.ds(j % 2 * half, half)]
            return remote(src, stage.at[j], out_sem.at[j], stage_sem.at[j], shift(me, az, ay), col)

        def leg_two(j):
            (dz, dy), _, (bz, by) = HOPS[j]
            dst = got_ref.at[dz * 4 + dy, pl.ds(j % 2 * half, half)]
            return remote(stage.at[j], dst, out_sem.at[14 + j], got_sem.at[j], shift(me, bz, by), col)

        def direct(j):
            d = shift(me, *DIRECT[j])
            return remote(sends.at[d], got_ref.at[DIRECT[j][0] * 4 + DIRECT[j][1]], out_sem.at[28 + j], got_sem.at[14 + j], d, col)

        pay_sends, pay_came = to_dp(pay, pay_got, pay_out, pay_in)
        for cp in pay_sends:
            cp.start()
        pay_got[me] = pay[...]

        for k in range(16):
            fetch(k).wait()
            d = shift(me, *ORDER[k])

            def rows(r, _):
                here = pl.ds(pl.multiple_of(r * 16, 16), 16)
                cap = jnp.tanh(raw[d, here].astype(f32) * inv_cap)
                sends[d, here] = jnp.exp(SOFT_CAP * cap - SOFT_CAP)
                return 0

            lax.fori_loop(0, tokens // 16, rows, 0)
            if k < 7:
                leg_one(2 * k).start()
                leg_one(2 * k + 1).start()
            elif k < 15:
                direct(k - 7).start()

        def keep(r, _):
            here = pl.ds(pl.multiple_of(r * 16, 16), 16)
            got_ref[0, here] = sends[me, here]
            return 0

        lax.fori_loop(0, tokens // 16, keep, 0)

        def fold(v):
            total = v[:, 0:128]
            for c in range(1, v.shape[1] // 128):
                total = total + v[:, c * 128:(c + 1) * 128]
            return total

        def student(slot, here):
            z = lax.dot_general(x_buf[...], tabs[slot, here], (((1,), (1,)), ((), ())), preferred_element_type=f32)
            ratio = jnp.tanh(z * inv_cap)
            return ratio, jnp.exp(SOFT_CAP * ratio - SOFT_CAP)

        def forward(i, sums):
            slot = lax.rem(i, 3)
            tab_copy(i).wait()
            tab_copy(i + 2).start()
            s_sum, t_sum, k_sum = sums
            for c in range(part // sub):
                here = pl.ds(c * sub, sub)
                ratio, stu = student(slot, here)
                cap = jnp.tanh(raw[i, :, here].astype(f32) * inv_cap)
                tea = sends[i, :, here]
                s_sum = s_sum + fold(stu)
                t_sum = t_sum + fold(tea)
                k_sum = k_sum + fold(tea * (cap - ratio))
            return s_sum, t_sum, k_sum

        zero = jnp.zeros((tokens, 128), f32)
        s_sum, t_sum, k_sum = lax.fori_loop(0, 16, forward, (zero, zero, zero))
        lane = lax.broadcasted_iota(jnp.int32, (tokens, 128), 1)
        sums = jnp.where(lane == 0, jnp.sum(s_sum, axis=1, keepdims=True), 0.0)
        sums = jnp.where(lane == 1, jnp.sum(t_sum, axis=1, keepdims=True), sums)
        sums = jnp.where(lane == 2, SOFT_CAP * jnp.sum(k_sum, axis=1, keepdims=True), sums)
        own_col[...] = sums
        tp_got[col] = sums
        tp_sends, tp_came = to_tp(lambda c: own_col, tp_got, tp_out, tp_in)
        for cp in tp_sends:
            cp.start()
        for cp in tp_came:
            cp.wait_recv()
        total = tp_got[0]
        for j in range(1, 8):
            total = total + tp_got[j]
        stats = jnp.where(lane == 3, mask_col, total)
        square[0:tokens] = stats
        line = jnp.transpose(square[...])[0:8]
        own_row[...] = line
        all_ref[me] = line
        dp_sends, dp_came = to_dp(own_row, all_ref, dp_out, dp_in)
        for cp in dp_sends:
            cp.start()
        for j in range(14):
            leg_one(j).wait_recv()
            leg_two(j).start()

        for cp in pay_came:
            cp.wait_recv()
        x_got[col] = pay_got[...]
        xt_sends, xt_came = to_tp(lambda c: pay_got, x_got, xt_out, xt_in)
        for cp in xt_sends:
            cp.start()
        masks = pay_got[0, 8:9]
        for d in range(1, 16):
            masks = masks + pay_got[d, 8:9]
        count = jnp.sum(masks, axis=1, keepdims=True)
        inv_s, inv_t, weight = 1.0 / total[:, 0:1], 1.0 / total[:, 1:2], mask_col / count
        dx[...] = jnp.zeros((tokens, dim), f32)

        def backward(i, _):
            slot = lax.rem(i, 3)
            tab_copy(i).wait()

            @pl.when(i + 2 < 32)
            def _():
                tab_copy(i + 2).start()

            for c in range(part // sub):
                here = pl.ds(c * sub, sub)
                ratio, stu = student(slot, here)
                diff = (stu * inv_s - sends[i - 16, :, here] * inv_t) * weight
                g = (diff * (1.0 - ratio * ratio)).astype(jnp.bfloat16)
                dx[...] += jnp.dot(g, tabs[slot, here], preferred_element_type=f32)
            return 0

        lax.fori_loop(16, 32, backward, 0)

        rs_got[col] = dx[my_few]
        rs_sends, rs_came = to_tp(lambda c: dx.at[pl.ds(pl.multiple_of(c * few, few), few)], rs_got, rs_out, rs_in)
        for cp in rs_sends:
            cp.start()
        for cp in rs_came:
            cp.wait_recv()
        my_x = rs_got[0]
        for j in range(1, 8):
            my_x = my_x + rs_got[j]
        my_n = n_buf[my_few]
        grad_n = my_x * w_ref[...]
        my_h = inv_buf[my_few, 0:1] * (grad_n - my_n * jnp.mean(grad_n * my_n, axis=1, keepdims=True))
        ag_own[...] = jnp.zeros((16, dim), f32)
        ag_own[0:few] = my_h
        ag_own[8:9] = jnp.sum(my_x * my_n, axis=0, keepdims=True)
        ag_got[col] = ag_own[...]
        ag_sends, ag_came = to_tp(lambda c: ag_own, ag_got, ag_out, ag_in)
        for cp in ag_sends:
            cp.start()
        for cp in ag_came:
            cp.wait_recv()
        gh_ref[...] = jnp.concatenate([ag_got[j, 0:few] for j in range(8)], axis=0).astype(jnp.bfloat16)
        line = ag_got[0, 8:16]
        for j in range(1, 8):
            line = line + ag_got[j, 8:16]
        gn_own[...] = line
        gn_got[me] = line
        gn_sends, gn_came = to_dp(gn_own, gn_got, gn_out, gn_in)
        for cp in gn_sends:
            cp.start()

        for cp in xt_came:
            cp.wait_recv()

        def widen(d, _):
            rows = jnp.concatenate([x_got[j, d, 0:few] for j in range(8)], axis=0)
            x_out[pl.ds(pl.multiple_of(d * tokens, tokens), tokens)] = (rows * w_ref[...]).astype(jnp.bfloat16)
            return 0

        lax.fori_loop(0, 16, widen, 0)
        for cp in dp_came:
            cp.wait_recv()
        row = lax.broadcasted_iota(jnp.int32, (8, 128), 0)
        lanes = lax.broadcasted_iota(jnp.int32, (8, 128), 1)
        for d in range(16):
            block = all_ref[d]
            safe = jnp.where((row < 2) & (lanes < tokens), block, 1.0)
            rel[d * 8:(d + 1) * 8] = jnp.where(row < 2, 1.0 / safe, block / count)
        for k, (dz, dy) in enumerate(OFFSETS):
            square[k * 8:(k + 1) * 8] = rel[pl.ds(pl.multiple_of(shift(me, -dz, -dy) * 8, 8), 8)]
        coef_ref[...] = jnp.transpose(square[...])

        for cp in gn_came:
            cp.wait_recv()
        line = gn_got[0]
        for d in range(1, 16):
            line = line + gn_got[d]
        gg_ref[...] = line
        own_tab.wait()
        for j in range(8):
            direct(j).wait_recv()
        for j in range(14):
            leg_two(j).wait_recv()
        for j in range(14):
            leg_one(j).wait_send()
            leg_two(j).wait_send()
        for j in range(8):
            direct(j).wait_send()
        for cp in (*pay_sends, *tp_sends, *dp_sends, *xt_sends, *rs_sends, *ag_sends, *gn_sends):
            cp.wait_send()

    vm = pl.BlockSpec(memory_space=pltpu.VMEM)
    hb = pl.BlockSpec(memory_space=pltpu.HBM)
    dma = pltpu.SemaphoreType.DMA
    return pl.pallas_call(
        kern,
        out_shape=(jax.ShapeDtypeStruct((16, tokens, part), f32), jax.ShapeDtypeStruct((16 * tokens, dim), jnp.bfloat16),
                   jax.ShapeDtypeStruct((part, dim), table.dtype), jax.ShapeDtypeStruct((128, 128), f32), jax.ShapeDtypeStruct((16, 8, 128), f32),
                   jax.ShapeDtypeStruct((tokens, dim), jnp.bfloat16), jax.ShapeDtypeStruct((8, dim), f32)),
        in_specs=[vm, vm, vm, hb, hb], out_specs=(vm, vm, vm, vm, vm, vm, vm),
        scratch_shapes=[
            pltpu.VMEM((16, tokens, part), teacher.dtype), pltpu.VMEM((16, tokens, part), f32), pltpu.VMEM((14, half, part), f32),
            pltpu.VMEM((3, part, dim), table.dtype), pltpu.VMEM((tokens, dim), f32), pltpu.VMEM((tokens, dim), jnp.bfloat16),
            pltpu.VMEM((tokens, 128), f32), pltpu.VMEM((128, 128), f32), pltpu.VMEM((16, dim), f32), pltpu.VMEM((16, 16, dim), f32),
            pltpu.VMEM((8, 16, 16, dim), f32), pltpu.VMEM((8, tokens, 128), f32), pltpu.VMEM((tokens, 128), f32), pltpu.VMEM((8, 128), f32),
            pltpu.VMEM((128, 128), f32), pltpu.VMEM((tokens, dim), f32), pltpu.VMEM((8, few, dim), f32), pltpu.VMEM((16, dim), f32),
            pltpu.VMEM((8, 16, dim), f32), pltpu.VMEM((8, dim), f32), pltpu.VMEM((16, 8, dim), f32),
            dma((16,)), dma((3,)), dma, dma((36,)), dma((14,)), dma((22,)), dma((8,)), dma((8,)), dma((16,)), dma((16,)),
            dma((16,)), dma((16,)), dma((8,)), dma((8,)), dma((8,)), dma((8,)), dma((8,)), dma((8,)), dma((16,)), dma((16,))],
        compiler_params=pltpu.CompilerParams(collective_id=0, has_side_effects=True, vmem_limit_bytes=VMEM_FRONT),
        cost_estimate=pl.CostEstimate(flops=3 * 10 ** 9, bytes_accessed=10 ** 8, transcendentals=0), name='front')(
            hidden, gain_row, mask_row, pltpu.with_memory_space_constraint(teacher, pltpu.HBM), pltpu.with_memory_space_constraint(table, pltpu.HBM))


def finish(teas, x_all, tab_part, coef, group):
    n, tokens, part = teas.shape
    total, dim = x_all.shape
    span = part // SPLIT
    tile = span // 2
    inv_cap = 1.0 / SOFT_CAP

    def kern(tea_ref, x_ref, tab_ref, coef_ref, out_ref, z_buf, g_buf):
        me = lax.axis_index('dp')
        for t in range(2):
            base = group * span + t * tile
            z_buf[t] = lax.dot_general(x_ref[...], tab_ref[base:base + tile], (((1,), (1,)), ((), ())), preferred_element_type=jnp.float32)
        for t in range(2):
            base = group * span + t * tile
            for k, (dz, dy) in enumerate(OFFSETS):
                here = pl.ds(pl.multiple_of(shift(me, -dz, -dy) * tokens, tokens), tokens)
                ratio = jnp.tanh(z_buf[t, here] * inv_cap)
                stu = jnp.exp(SOFT_CAP * ratio - SOFT_CAP)
                inv_s, inv_t = coef_ref[0:tokens, k * 8:k * 8 + 1], coef_ref[0:tokens, k * 8 + 1:k * 8 + 2]
                wgt = coef_ref[0:tokens, k * 8 + 3:k * 8 + 4]
                diff = (stu * inv_s - tea_ref[k, :, base:base + tile] * inv_t) * wgt
                g_buf[t, here] = (diff * (1.0 - ratio * ratio)).astype(jnp.bfloat16)
            out_ref[t * tile:(t + 1) * tile] = lax.dot_general(g_buf[t], x_ref[...], (((0,), (0,)), ((), ())), preferred_element_type=jnp.float32)

    vm = pl.BlockSpec(memory_space=pltpu.VMEM)
    hb = pl.BlockSpec(memory_space=pltpu.HBM)
    return pl.pallas_call(kern, out_shape=jax.ShapeDtypeStruct((span, dim), jnp.float32), in_specs=[vm, vm, vm, vm], out_specs=vm,
        scratch_shapes=[pltpu.VMEM((2, total, tile), jnp.float32), pltpu.VMEM((2, total, tile), jnp.bfloat16)], name='finish',
        compiler_params=pltpu.CompilerParams(vmem_limit_bytes=26 * 2 ** 20),
        cost_estimate=pl.CostEstimate(flops=10 ** 9, bytes_accessed=10 ** 7, transcendentals=0))(
            teas, x_all, tab_part, coef)


def solution(mesh):
    def local_step(hid_rows, w_final, tab_rows, tea_rows, mask_rows):
        tokens, dim = hid_rows.shape
        vocab = tab_rows.shape[0]
        teas, x_all, tab_part, coef, stats, grad_h, gain_lines = front(hid_rows, (1.0 + w_final)[None], mask_rows[None], tea_rows, tab_rows)
        groups = [finish(teas, x_all, tab_part, coef, c) for c in range(SPLIT)]
        table = gather_rings(groups, vocab)
        stats = stats[:, :, :tokens]
        all_kl = stats[:, 2] / stats[:, 1] + jnp.log(stats[:, 0]) - jnp.log(stats[:, 1])
        loss_val = jnp.sum(stats[:, 3] * all_kl) / jnp.sum(stats[:, 3])
        return loss_val, grad_h, gain_lines[0], table

    return jax.shard_map(local_step, mesh=mesh, in_specs=(P('dp', None), P(None), P('tp', None), P('dp', 'tp'), P('dp')), out_specs=(P(), P('dp', None), P(None), P('tp', None)), check_vma=False)
```

```python
import jax
import jax.numpy as jnp
from jax import lax
from jax.experimental import pallas as pl
from jax.experimental.pallas import tpu as pltpu
from jax.sharding import PartitionSpec as P


SOFT_CAP = 30.0
INV_CAP = 1.0 / SOFT_CAP
NORM_EPS = 1e-6
SIDE, N_DP, N_TP, LANES = 4, 16, 8, 128
UP, DOWN, AWAY = 1, 3, 2
MIB = 2 ** 20
MESH = pl.DeviceIdType.MESH
VM = pl.BlockSpec(memory_space=pltpu.VMEM)
HB = pl.BlockSpec(memory_space=pltpu.HBM)
F32, BF16 = jnp.float32, jnp.bfloat16
ROWS_BY_ROWS = (((1,), (1,)), ((), ()))
COLS_BY_COLS = (((0,), (0,)), ((), ()))

OFFSETS = tuple((dz, dy) for dz in range(SIDE) for dy in range(SIDE))
ORDER = tuple(sorted(OFFSETS, key=lambda o: -sum(min(d, SIDE - d) for d in o)))


def shift(dp, dz, dy):
    return (dp // SIDE + dz + SIDE) % SIDE * SIDE + (dp % SIDE + dy + SIDE) % SIDE


def aligned(start, size, unit=LANES):
    return pl.ds(pl.multiple_of(start, unit), size)


def hops(kind, dz, dy):
    along_z = [(dz, 0)] if dz % 2 else [(UP if dy < AWAY else DOWN, 0)] * dz
    along_y = [(0, dy)] if dy % 2 else [(0, UP if dz < AWAY else DOWN)] * dy
    return along_y + along_z if kind else along_z + along_y


JOBS = tuple((kind, o) for o in ORDER[:-1] for kind in range(2))
PATHS = tuple(hops(kind, *o) for kind, o in JOBS)
STEPS = tuple((j, level) for level in range(SIDE) for j, path in enumerate(PATHS) if len(path) > level)
MIDDLE = tuple((j, level) for j, level in STEPS if len(PATHS[j]) > level + 1)


def front(hidden, gain_row, mask_row, teacher, table):
    tokens, vocab = teacher.shape
    dim = hidden.shape[1]
    part = vocab // N_DP
    half = tokens // 2
    few = tokens // N_TP
    pack = 16
    sub = 512
    tile = part // 2
    tiles = vocab // tile
    depth = 3

    def kern(hid_hbm, gain_ref, mask_in, tea_ref, tab_ref, got_ref, x_out, tab_out, coef_ref, all_ref, gh_ref, gg_ref,
             hid_ref, w_ref, raw, sends, stage, tabs, n_buf, x_buf, inv_buf, square, pay, pay_got, mask_own, mask_got, x_got, tp_got, own_col,
             own_row, rel, dx, rs_got, ag_own, ag_got, gn_own, gn_got, raw_sem, tab_sem, in_sem, hop_sem, dp_sem, tp_sem):
        me, col = lax.axis_index('dp'), lax.axis_index('tp')
        my_few = aligned(col * few, few, few)

        def fetch(k):
            d = shift(me, *ORDER[k])
            return pltpu.make_async_copy(tea_ref.at[:, aligned(d * part, part)], raw.at[d], raw_sem.at[k])

        def tab_copy(i):
            slot = lax.rem(i, depth)
            return pltpu.make_async_copy(tab_ref.at[aligned(lax.rem(i, tiles) * tile, tile)], tabs.at[slot], tab_sem.at[slot])

        own_hid = pltpu.make_async_copy(hid_hbm, hid_ref, in_sem.at[0])
        own_tab = pltpu.make_async_copy(tab_ref.at[aligned(me * part, part)], tab_out, in_sem.at[1])
        own_hid.start()
        for k in range(N_DP):
            fetch(k).start()
        for i in range(depth - 1):
            tab_copy(i).start()
        own_tab.start()
        barrier = pltpu.get_barrier_semaphore()
        for dz, dy in ORDER[:-1]:
            pl.semaphore_signal(barrier, inc=1, device_id=(shift(me, dz, dy), col), device_id_type=MESH)
        for j in range(1, N_TP):
            pl.semaphore_signal(barrier, inc=1, device_id=(me, (col + j) % N_TP), device_id_type=MESH)

        w_ref[...] = 1.0 + gain_ref[...]
        own_hid.wait()
        hid = hid_ref[...].astype(F32)
        inv = lax.rsqrt(jnp.mean(hid * hid, axis=1, keepdims=True) + NORM_EPS)
        n_buf[...] = hid * inv
        x_buf[...] = (n_buf[...] * w_ref[...]).astype(BF16)
        inv_buf[...] = jnp.broadcast_to(inv, (tokens, LANES))
        pay[...] = n_buf[my_few]
        square[...] = jnp.zeros((LANES, LANES), F32)
        square[0:1, 0:tokens] = mask_in[...]
        mask_own[...] = square[0:few]
        mask_col = jnp.transpose(square[...])[0:tokens, 0:1]
        pl.semaphore_wait(barrier, N_DP + N_TP - 2)

        def remote(src, dst, out, into, dp, tp):
            return pltpu.make_async_remote_copy(src_ref=src, dst_ref=dst, send_sem=out, recv_sem=into, device_id=(dp, tp), device_id_type=MESH)

        def to_dp(src, dst, x):
            def send(o):
                d = shift(me, *o)
                return remote(src, dst.at[me], dp_sem.at[x, 0, d], dp_sem.at[x, 1, me], d, col)

            def came(o):
                d = shift(me, *o)
                return remote(src, dst.at[d], dp_sem.at[x, 0, d], dp_sem.at[x, 1, d], d, col)

            return [send(o) for o in ORDER[:-1]], [came(o) for o in ORDER[:-1]]

        def to_tp(srcs, dst, x):
            def send(j):
                c = (col + j) % N_TP
                return remote(srcs(c), dst.at[col], tp_sem.at[x, 0, c], tp_sem.at[x, 1, col], me, c)

            def came(j):
                c = (col + j) % N_TP
                return remote(srcs(c), dst.at[c], tp_sem.at[x, 0, c], tp_sem.at[x, 1, c], me, c)

            return [send(j) for j in range(1, N_TP)], [came(j) for j in range(1, N_TP)]

        def start(copies):
            for cp in copies:
                cp.start()

        def arrive(copies):
            for cp in copies:
                cp.wait_recv()

        def added(ref, here=slice(None)):
            total = ref[0, here]
            for d in range(1, ref.shape[0]):
                total = total + ref[d, here]
            return total

        def hop(j, level):
            kind, (dz, dy) = JOBS[j]
            tok = pl.ds(kind * half, half)
            src = stage.at[MIDDLE.index((j, level - 1))] if level else sends.at[shift(me, dz, dy), tok]
            dst = stage.at[MIDDLE.index((j, level))] if (j, level) in MIDDLE else got_ref.at[dz * SIDE + dy, tok]
            k = STEPS.index((j, level))
            return remote(src, dst, hop_sem.at[0, k], hop_sem.at[1, k], shift(me, *PATHS[j][level]), col)

        def relay(level):
            for j, at in MIDDLE:
                if at == level:
                    hop(j, level).wait_recv()
                    hop(j, level + 1).start()

        pay_sends, pay_came = to_dp(pay, pay_got, 0)
        start(pay_sends)
        pay_got[me] = pay[...]
        mask_sends, mask_came = to_dp(mask_own, mask_got, 1)
        start(mask_sends)
        mask_got[me] = mask_own[...]

        for k, o in enumerate(ORDER):
            fetch(k).wait()
            d = shift(me, *o)

            def weigh(r, _):
                here = aligned(r * pack, pack, pack)
                cap = jnp.tanh(raw[d, here].astype(F32) * INV_CAP)
                sends[d, here] = jnp.exp(SOFT_CAP * cap - SOFT_CAP)
                return 0

            lax.fori_loop(0, tokens // pack, weigh, 0)
            for j, (_, to) in enumerate(JOBS):
                if to == o:
                    hop(j, 0).start()

        def keep(r, _):
            here = aligned(r * pack, pack, pack)
            got_ref[0, here] = sends[me, here]
            return 0

        lax.fori_loop(0, tokens // pack, keep, 0)

        def fold(v):
            total = v[:, :LANES]
            for c in range(LANES, v.shape[1], LANES):
                total = total + v[:, c:c + LANES]
            return total

        def student(slot, here):
            z = lax.dot_general(x_buf[...], tabs[slot, here], ROWS_BY_ROWS, preferred_element_type=F32)
            ratio = jnp.tanh(z * INV_CAP)
            return ratio, jnp.exp(SOFT_CAP * ratio - SOFT_CAP)

        def forward(i, sums):
            slot = lax.rem(i, depth)
            tab_copy(i).wait()
            tab_copy(i + depth - 1).start()
            s_sum, t_sum, k_sum = sums
            for c in range(0, tile, sub):
                ratio, stu = student(slot, pl.ds(c, sub))
                here = aligned(i % 2 * tile + c, sub)
                cap = jnp.tanh(raw[i // 2, :, here].astype(F32) * INV_CAP)
                tea = sends[i // 2, :, here]
                s_sum = s_sum + fold(stu)
                t_sum = t_sum + fold(tea)
                k_sum = k_sum + fold(tea * (cap - ratio))
            return s_sum, t_sum, k_sum

        zero = jnp.zeros((tokens, LANES), F32)
        s_sum, t_sum, k_sum = lax.fori_loop(0, tiles, forward, (zero, zero, zero))
        lane = lax.broadcasted_iota(jnp.int32, (tokens, LANES), 1)
        sums = jnp.where(lane == 0, jnp.sum(s_sum, axis=1, keepdims=True), 0.0)
        sums = jnp.where(lane == 1, jnp.sum(t_sum, axis=1, keepdims=True), sums)
        sums = jnp.where(lane == AWAY, SOFT_CAP * jnp.sum(k_sum, axis=1, keepdims=True), sums)
        own_col[...] = sums
        tp_got[col] = sums
        tp_sends, tp_came = to_tp(lambda c: own_col, tp_got, 0)
        start(tp_sends)
        arrive(tp_came)
        total = added(tp_got)
        square[0:tokens] = jnp.where(lane == DOWN, mask_col, total)
        line = jnp.transpose(square[...])[0:few]
        own_row[...] = line
        all_ref[me] = line
        dp_sends, dp_came = to_dp(own_row, all_ref, 2)
        start(dp_sends)
        relay(0)

        arrive((*pay_came, *mask_came))
        x_got[col] = pay_got[...]
        xt_sends, xt_came = to_tp(lambda c: pay_got, x_got, 1)
        start(xt_sends)
        count = jnp.sum(added(mask_got, slice(1)), axis=1, keepdims=True)
        inv_s, inv_t, weight = 1.0 / total[:, 0:1], 1.0 / total[:, 1:2], mask_col / count
        dx[...] = jnp.zeros((tokens, dim), F32)

        def backward(i, _):
            slot = lax.rem(i, depth)
            tab_copy(i).wait()

            @pl.when(i + depth - 1 < 2 * tiles)
            def _():
                tab_copy(i + depth - 1).start()

            for c in range(0, tile, sub):
                here = pl.ds(c, sub)
                ratio, stu = student(slot, here)
                tea = sends[(i - tiles) // 2, :, aligned(i % 2 * tile + c, sub)]
                diff = (stu * inv_s - tea * inv_t) * weight
                g = (diff * (1.0 - ratio * ratio)).astype(BF16)
                dx[...] += jnp.dot(g, tabs[slot, here], preferred_element_type=F32)
            return 0

        lax.fori_loop(tiles, 2 * tiles, backward, 0)
        relay(1)

        rs_got[col] = dx[my_few]
        rs_sends, rs_came = to_tp(lambda c: dx.at[aligned(c * few, few, few)], rs_got, 2)
        start(rs_sends)
        arrive(rs_came)
        my_x = added(rs_got)
        my_n = n_buf[my_few]
        grad_n = my_x * w_ref[...]
        my_h = inv_buf[my_few, 0:1] * (grad_n - my_n * jnp.mean(grad_n * my_n, axis=1, keepdims=True))
        ag_own[...] = jnp.zeros((2 * few, dim), F32)
        ag_own[0:few] = my_h
        ag_own[few:few + 1] = jnp.sum(my_x * my_n, axis=0, keepdims=True)
        ag_got[col] = ag_own[...]
        ag_sends, ag_came = to_tp(lambda c: ag_own, ag_got, DOWN)
        start(ag_sends)
        arrive(ag_came)
        gh_ref[...] = jnp.concatenate([ag_got[j, 0:few] for j in range(N_TP)], axis=0)
        line = added(ag_got, slice(few, 2 * few))
        gn_own[...] = line
        gn_got[me] = line
        gn_sends, gn_came = to_dp(gn_own, gn_got, DOWN)
        start(gn_sends)

        arrive(xt_came)

        def widen(d, _):
            rows = jnp.concatenate([x_got[j, d] for j in range(N_TP)], axis=0)
            x_out[aligned(d * tokens, tokens, tokens)] = (rows * w_ref[...]).astype(BF16)
            return 0

        lax.fori_loop(0, N_DP, widen, 0)
        arrive(dp_came)
        row = lax.broadcasted_iota(jnp.int32, (few, LANES), 0)
        lanes = lax.broadcasted_iota(jnp.int32, (few, LANES), 1)
        for d in range(N_DP):
            block = all_ref[d]
            safe = jnp.where((row < AWAY) & (lanes < tokens), block, 1.0)
            rel[d * few:(d + 1) * few] = jnp.where(row < AWAY, 1.0 / safe, block / count)
        for k, (dz, dy) in enumerate(OFFSETS):
            square[k * few:(k + 1) * few] = rel[aligned(shift(me, -dz, -dy) * few, few, few)]
        coef_ref[...] = jnp.transpose(square[...])

        relay(2)
        arrive(gn_came)
        gg_ref[...] = added(gn_got)
        own_tab.wait()
        for j, path in enumerate(PATHS):
            hop(j, len(path) - 1).wait_recv()
        for j, level in STEPS:
            hop(j, level).wait_send()
        for cp in (*pay_sends, *mask_sends, *tp_sends, *dp_sends, *xt_sends, *rs_sends, *ag_sends, *gn_sends):
            cp.wait_send()

    dma = pltpu.SemaphoreType.DMA
    wide, flat = (tokens, dim), (few, LANES)
    return pl.pallas_call(
        kern,
        out_shape=tuple(jax.ShapeDtypeStruct(shape, kind) for shape, kind in (
            ((N_DP, tokens, part), F32), ((N_DP * tokens, dim), BF16), ((part, dim), BF16), ((LANES, LANES), F32), ((N_DP, *flat), F32), (wide, F32),
            ((few, dim), F32))),
        in_specs=[HB, VM, VM, HB, HB], out_specs=(VM,) * 7,
        scratch_shapes=[pltpu.VMEM(shape, kind) for shape, kind in (
            (wide, BF16), ((1, dim), F32), ((N_DP, tokens, part), BF16), ((N_DP, tokens, part), F32), ((len(MIDDLE), half, part), F32),
            ((depth, tile, dim), BF16), (wide, F32), (wide, BF16), ((tokens, LANES), F32), ((LANES, LANES), F32), ((few, dim), F32),
            ((N_DP, few, dim), F32), (flat, F32), ((N_DP, *flat), F32), ((N_TP, N_DP, few, dim), F32), ((N_TP, tokens, LANES), F32),
            ((tokens, LANES), F32), (flat, F32), ((LANES, LANES), F32), (wide, F32), ((N_TP, few, dim), F32), ((2 * few, dim), F32),
            ((N_TP, 2 * few, dim), F32), ((few, dim), F32), ((N_DP, few, dim), F32))] + [
            dma((N_DP,)), dma((depth,)), dma((2,)), dma((2, len(STEPS))), dma((SIDE, 2, N_DP)), dma((SIDE, 2, N_TP))],
        compiler_params=pltpu.CompilerParams(collective_id=0, has_side_effects=True, vmem_limit_bytes=40 * MIB),
        cost_estimate=pl.CostEstimate(flops=3 * 10 ** 9, bytes_accessed=100 * MIB, transcendentals=0), name='front')(
            pltpu.with_memory_space_constraint(hidden, pltpu.HBM), gain_row, mask_row,
            pltpu.with_memory_space_constraint(teacher, pltpu.HBM), pltpu.with_memory_space_constraint(table, pltpu.HBM))


def finish(teas, x_all, tab_part, coef, block):
    tokens, part = teas.shape[1:]
    total, dim = x_all.shape
    span = part // SIDE
    few = LANES // N_DP

    def kern(tea_ref, x_ref, tab_ref, coef_ref, out_ref, z_buf, g_buf):
        me = lax.axis_index('dp')
        mine = pl.ds(block * span, span)
        z_buf[...] = lax.dot_general(x_ref[...], tab_ref[mine], ROWS_BY_ROWS, preferred_element_type=F32)
        for k, (dz, dy) in enumerate(OFFSETS):
            here = aligned(shift(me, -dz, -dy) * tokens, tokens, tokens)
            ratio = jnp.tanh(z_buf[here] * INV_CAP)
            stu = jnp.exp(SOFT_CAP * ratio - SOFT_CAP)
            inv_s, inv_t, _, weight = (coef_ref[0:tokens, k * few + i:k * few + i + 1] for i in range(SIDE))
            diff = (stu * inv_s - tea_ref[k, :, mine] * inv_t) * weight
            g_buf[here] = (diff * (1.0 - ratio * ratio)).astype(BF16)
        out_ref[...] = lax.dot_general(g_buf[...], x_ref[...], COLS_BY_COLS, preferred_element_type=F32)

    return pl.pallas_call(kern, out_shape=jax.ShapeDtypeStruct((span, dim), F32), in_specs=[VM] * 4, out_specs=VM,
        scratch_shapes=[pltpu.VMEM((total, span), F32), pltpu.VMEM((total, span), BF16)], name='finish',
        compiler_params=pltpu.CompilerParams(vmem_limit_bytes=22 * MIB),
        cost_estimate=pl.CostEstimate(flops=10 ** 9, bytes_accessed=8 * MIB, transcendentals=0))(teas, x_all, tab_part, coef)


def place(table, pieces, vocab):
    arrays = [p[0] for p in pieces]
    n = len(arrays)
    dim = arrays[0].shape[1]
    rows = vocab // N_DP
    cut = 256
    chunks = [(i, r) for i in range(n) for r in range(0, arrays[i].shape[0], cut)]
    size = sum(a.size for a in arrays)

    def kern(*refs):
        dst, sem = refs[-2], refs[-1]
        me = lax.axis_index('dp')
        copies = []
        for k, (i, r) in enumerate(chunks):
            _, dz, dy, first = pieces[i]
            there = aligned(shift(me, dz, dy) * rows + first + r, cut, cut)
            copies.append(pltpu.make_async_copy(refs[i].at[pl.ds(r, cut)], dst.at[there], sem.at[k]))
        for cp in copies:
            cp.start()
        for cp in copies:
            cp.wait()

    args = arrays if table is None else [*arrays, table]
    return pl.pallas_call(kern, out_shape=jax.ShapeDtypeStruct((vocab, dim), F32), in_specs=[VM] * n + [HB] * (len(args) - n), out_specs=HB,
        scratch_shapes=[pltpu.SemaphoreType.DMA((len(chunks),))], input_output_aliases={} if table is None else {n: 0}, name='place',
        compiler_params=pltpu.CompilerParams(vmem_limit_bytes=4 * size + MIB),
        cost_estimate=pl.CostEstimate(flops=10 * MIB, bytes_accessed=8 * size, transcendentals=0))(*args)


def gather(blocks, vocab):
    quarter = blocks[0].shape[0]
    sets, ways = range(2), (UP, DOWN)
    table, event = None, 0

    def send(pair, axis, step):
        out = []
        for k in sets:
            dz, dy = (step, 0) if axis == k else (0, step)
            out.append(lax.ppermute(pair[k], 'dp', [(d, shift(d, dz, dy)) for d in range(N_DP)]))
        return out

    def put(pair, a, b, c=0):
        return [(pair[k], *((b, a) if k else (a, b)), (2 * k + c) * quarter) for k in sets]

    def settle(*pieces):
        nonlocal table
        table = place(table, [p for ps in pieces for p in ps], vocab)

    def wait(*pairs):
        nonlocal table, event
        event += 1
        table, *flat = lax.optimization_barrier((table, *(x for pair in pairs for x in pair)))
        return [flat[2 * i:2 * i + 2] for i in range(len(pairs))]

    def join(one, other):
        return [jnp.concatenate(pair) for pair in zip(one, other)]

    own = [[blocks[c], blocks[2 + c]] for c in range(2)]
    low, high = ([send(own[c], 0, way) for c in range(2)] for way in ways)
    whole = join(*own)
    side = {way: send(whole, 1, way) for way in ways}
    settle(put(own[0], 0, 0, 0), put(own[1], 0, 0, 1))

    low[0], high[0] = wait(low[0], high[0])
    far_low = send(low[0], 0, UP)
    settle(put(low[0], DOWN, 0, 0), put(high[0], UP, 0, 0))

    low[1], high[1] = wait(low[1], high[1])
    far_high = send(high[1], 0, DOWN)
    low_whole, high_whole = join(*low), join(*high)
    low_side = {way: send(low_whole, 1, way) for way in ways}
    settle(put(low[1], DOWN, 0, 1), put(high[1], UP, 0, 1))

    side[UP], side[DOWN], high_whole = wait(side[UP], side[DOWN], high_whole)
    high_side = {way: send(high_whole, 1, way) for way in ways}
    side_far = send(side[UP], 1, UP)
    settle(put(side[UP], 0, DOWN))
    settle(put(side[DOWN], 0, UP))

    far_low, far_high = wait(far_low, far_high)
    far_side = {(c, way): send(pair, 1, way) for way in ways for c, pair in enumerate((far_low, far_high))}
    settle(put(far_low, AWAY, 0, 0), put(far_high, AWAY, 0, 1))

    low_side[UP], low_side[DOWN] = wait(low_side[UP], low_side[DOWN])
    low_far = send(low_side[DOWN], 1, DOWN)
    settle(put(low_side[UP], DOWN, DOWN))
    settle(put(low_side[DOWN], DOWN, UP))

    high_side[UP], high_side[DOWN] = wait(high_side[UP], high_side[DOWN])
    high_far = [send([x[:quarter] for x in high_side[UP]], 1, UP), send([x[quarter:] for x in high_side[DOWN]], 1, DOWN)]
    settle(put(high_side[UP], UP, DOWN))
    settle(put(high_side[DOWN], UP, UP))

    far_side[0, DOWN], far_side[1, DOWN], side_far = wait(far_side[0, DOWN], far_side[1, DOWN], side_far)
    last_down = send(far_side[1, DOWN], 1, DOWN)
    settle(put(far_side[0, DOWN], AWAY, UP, 0), put(far_side[1, DOWN], AWAY, UP, 1))
    settle(put(side_far, 0, AWAY))

    far_side[0, UP], = wait(far_side[0, UP])
    last_up = send(far_side[0, UP], 1, UP)
    settle(put(far_side[0, UP], AWAY, DOWN, 0))

    far_side[1, UP], low_far = wait(far_side[1, UP], low_far)
    settle(put(far_side[1, UP], AWAY, DOWN, 1))
    settle(put(low_far, DOWN, AWAY))

    high_far = wait(*high_far)
    settle(put(high_far[0], UP, AWAY, 0), put(high_far[1], UP, AWAY, 1))
    last_up, last_down = wait(last_up, last_down)
    settle(put(last_up, AWAY, AWAY, 0), put(last_down, AWAY, AWAY, 1))
    return table


def solution(mesh):
    def local_step(hid_rows, w_final, tab_rows, tea_rows, mask_rows):
        tokens = hid_rows.shape[0]
        teas, x_all, tab_part, coef, stats, grad_h, gain_lines = front(hid_rows, w_final[None], mask_rows[None], tea_rows, tab_rows)
        blocks = [None] * SIDE
        for i in (0, 2, 1, 3):
            blocks[i] = finish(teas, x_all, tab_part, coef, i)
            coef, blocks[i] = lax.optimization_barrier((coef, blocks[i]))
        table = gather(blocks, tab_rows.shape[0])
        s_sum, t_sum, k_sum, masks = (stats[:, i, :tokens] for i in range(SIDE))
        all_kl = k_sum / t_sum + jnp.log(s_sum) - jnp.log(t_sum)
        loss_val = jnp.sum(masks * all_kl) / jnp.sum(masks)
        return loss_val, grad_h.astype(BF16), gain_lines[0], table

    return jax.shard_map(local_step, mesh=mesh, in_specs=(P('dp', None), P(None), P('tp', None), P('dp', 'tp'), P('dp')), out_specs=(P(), P('dp', None), P(None), P('tp', None)), check_vma=False)
```

```python
import jax
import jax.numpy as jnp
from jax import lax
from jax.experimental import pallas as pl
from jax.experimental.pallas import tpu as pltpu
from jax.sharding import PartitionSpec as P


SOFT_CAP = 30.0
INV_CAP = 1.0 / SOFT_CAP
NORM_EPS = 1e-6
SIDE, N_DP, N_TP, LANES = 4, 16, 8, 128
UP, DOWN, AWAY = 1, 3, 2
MIB = 2 ** 20
L_FRONT = 41
MESH = pl.DeviceIdType.MESH
VM = pl.BlockSpec(memory_space=pltpu.VMEM)
HB = pl.BlockSpec(memory_space=pltpu.HBM)
F32, BF16 = jnp.float32, jnp.bfloat16
ROWS_BY_ROWS = (((1,), (1,)), ((), ()))
COLS_BY_COLS = (((0,), (0,)), ((), ()))

OFFSETS = tuple((dz, dy) for dz in range(SIDE) for dy in range(SIDE))
ORDER = tuple(sorted(OFFSETS, key=lambda o: -sum(min(d, SIDE - d) for d in o)))


def shift(dp, dz, dy):
    return (dp // SIDE + dz + SIDE) % SIDE * SIDE + (dp % SIDE + dy + SIDE) % SIDE


def peers():
    me = lax.axis_index('dp')
    z, y = lax.div(me, SIDE), lax.rem(me, SIDE)
    zs = [lax.rem(z + d, SIDE) * SIDE for d in range(SIDE)]
    ys = [lax.rem(y + d, SIDE) for d in range(SIDE)]
    return me, {(dz, dy): zs[dz] + ys[dy] for dz in range(-DOWN, SIDE) for dy in range(-DOWN, SIDE)}


def aligned(start, size, unit=LANES):
    return pl.ds(pl.multiple_of(start, unit), size)


def hops(kind, dz, dy):
    along_z = [(dz, 0)] if dz % 2 else [(UP if dy < AWAY else DOWN, 0)] * dz
    along_y = [(0, dy)] if dy % 2 else [(0, UP if dz < AWAY else DOWN)] * dy
    return along_y + along_z if kind else along_z + along_y


JOBS = tuple((kind, o) for o in ORDER[:-1] for kind in range(2))
PATHS = tuple(hops(kind, *o) for kind, o in JOBS)
MIDDLE = tuple((j, level) for level in range(SIDE) for j, path in enumerate(PATHS) if len(path) > level + 1)


def waves(j, level):
    return (None,) if (j, level) in MIDDLE and level < 2 else (0, 1)


COPIES = tuple((j, level, w) for j, path in enumerate(PATHS) for level in range(len(path)) for w in waves(j, level))


def grad_block(at, tea_ref, x_ref, tab_rows, coef_ref, z_buf, g_buf, out_ref, block):
    tokens = tea_ref.shape[1]
    span = tab_rows.shape[0]
    few = LANES // N_DP
    cols = aligned(block * span, span)
    z_buf[:, :span] = lax.dot_general(x_ref[...], tab_rows, ROWS_BY_ROWS, preferred_element_type=F32)
    for k, (dz, dy) in enumerate(OFFSETS):
        here = aligned(at[-dz, -dy] * tokens, tokens, tokens)
        ratio = jnp.tanh(z_buf[here, :span] * INV_CAP)
        stu = jnp.exp(SOFT_CAP * ratio - SOFT_CAP)
        inv_s, inv_t, _, weight = (coef_ref[0:tokens, k * few + i:k * few + i + 1] for i in range(SIDE))
        diff = (stu * inv_s - tea_ref[k, :, cols] * inv_t) * weight
        g_buf[here, :span] = (diff * (1.0 - ratio * ratio)).astype(BF16)
    out_ref[block] = lax.dot_general(g_buf[:, :span], x_ref[...], COLS_BY_COLS, preferred_element_type=F32)


def front(hidden, gain_row, mask_row, teacher, table):
    tokens, vocab = teacher.shape
    dim = hidden.shape[1]
    part = vocab // N_DP
    half = tokens // 2
    few = tokens // N_TP
    pack = 16
    sub = 512
    tile = part // 2
    tiles = vocab // tile
    depth = 3

    def kern(hid_hbm, gain_hbm, mask_hbm, tea_ref, tab_ref, got_late, blocks_ref, x_out, tab_out, coef_ref, all_ref, gh_ref, gg_ref,
             hid_ref, gain_ref, mask_in, w_ref, raw, sends, stage, got_soon, tabs, n_buf, x_buf, inv_buf, square, pay, pay_got, mask_own, mask_got, x_got, tp_got, own_col,
             own_row, rel, dx, rs_got, ag_own, ag_got, gn_own, gn_got, raw_sem, tab_sem, in_sem, hop_sem, dp_sem, tp_sem):
        me, at = peers()
        col = lax.axis_index('tp')
        mates = [lax.rem(col + j, N_TP) for j in range(N_TP)]
        my_few = aligned(col * few, few, few)

        def fetch(k):
            d = at[ORDER[k]]
            return pltpu.make_async_copy(tea_ref.at[:, aligned(d * part, part)], raw.at[aligned(d * tokens, tokens, tokens)], raw_sem.at[k])

        def tab_copy(i):
            slot = lax.rem(i, depth)
            return pltpu.make_async_copy(tab_ref.at[aligned(lax.rem(i, tiles) * tile, tile)], tabs.at[slot], tab_sem.at[slot])

        inputs = [pltpu.make_async_copy(src, dst, in_sem.at[2 + i])
                  for i, (src, dst) in enumerate(((hid_hbm, hid_ref), (gain_hbm, gain_ref), (mask_hbm, mask_in)))]
        own_tab = pltpu.make_async_copy(tab_ref.at[aligned(me * part, part)], tab_out, in_sem.at[1])
        for cp in inputs:
            cp.start()
        for k in range(N_DP):
            fetch(k).start()
        for i in range(depth - 1):
            tab_copy(i).start()
        own_tab.start()
        barrier = pltpu.get_barrier_semaphore()
        for dz, dy in ORDER[:-1]:
            pl.semaphore_signal(barrier, inc=1, device_id=(at[dz, dy], col), device_id_type=MESH)
        for j in range(1, N_TP):
            pl.semaphore_signal(barrier, inc=1, device_id=(me, mates[j]), device_id_type=MESH)

        for cp in inputs:
            cp.wait()
        w_ref[...] = 1.0 + jnp.concatenate([gain_ref[i:i + 1] for i in range(dim // LANES)], axis=1)
        hid = hid_ref[...].astype(F32)
        inv = lax.rsqrt(jnp.mean(hid * hid, axis=1, keepdims=True) + NORM_EPS)
        n_buf[...] = hid * inv
        x_buf[...] = (n_buf[...] * w_ref[...]).astype(BF16)
        inv_buf[...] = jnp.broadcast_to(inv, (tokens, LANES))
        pay[...] = n_buf[my_few]
        square[...] = jnp.zeros((LANES, LANES), F32)
        square[0:1, 0:tokens] = mask_in[...]
        mask_own[...] = square[0:few]
        mask_col = jnp.transpose(square[...])[0:tokens, 0:1]
        pl.semaphore_wait(barrier, N_DP + N_TP - 2)

        def remote(src, dst, out, into, dp, tp):
            return pltpu.make_async_remote_copy(src_ref=src, dst_ref=dst, send_sem=out, recv_sem=into, device_id=(dp, tp), device_id_type=MESH)

        def to_dp(src, dst, x, rows=slice(None)):
            def send(o):
                d = at[o]
                return remote(src.at[rows], dst.at[me, rows], dp_sem.at[x, 0, d], dp_sem.at[x, 1, me], d, col)

            def into(o):
                d = at[o]
                return remote(src.at[rows], dst.at[d, rows], dp_sem.at[x, 0, d], dp_sem.at[x, 1, d], d, col)

            return [send(o) for o in ORDER[:-1]], [into(o) for o in ORDER[:-1]]

        def to_tp(srcs, dst, x):
            def send(j):
                c = mates[j]
                return remote(srcs(c), dst.at[col], tp_sem.at[x, 0, c], tp_sem.at[x, 1, col], me, c)

            def into(j):
                c = mates[j]
                return remote(srcs(c), dst.at[c], tp_sem.at[x, 0, c], tp_sem.at[x, 1, c], me, c)

            return [send(j) for j in range(1, N_TP)], [into(j) for j in range(1, N_TP)]

        def start(copies):
            for cp in copies:
                cp.start()

        def arrive(copies):
            for cp in copies:
                cp.wait_recv()

        def added(ref, here=slice(None)):
            total = ref[0, here]
            for d in range(1, ref.shape[0]):
                total = total + ref[d, here]
            return total

        gots = (got_soon, got_late)
        late = part // 2

        def hop(j, level, w):
            kind, (dz, dy) = JOBS[j]
            tok = pl.ds(kind * half, half)
            rows = slice(None) if w is None else pl.ds(w * late, late)
            src = stage.at[MIDDLE.index((j, level - 1)), :, rows] if level else sends.at[aligned(at[dz, dy] * tokens + kind * half, half, half), rows]
            dst = stage.at[MIDDLE.index((j, level)), :, rows] if (j, level) in MIDDLE else gots[w].at[dz * SIDE + dy, tok]
            k = COPIES.index((j, level, w))
            return remote(src, dst, hop_sem.at[0, k], hop_sem.at[1, k], at[PATHS[j][level]], col)

        def came(level, w=None):
            for j, at in MIDDLE:
                if at == level:
                    hop(j, level, w).wait_recv()

        def onward(level, far, *ws):
            for w in ws:
                for j, at in MIDDLE:
                    if at == level - 1 and far == (len(PATHS[j]) > 2):
                        hop(j, level, w).start()

        pay_sends, pay_came = to_dp(pay, pay_got, 0)
        start(pay_sends)
        pay_got[me] = pay[...]
        mask_sends, mask_came = to_dp(mask_own, mask_got, 1, pl.ds(0, 1))
        start(mask_sends)
        mask_got[me] = mask_own[...]

        for k, o in enumerate(ORDER):
            fetch(k).wait()
            d = at[o]

            def weigh(r, _):
                here = aligned(d * tokens + r * pack, pack, pack)
                cap = jnp.tanh(raw[here].astype(F32) * INV_CAP)
                sends[here] = jnp.exp(SOFT_CAP * cap - SOFT_CAP)
                return 0

            lax.fori_loop(0, tokens // pack, weigh, 0)
            for j, (_, to) in enumerate(JOBS):
                if to == o:
                    for w in waves(j, 0):
                        hop(j, 0, w).start()

        def keep(r, _):
            here, there = aligned(me * tokens + r * pack, pack, pack), aligned(r * pack, pack, pack)
            got_soon[0, there] = sends[here, :late]
            got_late[0, there] = sends[here, late:]
            return 0

        lax.fori_loop(0, tokens // pack, keep, 0)

        def fold(v):
            total = v[:, :LANES]
            for c in range(LANES, v.shape[1], LANES):
                total = total + v[:, c:c + LANES]
            return total

        def student(slot, here):
            z = lax.dot_general(x_buf[...], tabs[slot, here], ROWS_BY_ROWS, preferred_element_type=F32)
            ratio = jnp.tanh(z * INV_CAP)
            return ratio, jnp.exp(SOFT_CAP * ratio - SOFT_CAP)

        def forward(i, sums):
            slot = lax.rem(i, depth)
            tab_copy(i).wait()
            tab_copy(i + depth - 1).start()
            s_sum, t_sum, k_sum = sums
            for c in range(0, tile, sub):
                ratio, stu = student(slot, pl.ds(c, sub))
                toks, here = aligned(lax.div(i, 2) * tokens, tokens, tokens), aligned(lax.rem(i, 2) * tile + c, sub)
                cap = jnp.tanh(raw[toks, here].astype(F32) * INV_CAP)
                tea = sends[toks, here]
                s_sum = s_sum + fold(stu)
                t_sum = t_sum + fold(tea)
                k_sum = k_sum + fold(tea * (cap - ratio))
            return s_sum, t_sum, k_sum

        zero = jnp.zeros((tokens, LANES), F32)
        s_sum, t_sum, k_sum = lax.fori_loop(0, tiles, forward, (zero, zero, zero))
        lane = lax.broadcasted_iota(jnp.int32, (tokens, LANES), 1)
        sums = jnp.where(lane == 0, jnp.sum(s_sum, axis=1, keepdims=True), 0.0)
        sums = jnp.where(lane == 1, jnp.sum(t_sum, axis=1, keepdims=True), sums)
        sums = jnp.where(lane == AWAY, SOFT_CAP * jnp.sum(k_sum, axis=1, keepdims=True), sums)
        own_col[...] = sums
        tp_got[col] = sums
        tp_sends, tp_came = to_tp(lambda c: own_col, tp_got, 0)
        start(tp_sends)
        arrive(tp_came)
        total = added(tp_got)
        square[0:tokens] = jnp.where(lane == DOWN, mask_col, total)
        line = jnp.transpose(square[...])[0:few]
        own_row[...] = line
        all_ref[me] = line
        dp_sends, dp_came = to_dp(own_row, all_ref, 2)
        start(dp_sends)
        came(0)
        onward(1, True, None)
        onward(1, False, 0, 1)

        arrive((*pay_came, *mask_came))
        x_got[col] = pay_got[...]
        xt_sends, xt_came = to_tp(lambda c: pay_got, x_got, 1)
        start(xt_sends)
        count = jnp.sum(added(mask_got, slice(1)), axis=1, keepdims=True)
        inv_s, inv_t, weight = 1.0 / total[:, 0:1], 1.0 / total[:, 1:2], mask_col / count
        dx[...] = jnp.zeros((tokens, dim), F32)

        def backward(i, _):
            slot = lax.rem(i, depth)
            tab_copy(i).wait()

            @pl.when(i + depth - 1 < 2 * tiles)
            def _():
                tab_copy(i + depth - 1).start()

            for c in range(0, tile, sub):
                here = pl.ds(c, sub)
                ratio, stu = student(slot, here)
                tea = sends[aligned(lax.div(i - tiles, 2) * tokens, tokens, tokens), aligned(lax.rem(i, 2) * tile + c, sub)]
                diff = (stu * inv_s - tea * inv_t) * weight
                g = (diff * (1.0 - ratio * ratio)).astype(BF16)
                dx[...] += jnp.dot(g, tabs[slot, here], preferred_element_type=F32)
            return 0

        lax.fori_loop(tiles, 2 * tiles, backward, 0)
        came(1)
        onward(2, True, 0)

        rs_got[col] = dx[my_few]
        rs_sends, rs_came = to_tp(lambda c: dx.at[aligned(c * few, few, few)], rs_got, 2)
        start(rs_sends)
        arrive(rs_came)
        my_x = added(rs_got)
        my_n = n_buf[my_few]
        grad_n = my_x * w_ref[...]
        my_h = inv_buf[my_few, 0:1] * (grad_n - my_n * jnp.mean(grad_n * my_n, axis=1, keepdims=True))
        ag_own[...] = jnp.zeros((2 * few, dim), F32)
        ag_own[0:few] = my_h
        ag_own[few:few + 1] = jnp.sum(my_x * my_n, axis=0, keepdims=True)
        ag_got[col] = ag_own[...]
        ag_sends, ag_came = to_tp(lambda c: ag_own, ag_got, DOWN)
        start(ag_sends)
        arrive(ag_came)
        gh_ref[...] = jnp.concatenate([ag_got[j, 0:few] for j in range(N_TP)], axis=0)
        line = added(ag_got, slice(few, few + 1))
        gn_own[0:1] = line
        gn_got[me, 0:1] = line
        gn_sends, gn_came = to_dp(gn_own, gn_got, DOWN, pl.ds(0, 1))
        start(gn_sends)

        arrive(xt_came)

        def widen(d, _):
            rows = jnp.concatenate([x_got[j, d] for j in range(N_TP)], axis=0)
            x_out[aligned(d * tokens, tokens, tokens)] = (rows * w_ref[...]).astype(BF16)
            return 0

        lax.fori_loop(0, N_DP, widen, 0)
        arrive(dp_came)
        row = lax.broadcasted_iota(jnp.int32, (few, LANES), 0)
        lanes = lax.broadcasted_iota(jnp.int32, (few, LANES), 1)
        for d in range(N_DP):
            block = all_ref[d]
            safe = jnp.where((row < AWAY) & (lanes < tokens), block, 1.0)
            rel[d * few:(d + 1) * few] = jnp.where(row < AWAY, 1.0 / safe, block / count)
        for k, (dz, dy) in enumerate(OFFSETS):
            square[k * few:(k + 1) * few] = rel[aligned(at[-dz, -dy] * few, few, few)]
        coef_ref[...] = jnp.transpose(square[...])

        arrive(gn_came)
        gg_ref[...] = added(gn_got, slice(1))
        own_tab.wait()
        came(2, 0)
        onward(DOWN, True, 0)
        onward(2, True, 1)
        for j, path in enumerate(PATHS):
            hop(j, len(path) - 1, 0).wait_recv()
        for j, level, w in COPIES:
            if level == 0:
                hop(j, level, w).wait_send()
        came(2, 1)
        onward(DOWN, True, 1)

        def block(b, _):
            grad_block(at, got_soon, x_out, tab_out[aligned(b * sub, sub)], coef_ref, sends, raw, blocks_ref, b)
            return 0

        lax.fori_loop(0, 2, block, 0)
        for j, path in enumerate(PATHS):
            hop(j, len(path) - 1, 1).wait_recv()
        for j, level, w in COPIES:
            if level:
                hop(j, level, w).wait_send()
        for cp in (*pay_sends, *mask_sends, *tp_sends, *dp_sends, *xt_sends, *rs_sends, *ag_sends, *gn_sends):
            cp.wait_send()

    dma = pltpu.SemaphoreType.DMA
    wide, flat = (tokens, dim), (few, LANES)
    return pl.pallas_call(
        kern,
        out_shape=tuple(jax.ShapeDtypeStruct(shape, kind) for shape, kind in (
            ((N_DP, tokens, part // 2), F32), ((2, sub, dim), F32), ((N_DP * tokens, dim), BF16), ((part, dim), BF16), ((LANES, LANES), F32), ((N_DP, *flat), F32), (wide, F32),
            ((1, dim), F32))),
        in_specs=[HB] * 5, out_specs=(VM,) * 8,
        scratch_shapes=[pltpu.VMEM(shape, kind) for shape, kind in (
            (wide, BF16), ((dim // LANES, LANES), F32), ((1, tokens), F32), ((1, dim), F32), ((N_DP * tokens, part), BF16), ((N_DP * tokens, part), F32),
            ((len(MIDDLE), half, part), F32), ((N_DP, tokens, part // 2), F32),
            ((depth, tile, dim), BF16), (wide, F32), (wide, BF16), ((tokens, LANES), F32), ((LANES, LANES), F32), ((few, dim), F32),
            ((N_DP, few, dim), F32), (flat, F32), ((N_DP, *flat), F32), ((N_TP, N_DP, few, dim), F32), ((N_TP, tokens, LANES), F32),
            ((tokens, LANES), F32), (flat, F32), ((LANES, LANES), F32), (wide, F32), ((N_TP, few, dim), F32), ((2 * few, dim), F32),
            ((N_TP, 2 * few, dim), F32), ((few, dim), F32), ((N_DP, few, dim), F32))] + [
            dma((N_DP,)), dma((depth,)), dma((5,)), dma((2, len(COPIES))), dma((SIDE, 2, N_DP)), dma((SIDE, 2, N_TP))],
        compiler_params=pltpu.CompilerParams(collective_id=0, has_side_effects=True, vmem_limit_bytes=L_FRONT * MIB),
        cost_estimate=pl.CostEstimate(flops=3 * 10 ** 9, bytes_accessed=100 * MIB, transcendentals=0), name='front')(
            *(pltpu.with_memory_space_constraint(a, pltpu.HBM) for a in (hidden, gain_row, mask_row, teacher, table)))


def finish(teas, x_all, tab_part, coef):
    n, tokens, late = teas.shape
    dim = x_all.shape[1]
    span = late // 2

    def kern(tea_ref, x_ref, tab_ref, coef_ref, out_ref, z_buf, g_buf):
        at = peers()[1]

        def block(b, _):
            grad_block(at, tea_ref, x_ref, tab_ref[aligned(late + b * span, span)], coef_ref, z_buf, g_buf, out_ref, b)
            return 0

        lax.fori_loop(0, 2, block, 0)

    return pl.pallas_call(kern, out_shape=jax.ShapeDtypeStruct((2, span, dim), F32), in_specs=[VM] * 4, out_specs=VM,
        scratch_shapes=[pltpu.VMEM((n * tokens, span), F32), pltpu.VMEM((n * tokens, span), BF16)], name='finish',
        compiler_params=pltpu.CompilerParams(vmem_limit_bytes=22 * MIB),
        cost_estimate=pl.CostEstimate(flops=10 ** 9, bytes_accessed=8 * MIB, transcendentals=0))(teas, x_all, tab_part, coef)


def place(table, pieces, vocab):
    arrays = [p[0] for p in pieces]
    n = len(arrays)
    dim = arrays[0].shape[1]
    rows = vocab // N_DP
    quarter = rows // SIDE
    cut = 256
    chunks = [(i, r) for i in range(n) for r in range(0, arrays[i].shape[0], cut)]

    def kern(*refs):
        dst, buf, sem = refs[-DOWN:]
        at = peers()[1]
        reads, writes = [], []
        for k, (i, r) in enumerate(chunks):
            _, dz, dy, kind, half = pieces[i]
            first = (2 * (half + r // quarter) + kind) * quarter + r % quarter
            there = aligned(at[dz, dy] * rows + first, cut, cut)
            reads.append(pltpu.make_async_copy(refs[i].at[pl.ds(r, cut)], buf.at[k], sem.at[0, k]))
            writes.append(pltpu.make_async_copy(buf.at[k], dst.at[there], sem.at[1, k]))
        for cp in reads:
            cp.start()
        for read, write in zip(reads, writes):
            read.wait()
            write.start()
        for cp in writes:
            cp.wait()

    args = arrays if table is None else [*arrays, table]
    size = len(chunks) * cut * dim
    return pl.pallas_call(kern, out_shape=jax.ShapeDtypeStruct((vocab, dim), F32), in_specs=[pl.BlockSpec(memory_space=pl.ANY)] * n + [HB] * (len(args) - n),
        out_specs=HB, scratch_shapes=[pltpu.VMEM((len(chunks), cut, dim), F32), pltpu.SemaphoreType.DMA((2, len(chunks)))],
        input_output_aliases={} if table is None else {n: 0}, name='place', compiler_params=pltpu.CompilerParams(vmem_limit_bytes=4 * size + MIB),
        cost_estimate=pl.CostEstimate(flops=10 * MIB, bytes_accessed=8 * size, transcendentals=0))(*args)


def gather(first, rest, vocab):
    quarter = first[0].shape[0]
    sets, ways = range(2), (UP, DOWN)
    table, event = None, 0

    def send(pair, axis, step):
        out = []
        for k in sets:
            dz, dy = (step, 0) if axis == k else (0, step)
            out.append(lax.ppermute(pair[k], 'dp', [(d, shift(d, dz, dy)) for d in range(N_DP)]))
        return out

    def put(pair, a, b, c=0):
        return [(pair[k], *((b, a) if k else (a, b)), k, c) for k in sets]

    def settle(*pieces):
        nonlocal table
        table = place(table, [p for ps in pieces for p in ps], vocab)

    def wait(*pairs):
        nonlocal table, event
        event += 1
        table, *flat = lax.optimization_barrier((table, *(x for pair in pairs for x in pair)))
        return [flat[2 * i:2 * i + 2] for i in range(len(pairs))]

    def join(one, other):
        return [jnp.concatenate(pair) for pair in zip(one, other)]

    own = [first]
    low, high = ([send(own[0], 0, way)] for way in ways)
    later = rest()
    event = 1
    own.append([later[k] for k in sets])
    low.append(send(own[1], 0, UP))
    high.append(send(own[1], 0, DOWN))
    whole = join(*own)
    side = {way: send(whole, 1, way) for way in ways}
    settle(put(own[0], 0, 0, 0), put(own[1], 0, 0, 1))

    low[0], high[0] = wait(low[0], high[0])
    far_low = send(low[0], 0, UP)
    settle(put(low[0], DOWN, 0, 0), put(high[0], UP, 0, 0))

    low[1], high[1] = wait(low[1], high[1])
    far_high = send(high[1], 0, DOWN)
    low_whole, high_whole = join(*low), join(*high)
    low_side = {way: send(low_whole, 1, way) for way in ways}
    settle(put(low[1], DOWN, 0, 1), put(high[1], UP, 0, 1))

    side[UP], side[DOWN], high_whole = wait(side[UP], side[DOWN], high_whole)
    high_side = {way: send(high_whole, 1, way) for way in ways}
    side_far = send(side[UP], 1, UP)
    settle(put(side[UP], 0, DOWN))
    settle(put(side[DOWN], 0, UP))

    far_low, far_high = wait(far_low, far_high)
    far_side = {(c, way): send(pair, 1, way) for way in ways for c, pair in enumerate((far_low, far_high))}
    settle(put(far_low, AWAY, 0, 0), put(far_high, AWAY, 0, 1))

    low_side[UP], low_side[DOWN] = wait(low_side[UP], low_side[DOWN])
    low_far = send(low_side[DOWN], 1, DOWN)
    settle(put(low_side[UP], DOWN, DOWN))
    settle(put(low_side[DOWN], DOWN, UP))

    high_side[UP], high_side[DOWN] = wait(high_side[UP], high_side[DOWN])
    high_far = [send([x[:quarter] for x in high_side[UP]], 1, UP), send([x[quarter:] for x in high_side[DOWN]], 1, DOWN)]
    settle(put(high_side[UP], UP, DOWN))
    settle(put(high_side[DOWN], UP, UP))

    far_side[0, DOWN], far_side[1, DOWN], side_far = wait(far_side[0, DOWN], far_side[1, DOWN], side_far)
    last_down = send(far_side[1, DOWN], 1, DOWN)
    settle(put(far_side[0, DOWN], AWAY, UP, 0), put(far_side[1, DOWN], AWAY, UP, 1))
    settle(put(side_far, 0, AWAY))

    far_side[0, UP], = wait(far_side[0, UP])
    last_up = send(far_side[0, UP], 1, UP)
    settle(put(far_side[0, UP], AWAY, DOWN, 0))

    far_side[1, UP], low_far = wait(far_side[1, UP], low_far)
    settle(put(far_side[1, UP], AWAY, DOWN, 1))
    settle(put(low_far, DOWN, AWAY))

    high_far = wait(*high_far)
    settle(put(high_far[0], UP, AWAY, 0), put(high_far[1], UP, AWAY, 1))
    for k in (1, 0):
        table, up, down = lax.optimization_barrier((table, last_up[k], last_down[k]))
        table = place(table, [put([up] * 2, AWAY, AWAY, 0)[k], put([down] * 2, AWAY, AWAY, 1)[k]], vocab)
    return table


def solution(mesh):
    def local_step(hid_rows, w_final, tab_rows, tea_rows, mask_rows):
        tokens = hid_rows.shape[0]
        late, soon, x_all, tab_part, coef, stats, grad_h, gain_line = front(hid_rows, w_final.reshape(-1, LANES), mask_rows[None], tea_rows, tab_rows)
        coef, *first = lax.optimization_barrier((coef, soon[0], soon[1]))
        table = gather(first, lambda: finish(late, x_all, tab_part, coef), tab_rows.shape[0])
        s_sum, t_sum, k_sum, masks = (stats[:, i, :tokens] for i in range(SIDE))
        all_kl = k_sum / t_sum + jnp.log(s_sum) - jnp.log(t_sum)
        loss_val = jnp.sum(masks * all_kl) / jnp.sum(masks)
        return loss_val, grad_h.astype(BF16), gain_line[0], table

    return jax.shard_map(local_step, mesh=mesh, in_specs=(P('dp', None), P(None), P('tp', None), P('dp', 'tp'), P('dp')), out_specs=(P(), P('dp', None), P(None), P('tp', None)), check_vma=False)
```

```python
import jax
import jax.numpy as jnp
from jax import lax
from jax.experimental import pallas as pl
from jax.experimental.pallas import tpu as pltpu
from jax.sharding import PartitionSpec as P


SOFT_CAP = 30.0
INV_CAP = 1.0 / SOFT_CAP
NORM_EPS = 1e-6
SIDE, N_DP, N_TP, LANES = 4, 16, 8, 128
UP, DOWN, AWAY = 1, 3, 2
MIB = 2 ** 20
L_FRONT = 41
MESH = pl.DeviceIdType.MESH
VM = pl.BlockSpec(memory_space=pltpu.VMEM)
HB = pl.BlockSpec(memory_space=pltpu.HBM)
F32, BF16 = jnp.float32, jnp.bfloat16
ROWS_BY_ROWS = (((1,), (1,)), ((), ()))
COLS_BY_COLS = (((0,), (0,)), ((), ()))

OFFSETS = tuple((dz, dy) for dz in range(SIDE) for dy in range(SIDE))
ORDER = tuple(sorted(OFFSETS, key=lambda o: -sum(min(d, SIDE - d) for d in o)))


def shift(dp, dz, dy):
    return (dp // SIDE + dz + SIDE) % SIDE * SIDE + (dp % SIDE + dy + SIDE) % SIDE


def peers():
    me = lax.axis_index('dp')
    z, y = lax.div(me, SIDE), lax.rem(me, SIDE)
    zs = [lax.rem(z + d, SIDE) * SIDE for d in range(SIDE)]
    ys = [lax.rem(y + d, SIDE) for d in range(SIDE)]
    return me, {(dz, dy): zs[dz] + ys[dy] for dz in range(-DOWN, SIDE) for dy in range(-DOWN, SIDE)}


def aligned(start, size, unit=LANES):
    return pl.ds(pl.multiple_of(start, unit), size)


def hops(kind, dz, dy):
    along_z = [(dz, 0)] if dz % 2 else [(UP if dy < AWAY else DOWN, 0)] * dz
    along_y = [(0, dy)] if dy % 2 else [(0, UP if dz < AWAY else DOWN)] * dy
    return along_y + along_z if kind else along_z + along_y


JOBS = tuple((kind, o) for o in ORDER[:-1] for kind in range(2))
PATHS = tuple(hops(kind, *o) for kind, o in JOBS)
MIDDLE = tuple((j, level) for level in range(SIDE) for j, path in enumerate(PATHS) if len(path) > level + 1)


def waves(j, level):
    return (None,) if (j, level) in MIDDLE and level < 2 else (0, 1)


COPIES = tuple((j, level, w) for j, path in enumerate(PATHS) for level in range(len(path)) for w in waves(j, level))


def grad_block(at, tea_ref, x_ref, tab_rows, coef_ref, z_buf, g_buf, out_ref, block):
    tokens = tea_ref.shape[1]
    span = tab_rows.shape[0]
    few = LANES // N_DP
    cols = aligned(block * span, span)
    z_buf[:, :span] = lax.dot_general(x_ref[...], tab_rows, ROWS_BY_ROWS, preferred_element_type=F32)
    for k, (dz, dy) in enumerate(OFFSETS):
        here = aligned(at[-dz, -dy] * tokens, tokens, tokens)
        ratio = jnp.tanh(z_buf[here, :span] * INV_CAP)
        stu = jnp.exp(SOFT_CAP * ratio - SOFT_CAP)
        inv_s, inv_t, _, weight = (coef_ref[0:tokens, k * few + i:k * few + i + 1] for i in range(SIDE))
        diff = (stu * inv_s - tea_ref[k, :, cols] * inv_t) * weight
        g_buf[here, :span] = (diff * (1.0 - ratio * ratio)).astype(BF16)
    out_ref[block] = lax.dot_general(g_buf[:, :span], x_ref[...], COLS_BY_COLS, preferred_element_type=F32)


def front(hidden, gain_row, mask_row, teacher, table):
    tokens, vocab = teacher.shape
    dim = hidden.shape[1]
    part = vocab // N_DP
    half = tokens // 2
    few = tokens // N_TP
    pack = 16
    sub = 512
    per = part // sub
    tiles = vocab // sub
    depth = 6

    def kern(hid_hbm, gain_hbm, mask_hbm, tea_ref, tab_ref, got_late, blocks_ref, x_out, tab_out, coef_ref, all_ref, gh_ref, gg_ref,
             hid_ref, gain_ref, mask_in, w_ref, raw, sends, stage, got_soon, tabs, n_buf, x_buf, inv_buf, square, pay, pay_got, mask_own, mask_got, x_got, tp_got, own_col,
             own_row, rel, dx, rs_got, ag_own, ag_got, gn_own, gn_got, raw_sem, tab_sem, in_sem, hop_sem, dp_sem, tp_sem):
        me, at = peers()
        col = lax.axis_index('tp')
        mates = [lax.rem(col + j, N_TP) for j in range(N_TP)]
        my_few = aligned(col * few, few, few)

        def fetch(k):
            d = at[ORDER[k]]
            return pltpu.make_async_copy(tea_ref.at[:, aligned(d * part, part)], raw.at[aligned(d * tokens, tokens, tokens)], raw_sem.at[k])

        def tab_copy(i):
            slot = lax.rem(i, depth)
            return pltpu.make_async_copy(tab_ref.at[aligned(lax.rem(i, tiles) * sub, sub)], tabs.at[slot], tab_sem.at[slot])

        inputs = [pltpu.make_async_copy(src, dst, in_sem.at[2 + i])
                  for i, (src, dst) in enumerate(((hid_hbm, hid_ref), (gain_hbm, gain_ref), (mask_hbm, mask_in)))]
        own_tab = pltpu.make_async_copy(tab_ref.at[aligned(me * part, part)], tab_out, in_sem.at[1])
        for cp in inputs:
            cp.start()
        for k in range(N_DP):
            fetch(k).start()
        for i in range(depth - 1):
            tab_copy(i).start()
        own_tab.start()
        barrier = pltpu.get_barrier_semaphore()
        for dz, dy in ORDER[:-1]:
            pl.semaphore_signal(barrier, inc=1, device_id=(at[dz, dy], col), device_id_type=MESH)
        for j in range(1, N_TP):
            pl.semaphore_signal(barrier, inc=1, device_id=(me, mates[j]), device_id_type=MESH)

        for cp in inputs:
            cp.wait()
        w_ref[...] = 1.0 + jnp.concatenate([gain_ref[i:i + 1] for i in range(dim // LANES)], axis=1)
        hid = hid_ref[...].astype(F32)
        inv = lax.rsqrt(jnp.mean(hid * hid, axis=1, keepdims=True) + NORM_EPS)
        n_buf[...] = hid * inv
        x_buf[...] = (n_buf[...] * w_ref[...]).astype(BF16)
        inv_buf[...] = jnp.broadcast_to(inv, (tokens, LANES))
        pay[...] = n_buf[my_few]
        square[...] = jnp.zeros((LANES, LANES), F32)
        square[0:1, 0:tokens] = mask_in[...]
        mask_own[...] = square[0:few]
        mask_col = jnp.transpose(square[...])[0:tokens, 0:1]

        def weigh(k):
            fetch(k).wait()
            d = at[ORDER[k]]

            def rows(r, _):
                here = aligned(d * tokens + r * pack, pack, pack)
                cap = jnp.tanh(raw[here].astype(F32) * INV_CAP)
                sends[here] = jnp.exp(SOFT_CAP * cap - SOFT_CAP)
                return 0

            lax.fori_loop(0, tokens // pack, rows, 0)

        weigh(0)
        weigh(1)
        pl.semaphore_wait(barrier, N_DP + N_TP - 2)

        def remote(src, dst, out, into, dp, tp):
            return pltpu.make_async_remote_copy(src_ref=src, dst_ref=dst, send_sem=out, recv_sem=into, device_id=(dp, tp), device_id_type=MESH)

        def to_dp(src, dst, x, rows=slice(None)):
            def send(o):
                d = at[o]
                return remote(src.at[rows], dst.at[me, rows], dp_sem.at[x, 0, d], dp_sem.at[x, 1, me], d, col)

            def into(o):
                d = at[o]
                return remote(src.at[rows], dst.at[d, rows], dp_sem.at[x, 0, d], dp_sem.at[x, 1, d], d, col)

            return [send(o) for o in ORDER[:-1]], [into(o) for o in ORDER[:-1]]

        def to_tp(srcs, dst, x):
            def send(j):
                c = mates[j]
                return remote(srcs(c), dst.at[col], tp_sem.at[x, 0, c], tp_sem.at[x, 1, col], me, c)

            def into(j):
                c = mates[j]
                return remote(srcs(c), dst.at[c], tp_sem.at[x, 0, c], tp_sem.at[x, 1, c], me, c)

            return [send(j) for j in range(1, N_TP)], [into(j) for j in range(1, N_TP)]

        def start(copies):
            for cp in copies:
                cp.start()

        def arrive(copies):
            for cp in copies:
                cp.wait_recv()

        def added(ref, here=slice(None)):
            total = ref[0, here]
            for d in range(1, ref.shape[0]):
                total = total + ref[d, here]
            return total

        gots = (got_soon, got_late)
        late = part // 2

        def hop(j, level, w):
            kind, (dz, dy) = JOBS[j]
            tok = pl.ds(kind * half, half)
            rows = slice(None) if w is None else pl.ds(w * late, late)
            src = stage.at[MIDDLE.index((j, level - 1)), :, rows] if level else sends.at[aligned(at[dz, dy] * tokens + kind * half, half, half), rows]
            dst = stage.at[MIDDLE.index((j, level)), :, rows] if (j, level) in MIDDLE else gots[w].at[dz * SIDE + dy, tok]
            k = COPIES.index((j, level, w))
            return remote(src, dst, hop_sem.at[0, k], hop_sem.at[1, k], at[PATHS[j][level]], col)

        def came(level, w=None):
            for j, at in MIDDLE:
                if at == level:
                    hop(j, level, w).wait_recv()

        def onward(level, far, *ws):
            for w in ws:
                for j, at in MIDDLE:
                    if at == level - 1 and far == (len(PATHS[j]) > 2):
                        hop(j, level, w).start()

        pay_sends, pay_came = to_dp(pay, pay_got, 0)
        start(pay_sends)
        pay_got[me] = pay[...]
        mask_sends, mask_came = to_dp(mask_own, mask_got, 1, pl.ds(0, 1))
        start(mask_sends)
        mask_got[me] = mask_own[...]

        for k, o in enumerate(ORDER):
            if k > 1:
                weigh(k)
            for j, (_, to) in enumerate(JOBS):
                if to == o:
                    for w in waves(j, 0):
                        hop(j, 0, w).start()

        def keep(r, _):
            here, there = aligned(me * tokens + r * pack, pack, pack), aligned(r * pack, pack, pack)
            got_soon[0, there] = sends[here, :late]
            got_late[0, there] = sends[here, late:]
            return 0

        lax.fori_loop(0, tokens // pack, keep, 0)

        def fold(v):
            total = v[:, :LANES]
            for c in range(LANES, v.shape[1], LANES):
                total = total + v[:, c:c + LANES]
            return total

        def student(slot):
            z = lax.dot_general(x_buf[...], tabs[slot], ROWS_BY_ROWS, preferred_element_type=F32)
            ratio = jnp.tanh(z * INV_CAP)
            return ratio, jnp.exp(SOFT_CAP * ratio - SOFT_CAP)

        def forward(i, sums):
            slot = lax.rem(i, depth)
            tab_copy(i).wait()
            tab_copy(i + depth - 1).start()
            s_sum, t_sum, k_sum = sums
            ratio, stu = student(slot)
            toks, here = aligned(lax.div(i, per) * tokens, tokens, tokens), aligned(lax.rem(i, per) * sub, sub)
            cap = jnp.tanh(raw[toks, here].astype(F32) * INV_CAP)
            tea = sends[toks, here]
            return s_sum + fold(stu), t_sum + fold(tea), k_sum + fold(tea * (cap - ratio))

        zero = jnp.zeros((tokens, LANES), F32)
        s_sum, t_sum, k_sum = lax.fori_loop(0, tiles, forward, (zero, zero, zero))
        lane = lax.broadcasted_iota(jnp.int32, (tokens, LANES), 1)
        sums = jnp.where(lane == 0, jnp.sum(s_sum, axis=1, keepdims=True), 0.0)
        sums = jnp.where(lane == 1, jnp.sum(t_sum, axis=1, keepdims=True), sums)
        sums = jnp.where(lane == AWAY, SOFT_CAP * jnp.sum(k_sum, axis=1, keepdims=True), sums)
        own_col[...] = sums
        tp_got[col] = sums
        tp_sends, tp_came = to_tp(lambda c: own_col, tp_got, 0)
        start(tp_sends)
        arrive(tp_came)
        total = added(tp_got)
        square[0:tokens] = jnp.where(lane == DOWN, mask_col, total)
        line = jnp.transpose(square[...])[0:few]
        own_row[...] = line
        all_ref[me] = line
        dp_sends, dp_came = to_dp(own_row, all_ref, 2)
        start(dp_sends)
        came(0)
        onward(1, True, None)
        onward(1, False, 0)

        arrive((*pay_came, *mask_came))
        x_got[col] = pay_got[...]
        xt_sends, xt_came = to_tp(lambda c: pay_got, x_got, 1)
        start(xt_sends)
        count = jnp.sum(added(mask_got, slice(1)), axis=1, keepdims=True)
        inv_s, inv_t, weight = 1.0 / total[:, 0:1], 1.0 / total[:, 1:2], mask_col / count
        dx[...] = jnp.zeros((tokens, dim), F32)

        def backward(i, _):
            slot = lax.rem(i, depth)
            tab_copy(i).wait()

            @pl.when(i + depth - 1 < 2 * tiles)
            def _():
                tab_copy(i + depth - 1).start()

            ratio, stu = student(slot)
            tea = sends[aligned(lax.div(i - tiles, per) * tokens, tokens, tokens), aligned(lax.rem(i, per) * sub, sub)]
            diff = (stu * inv_s - tea * inv_t) * weight
            g = (diff * (1.0 - ratio * ratio)).astype(BF16)
            dx[...] += jnp.dot(g, tabs[slot], preferred_element_type=F32)
            return 0

        lax.fori_loop(tiles, 2 * tiles, backward, 0)
        came(1)
        onward(2, True, 0)

        rs_got[col] = dx[my_few]
        rs_sends, rs_came = to_tp(lambda c: dx.at[aligned(c * few, few, few)], rs_got, 2)
        start(rs_sends)
        arrive(rs_came)
        my_x = added(rs_got)
        my_n = n_buf[my_few]
        grad_n = my_x * w_ref[...]
        my_h = inv_buf[my_few, 0:1] * (grad_n - my_n * jnp.mean(grad_n * my_n, axis=1, keepdims=True))
        ag_own[...] = jnp.zeros((2 * few, dim), F32)
        ag_own[0:few] = my_h
        ag_own[few:few + 1] = jnp.sum(my_x * my_n, axis=0, keepdims=True)
        ag_got[col] = ag_own[...]
        ag_sends, ag_came = to_tp(lambda c: ag_own, ag_got, DOWN)
        start(ag_sends)
        arrive(ag_came)
        gh_ref[...] = jnp.concatenate([ag_got[j, 0:few] for j in range(N_TP)], axis=0)
        line = added(ag_got, slice(few, few + 1))
        gn_own[0:1] = line
        gn_got[me, 0:1] = line
        gn_sends, gn_came = to_dp(gn_own, gn_got, DOWN, pl.ds(0, 1))
        start(gn_sends)

        came(2, 0)
        onward(DOWN, True, 0)
        onward(2, True, 1)
        onward(1, False, 1)
        arrive(xt_came)

        def widen(d, _):
            rows = jnp.concatenate([x_got[j, d] for j in range(N_TP)], axis=0)
            x_out[aligned(d * tokens, tokens, tokens)] = (rows * w_ref[...]).astype(BF16)
            return 0

        lax.fori_loop(0, N_DP, widen, 0)
        arrive(dp_came)
        row = lax.broadcasted_iota(jnp.int32, (few, LANES), 0)
        lanes = lax.broadcasted_iota(jnp.int32, (few, LANES), 1)
        for d in range(N_DP):
            block = all_ref[d]
            safe = jnp.where((row < AWAY) & (lanes < tokens), block, 1.0)
            rel[d * few:(d + 1) * few] = jnp.where(row < AWAY, 1.0 / safe, block / count)
        for k, (dz, dy) in enumerate(OFFSETS):
            square[k * few:(k + 1) * few] = rel[aligned(at[-dz, -dy] * few, few, few)]
        coef_ref[...] = jnp.transpose(square[...])

        own_tab.wait()
        for j, path in enumerate(PATHS):
            hop(j, len(path) - 1, 0).wait_recv()
        for j, level, w in COPIES:
            if level == 0:
                hop(j, level, w).wait_send()

        def block(b, _):
            @pl.when(b == 1)
            def _():
                came(2, 1)
                onward(DOWN, True, 1)

            grad_block(at, got_soon, x_out, tab_out[aligned(b * sub, sub)], coef_ref, sends, raw, blocks_ref, b)
            return 0

        lax.fori_loop(0, 2, block, 0)
        arrive(gn_came)
        gg_ref[...] = added(gn_got, slice(1))
        for j, path in enumerate(PATHS):
            hop(j, len(path) - 1, 1).wait_recv()
        for j, level, w in COPIES:
            if level:
                hop(j, level, w).wait_send()
        for cp in (*pay_sends, *mask_sends, *tp_sends, *dp_sends, *xt_sends, *rs_sends, *ag_sends, *gn_sends):
            cp.wait_send()

    dma = pltpu.SemaphoreType.DMA
    wide, flat = (tokens, dim), (few, LANES)
    return pl.pallas_call(
        kern,
        out_shape=tuple(jax.ShapeDtypeStruct(shape, kind) for shape, kind in (
            ((N_DP, tokens, part // 2), F32), ((2, sub, dim), F32), ((N_DP * tokens, dim), BF16), ((part, dim), BF16), ((LANES, LANES), F32), ((N_DP, *flat), F32), (wide, F32),
            ((1, dim), F32))),
        in_specs=[HB] * 5, out_specs=(VM,) * 8,
        scratch_shapes=[pltpu.VMEM(shape, kind) for shape, kind in (
            (wide, BF16), ((dim // LANES, LANES), F32), ((1, tokens), F32), ((1, dim), F32), ((N_DP * tokens, part), BF16), ((N_DP * tokens, part), F32),
            ((len(MIDDLE), half, part), F32), ((N_DP, tokens, part // 2), F32),
            ((depth, sub, dim), BF16), (wide, F32), (wide, BF16), ((tokens, LANES), F32), ((LANES, LANES), F32), ((few, dim), F32),
            ((N_DP, few, dim), F32), (flat, F32), ((N_DP, *flat), F32), ((N_TP, N_DP, few, dim), F32), ((N_TP, tokens, LANES), F32),
            ((tokens, LANES), F32), (flat, F32), ((LANES, LANES), F32), (wide, F32), ((N_TP, few, dim), F32), ((2 * few, dim), F32),
            ((N_TP, 2 * few, dim), F32), ((few, dim), F32), ((N_DP, few, dim), F32))] + [
            dma((N_DP,)), dma((depth,)), dma((5,)), dma((2, len(COPIES))), dma((SIDE, 2, N_DP)), dma((SIDE, 2, N_TP))],
        compiler_params=pltpu.CompilerParams(collective_id=0, has_side_effects=True, vmem_limit_bytes=L_FRONT * MIB),
        cost_estimate=pl.CostEstimate(flops=3 * 10 ** 9, bytes_accessed=100 * MIB, transcendentals=0), name='front')(
            *(pltpu.with_memory_space_constraint(a, pltpu.HBM) for a in (hidden, gain_row, mask_row, teacher, table)))


def finish(teas, x_all, tab_part, coef):
    n, tokens, late = teas.shape
    dim = x_all.shape[1]
    span = late // 2

    def kern(tea_ref, x_ref, tab_ref, coef_ref, out_ref, z_buf, g_buf):
        at = peers()[1]

        def block(b, _):
            grad_block(at, tea_ref, x_ref, tab_ref[aligned(late + b * span, span)], coef_ref, z_buf, g_buf, out_ref, b)
            return 0

        lax.fori_loop(0, 2, block, 0)

    return pl.pallas_call(kern, out_shape=jax.ShapeDtypeStruct((2, span, dim), F32), in_specs=[VM] * 4, out_specs=VM,
        scratch_shapes=[pltpu.VMEM((n * tokens, span), F32), pltpu.VMEM((n * tokens, span), BF16)], name='finish',
        compiler_params=pltpu.CompilerParams(vmem_limit_bytes=22 * MIB),
        cost_estimate=pl.CostEstimate(flops=10 ** 9, bytes_accessed=8 * MIB, transcendentals=0))(teas, x_all, tab_part, coef)


def place(table, pieces, vocab):
    arrays = [p[0] for p in pieces]
    n = len(arrays)
    dim = arrays[0].shape[1]
    rows = vocab // N_DP
    quarter = rows // SIDE
    cut = 128
    chunks = [(i, r) for i in range(n) for r in range(0, arrays[i].shape[0], cut)]

    def kern(*refs):
        dst, buf, sem = refs[-DOWN:]
        at = peers()[1]
        reads, writes = [], []
        for k, (i, r) in enumerate(chunks):
            _, dz, dy, kind, half, start = pieces[i]
            first = (2 * (half + r // quarter) + kind) * quarter + start + r % quarter
            there = aligned(at[dz, dy] * rows + first, cut, cut)
            reads.append(pltpu.make_async_copy(refs[i].at[pl.ds(r, cut)], buf.at[k], sem.at[0, k]))
            writes.append(pltpu.make_async_copy(buf.at[k], dst.at[there], sem.at[1, k]))
        for cp in reads:
            cp.start()
        for read, write in zip(reads, writes):
            read.wait()
            write.start()
        for cp in writes:
            cp.wait()

    args = arrays if table is None else [*arrays, table]
    size = len(chunks) * cut * dim
    return pl.pallas_call(kern, out_shape=jax.ShapeDtypeStruct((vocab, dim), F32), in_specs=[pl.BlockSpec(memory_space=pl.ANY)] * n + [HB] * (len(args) - n),
        out_specs=HB, scratch_shapes=[pltpu.VMEM((len(chunks), cut, dim), F32), pltpu.SemaphoreType.DMA((2, len(chunks)))],
        input_output_aliases={} if table is None else {n: 0}, name='place', compiler_params=pltpu.CompilerParams(vmem_limit_bytes=4 * size + MIB),
        cost_estimate=pl.CostEstimate(flops=10 * MIB, bytes_accessed=8 * size, transcendentals=0))(*args)


def gather(first, rest, vocab):
    quarter = first[0].shape[0]
    sets, ways = range(2), (UP, DOWN)
    most = quarter - LANES
    cuts = slice(0, most), slice(most, quarter)
    table, event = None, 0

    def send(pair, axis, step):
        out = []
        for k in sets:
            dz, dy = (step, 0) if axis == k else (0, step)
            out.append(lax.ppermute(pair[k], 'dp', [(d, shift(d, dz, dy)) for d in range(N_DP)]))
        return out

    def put(pair, a, b, c=0, start=0):
        return [(pair[k], *((b, a) if k else (a, b)), k, c, start) for k in sets]

    def settle(*pieces):
        nonlocal table
        table = place(table, [p for ps in pieces for p in ps], vocab)

    def wait(*pairs):
        nonlocal table, event
        event += 1
        table, *flat = lax.optimization_barrier((table, *(x for pair in pairs for x in pair)))
        return [flat[2 * i:2 * i + 2] for i in range(len(pairs))]

    def join(one, other):
        return [jnp.concatenate(pair) for pair in zip(one, other)]

    own = [first]
    low, high = ([send(own[0], 0, way)] for way in ways)
    later = rest()
    event = 1
    own.append([later[k] for k in sets])
    low.append(send(own[1], 0, UP))
    high.append(send(own[1], 0, DOWN))
    whole = join(*own)
    side = {way: send(whole, 1, way) for way in ways}
    settle(put(own[0], 0, 0, 0), put(own[1], 0, 0, 1))

    low[0], high[0] = wait(low[0], high[0])
    far_low = send(low[0], 0, UP)
    settle(put(low[0], DOWN, 0, 0), put(high[0], UP, 0, 0))

    low[1], high[1] = wait(low[1], high[1])
    far_high = send(high[1], 0, DOWN)
    low_whole, high_whole = join(*low), join(*high)
    low_side = {way: send(low_whole, 1, way) for way in ways}
    settle(put(low[1], DOWN, 0, 1), put(high[1], UP, 0, 1))

    side[UP], side[DOWN], high_whole = wait(side[UP], side[DOWN], high_whole)
    high_side = {way: send(high_whole, 1, way) for way in ways}
    side_far = send(side[UP], 1, UP)
    settle(put(side[UP], 0, DOWN))
    settle(put(side[DOWN], 0, UP))

    far_low, far_high = wait(far_low, far_high)
    far_side = {(c, way): send(pair, 1, way) for way in ways for c, pair in enumerate((far_low, far_high))}
    settle(put(far_low, AWAY, 0, 0), put(far_high, AWAY, 0, 1))

    low_side[UP], low_side[DOWN] = wait(low_side[UP], low_side[DOWN])
    low_far = send(low_side[DOWN], 1, DOWN)
    settle(put(low_side[UP], DOWN, DOWN))
    settle(put(low_side[DOWN], DOWN, UP))

    high_side[UP], high_side[DOWN] = wait(high_side[UP], high_side[DOWN])
    high_far = [send([x[:quarter] for x in high_side[UP]], 1, UP), send([x[quarter:] for x in high_side[DOWN]], 1, DOWN)]
    settle(put(high_side[UP], UP, DOWN))
    settle(put(high_side[DOWN], UP, UP))

    far_side[0, DOWN], far_side[1, DOWN], side_far = wait(far_side[0, DOWN], far_side[1, DOWN], side_far)
    last_down = [send([x[cut] for x in far_side[1, DOWN]], 1, DOWN) for cut in cuts]
    settle(put(far_side[0, DOWN], AWAY, UP, 0), put(far_side[1, DOWN], AWAY, UP, 1))
    settle(put(side_far, 0, AWAY))

    far_side[0, UP], = wait(far_side[0, UP])
    last_up = [send([x[cut] for x in far_side[0, UP]], 1, UP) for cut in cuts]
    settle(put(far_side[0, UP], AWAY, DOWN, 0))

    far_side[1, UP], low_far = wait(far_side[1, UP], low_far)
    settle(put(far_side[1, UP], AWAY, DOWN, 1))
    settle(put(low_far, DOWN, AWAY))

    high_far = wait(*high_far)
    settle(put(high_far[0], UP, AWAY, 0), put(high_far[1], UP, AWAY, 1))
    for up, down, cut in zip(last_up, last_down, cuts):
        up, down = wait(up, down)
        settle(put(up, AWAY, AWAY, 0, cut.start), put(down, AWAY, AWAY, 1, cut.start))
    return table


def solution(mesh):
    def local_step(hid_rows, w_final, tab_rows, tea_rows, mask_rows):
        tokens = hid_rows.shape[0]
        late, soon, x_all, tab_part, coef, stats, grad_h, gain_line = front(hid_rows, w_final.reshape(-1, LANES), mask_rows[None], tea_rows, tab_rows)
        coef, *first = lax.optimization_barrier((coef, soon[0], soon[1]))
        table = gather(first, lambda: finish(late, x_all, tab_part, coef), tab_rows.shape[0])
        s_sum, t_sum, k_sum, masks = (stats[:, i, :tokens] for i in range(SIDE))
        all_kl = k_sum / t_sum + jnp.log(s_sum) - jnp.log(t_sum)
        loss_val = jnp.sum(masks * all_kl) / jnp.sum(masks)
        return loss_val, grad_h.astype(BF16), gain_line[0], table

    return jax.shard_map(local_step, mesh=mesh, in_specs=(P('dp', None), P(None), P('tp', None), P('dp', 'tp'), P('dp')), out_specs=(P(), P('dp', None), P(None), P('tp', None)), check_vma=False)
```

```python
import jax
import jax.numpy as jnp
from jax import lax
from jax.experimental import pallas as pl
from jax.experimental.pallas import tpu as pltpu
from jax.sharding import PartitionSpec as P


SOFT_CAP = 30.0
INV_CAP = 1.0 / SOFT_CAP
NORM_EPS = 1e-6
SIDE, N_DP, N_TP, LANES = 4, 16, 8, 128
UP, DOWN, AWAY = 1, 3, 2
MIB = 2 ** 20
L_FRONT = 41
MESH = pl.DeviceIdType.MESH
VM = pl.BlockSpec(memory_space=pltpu.VMEM)
HB = pl.BlockSpec(memory_space=pltpu.HBM)
F32, BF16 = jnp.float32, jnp.bfloat16
ROWS_BY_ROWS = (((1,), (1,)), ((), ()))
COLS_BY_COLS = (((0,), (0,)), ((), ()))

OFFSETS = tuple((dz, dy) for dz in range(SIDE) for dy in range(SIDE))
ORDER = tuple(sorted(OFFSETS, key=lambda o: -sum(min(d, SIDE - d) for d in o)))


def shift(dp, dz, dy):
    return (dp // SIDE + dz + SIDE) % SIDE * SIDE + (dp % SIDE + dy + SIDE) % SIDE


def peers():
    me = lax.axis_index('dp')
    z, y = lax.div(me, SIDE), lax.rem(me, SIDE)
    zs = [lax.rem(z + d, SIDE) * SIDE for d in range(SIDE)]
    ys = [lax.rem(y + d, SIDE) for d in range(SIDE)]
    return me, {(dz, dy): zs[dz] + ys[dy] for dz in range(-DOWN, SIDE) for dy in range(-DOWN, SIDE)}


def aligned(start, size, unit=LANES):
    return pl.ds(pl.multiple_of(start, unit), size)


def hops(kind, dz, dy):
    along_z = [(dz, 0)] if dz % 2 else [(UP if dy < AWAY else DOWN, 0)] * dz
    along_y = [(0, dy)] if dy % 2 else [(0, UP if dz < AWAY else DOWN)] * dy
    return along_y + along_z if kind else along_z + along_y


JOBS = tuple((kind, o) for o in ORDER[:-1] for kind in range(2))
PATHS = tuple(hops(kind, *o) for kind, o in JOBS)
MIDDLE = tuple((j, level) for level in range(SIDE) for j, path in enumerate(PATHS) if len(path) > level + 1)


def waves(j, level):
    return (None,) if (j, level) in MIDDLE and level < 2 else (0, 1)


COPIES = tuple((j, level, w) for j, path in enumerate(PATHS) for level in range(len(path)) for w in waves(j, level))


def grad_block(at, tea_ref, x_ref, tab_rows, coef_ref, z_buf, g_buf, out_ref, block):
    tokens = tea_ref.shape[1]
    span = tab_rows.shape[0]
    few = LANES // N_DP
    cols = aligned(block * span, span)
    z_buf[:, :span] = lax.dot_general(x_ref[...], tab_rows, ROWS_BY_ROWS, preferred_element_type=F32)
    for k, (dz, dy) in enumerate(OFFSETS):
        here = aligned(at[-dz, -dy] * tokens, tokens, tokens)
        ratio = jnp.tanh(z_buf[here, :span] * INV_CAP)
        stu = jnp.exp(SOFT_CAP * ratio - SOFT_CAP)
        inv_s, inv_t, _, weight = (coef_ref[0:tokens, k * few + i:k * few + i + 1] for i in range(SIDE))
        diff = (stu * inv_s - tea_ref[k, :, cols] * inv_t) * weight
        g_buf[here, :span] = (diff * (1.0 - ratio * ratio)).astype(BF16)
    out_ref[block] = lax.dot_general(g_buf[:, :span], x_ref[...], COLS_BY_COLS, preferred_element_type=F32)


def front(hidden, gain_row, mask_row, teacher, table):
    tokens, vocab = teacher.shape
    dim = hidden.shape[1]
    part = vocab // N_DP
    half = tokens // 2
    few = tokens // N_TP
    pack = 16
    sub = 512
    per = part // sub
    tiles = vocab // sub
    depth = 6

    def kern(hid_hbm, gain_hbm, mask_hbm, tea_ref, tab_ref, got_late, blocks_ref, x_out, tab_out, coef_ref, all_ref, gh_ref, gg_ref,
             hid_ref, gain_ref, mask_in, w_ref, raw, sends, stage, got_soon, tabs, n_buf, x_buf, inv_buf, square, pay, pay_got, mask_own, mask_got, x_got, tp_got, own_col,
             own_row, rel, dx, rs_got, ag_own, ag_got, gn_own, gn_got, raw_sem, tab_sem, in_sem, hop_sem, dp_sem, tp_sem):
        me, at = peers()
        col = lax.axis_index('tp')
        mates = [lax.rem(col + j, N_TP) for j in range(N_TP)]
        my_few = aligned(col * few, few, few)

        def fetch(k):
            d = at[ORDER[k]]
            return pltpu.make_async_copy(tea_ref.at[:, aligned(d * part, part)], raw.at[aligned(d * tokens, tokens, tokens)], raw_sem.at[k])

        def tab_copy(i):
            slot = lax.rem(i, depth)
            return pltpu.make_async_copy(tab_ref.at[aligned(lax.rem(i, tiles) * sub, sub)], tabs.at[slot], tab_sem.at[slot])

        inputs = [pltpu.make_async_copy(src, dst, in_sem.at[2 + i])
                  for i, (src, dst) in enumerate(((hid_hbm, hid_ref), (gain_hbm, gain_ref), (mask_hbm, mask_in)))]
        own_tab = pltpu.make_async_copy(tab_ref.at[aligned(me * part, part)], tab_out, in_sem.at[1])
        for cp in inputs:
            cp.start()
        for k in range(N_DP):
            fetch(k).start()
        for i in range(depth - 1):
            tab_copy(i).start()
        own_tab.start()
        barrier = pltpu.get_barrier_semaphore()
        for dz, dy in ORDER[:-1]:
            pl.semaphore_signal(barrier, inc=1, device_id=(at[dz, dy], col), device_id_type=MESH)
        for j in range(1, N_TP):
            pl.semaphore_signal(barrier, inc=1, device_id=(me, mates[j]), device_id_type=MESH)

        for cp in inputs:
            cp.wait()
        w_ref[...] = 1.0 + jnp.concatenate([gain_ref[i:i + 1] for i in range(dim // LANES)], axis=1)
        hid = hid_ref[...].astype(F32)
        inv = lax.rsqrt(jnp.mean(hid * hid, axis=1, keepdims=True) + NORM_EPS)
        n_buf[...] = hid * inv
        x_buf[...] = (n_buf[...] * w_ref[...]).astype(BF16)
        inv_buf[...] = jnp.broadcast_to(inv, (tokens, LANES))
        pay[...] = n_buf[my_few]
        square[...] = jnp.zeros((LANES, LANES), F32)
        square[0:1, 0:tokens] = mask_in[...]
        mask_own[...] = square[0:few]
        mask_col = jnp.transpose(square[...])[0:tokens, 0:1]

        def weigh(k):
            fetch(k).wait()
            d = at[ORDER[k]]

            def rows(r, _):
                here = aligned(d * tokens + r * pack, pack, pack)
                cap = jnp.tanh(raw[here].astype(F32) * INV_CAP)
                sends[here] = jnp.exp(SOFT_CAP * cap - SOFT_CAP)
                return 0

            lax.fori_loop(0, tokens // pack, rows, 0)

        weigh(0)
        weigh(1)
        pl.semaphore_wait(barrier, N_DP + N_TP - 2)

        def remote(src, dst, out, into, dp, tp):
            return pltpu.make_async_remote_copy(src_ref=src, dst_ref=dst, send_sem=out, recv_sem=into, device_id=(dp, tp), device_id_type=MESH)

        def to_dp(src, dst, x, rows=slice(None)):
            def send(o):
                d = at[o]
                return remote(src.at[rows], dst.at[me, rows], dp_sem.at[x, 0, d], dp_sem.at[x, 1, me], d, col)

            def into(o):
                d = at[o]
                return remote(src.at[rows], dst.at[d, rows], dp_sem.at[x, 0, d], dp_sem.at[x, 1, d], d, col)

            return [send(o) for o in ORDER[:-1]], [into(o) for o in ORDER[:-1]]

        def to_tp(srcs, dst, x):
            def send(j):
                c = mates[j]
                return remote(srcs(c), dst.at[col], tp_sem.at[x, 0, c], tp_sem.at[x, 1, col], me, c)

            def into(j):
                c = mates[j]
                return remote(srcs(c), dst.at[c], tp_sem.at[x, 0, c], tp_sem.at[x, 1, c], me, c)

            return [send(j) for j in range(1, N_TP)], [into(j) for j in range(1, N_TP)]

        def start(copies):
            for cp in copies:
                cp.start()

        def arrive(copies):
            for cp in copies:
                cp.wait_recv()

        def added(ref, here=slice(None)):
            total = ref[0, here]
            for d in range(1, ref.shape[0]):
                total = total + ref[d, here]
            return total

        gots = (got_soon, got_late)
        late = part // 2

        def hop(j, level, w):
            kind, (dz, dy) = JOBS[j]
            tok = pl.ds(kind * half, half)
            rows = slice(None) if w is None else pl.ds(w * late, late)
            src = stage.at[MIDDLE.index((j, level - 1)), :, rows] if level else sends.at[aligned(at[dz, dy] * tokens + kind * half, half, half), rows]
            dst = stage.at[MIDDLE.index((j, level)), :, rows] if (j, level) in MIDDLE else gots[w].at[dz * SIDE + dy, tok]
            k = COPIES.index((j, level, w))
            return remote(src, dst, hop_sem.at[0, k], hop_sem.at[1, k], at[PATHS[j][level]], col)

        def came(level, w=None):
            for j, at in MIDDLE:
                if at == level:
                    hop(j, level, w).wait_recv()

        def onward(level, far, *ws):
            for w in ws:
                for j, at in MIDDLE:
                    if at == level - 1 and far == (len(PATHS[j]) > 2):
                        hop(j, level, w).start()

        pay_sends, pay_came = to_dp(pay, pay_got, 0)
        start(pay_sends)
        pay_got[me] = pay[...]
        mask_sends, mask_came = to_dp(mask_own, mask_got, 1, pl.ds(0, 1))
        start(mask_sends)
        mask_got[me] = mask_own[...]

        for k, o in enumerate(ORDER):
            if k > 1:
                weigh(k)
            for j, (_, to) in enumerate(JOBS):
                if to == o:
                    for w in waves(j, 0):
                        hop(j, 0, w).start()

        def keep(r, _):
            here, there = aligned(me * tokens + r * pack, pack, pack), aligned(r * pack, pack, pack)
            got_soon[0, there] = sends[here, :late]
            got_late[0, there] = sends[here, late:]
            return 0

        lax.fori_loop(0, tokens // pack, keep, 0)

        twin = col + 1 - 2 * lax.rem(col, 2)
        arrive((*pay_came, *mask_came))
        x_got[col] = pay_got[...]

        def across(j, origin):
            return remote(pay_got, x_got.at[origin], tp_sem.at[1, 0, mates[j]], tp_sem.at[1, 1, origin], me, mates[j])

        def to_twin(j, origin):
            return remote(x_got.at[origin], x_got.at[origin], tp_sem.at[1, 0, mates[j + 1]], tp_sem.at[1, 1, origin], me, twin)

        evens = range(0, N_TP, 2)
        xt_sends = [across(j, col) for j in evens[1:]]
        start(xt_sends)

        def fold(v):
            total = v[:, :LANES]
            for c in range(LANES, v.shape[1], LANES):
                total = total + v[:, c:c + LANES]
            return total

        def student(slot):
            z = lax.dot_general(x_buf[...], tabs[slot], ROWS_BY_ROWS, preferred_element_type=F32)
            ratio = jnp.tanh(z * INV_CAP)
            return ratio, jnp.exp(SOFT_CAP * ratio - SOFT_CAP)

        def forward(i, sums):
            slot = lax.rem(i, depth)
            tab_copy(i).wait()
            tab_copy(i + depth - 1).start()
            s_sum, t_sum, k_sum = sums
            ratio, stu = student(slot)
            toks, here = aligned(lax.div(i, per) * tokens, tokens, tokens), aligned(lax.rem(i, per) * sub, sub)
            cap = jnp.tanh(raw[toks, here].astype(F32) * INV_CAP)
            tea = sends[toks, here]
            return s_sum + fold(stu), t_sum + fold(tea), k_sum + fold(tea * (cap - ratio))

        zero = jnp.zeros((tokens, LANES), F32)
        s_sum, t_sum, k_sum = lax.fori_loop(0, tiles, forward, (zero, zero, zero))
        lane = lax.broadcasted_iota(jnp.int32, (tokens, LANES), 1)
        sums = jnp.where(lane == 0, jnp.sum(s_sum, axis=1, keepdims=True), 0.0)
        sums = jnp.where(lane == 1, jnp.sum(t_sum, axis=1, keepdims=True), sums)
        sums = jnp.where(lane == AWAY, SOFT_CAP * jnp.sum(k_sum, axis=1, keepdims=True), sums)
        own_col[...] = sums
        tp_got[col] = sums
        tp_sends, tp_came = to_tp(lambda c: own_col, tp_got, 0)
        start(tp_sends)
        arrive(tp_came)
        total = added(tp_got)
        square[0:tokens] = jnp.where(lane == DOWN, mask_col, total)
        line = jnp.transpose(square[...])[0:few]
        own_row[...] = line
        all_ref[me] = line
        dp_sends, dp_came = to_dp(own_row, all_ref, 2)
        start(dp_sends)
        arrive([across(j, mates[j]) for j in evens[1:]])
        twin_sends = [to_twin(j, mates[j]) for j in evens]
        start(twin_sends)
        came(0)
        onward(1, True, None)
        onward(1, False, 0)

        count = jnp.sum(added(mask_got, slice(1)), axis=1, keepdims=True)
        inv_s, inv_t, weight = 1.0 / total[:, 0:1], 1.0 / total[:, 1:2], mask_col / count
        dx[...] = jnp.zeros((tokens, dim), F32)

        def backward(i, _):
            slot = lax.rem(i, depth)
            tab_copy(i).wait()

            @pl.when(i + depth - 1 < 2 * tiles)
            def _():
                tab_copy(i + depth - 1).start()

            ratio, stu = student(slot)
            tea = sends[aligned(lax.div(i - tiles, per) * tokens, tokens, tokens), aligned(lax.rem(i, per) * sub, sub)]
            diff = (stu * inv_s - tea * inv_t) * weight
            g = (diff * (1.0 - ratio * ratio)).astype(BF16)
            dx[...] += jnp.dot(g, tabs[slot], preferred_element_type=F32)
            return 0

        lax.fori_loop(tiles, 2 * tiles, backward, 0)
        came(1)
        onward(2, True, 0)

        rs_got[col] = dx[my_few]
        rs_sends, rs_came = to_tp(lambda c: dx.at[aligned(c * few, few, few)], rs_got, 2)
        start(rs_sends)
        arrive(rs_came)
        my_x = added(rs_got)
        my_n = n_buf[my_few]
        grad_n = my_x * w_ref[...]
        my_h = inv_buf[my_few, 0:1] * (grad_n - my_n * jnp.mean(grad_n * my_n, axis=1, keepdims=True))
        ag_own[...] = jnp.zeros((2 * few, dim), F32)
        ag_own[0:few] = my_h
        ag_own[few:few + 1] = jnp.sum(my_x * my_n, axis=0, keepdims=True)
        ag_got[col] = ag_own[...]
        ag_sends, ag_came = to_tp(lambda c: ag_own, ag_got, DOWN)
        start(ag_sends)
        arrive(ag_came)
        gh_ref[...] = jnp.concatenate([ag_got[j, 0:few] for j in range(N_TP)], axis=0)
        line = added(ag_got, slice(few, few + 1))
        gn_own[0:1] = line
        gn_got[me, 0:1] = line
        gn_sends, gn_came = to_dp(gn_own, gn_got, DOWN, pl.ds(0, 1))
        start(gn_sends)

        came(2, 0)
        onward(DOWN, True, 0)
        onward(2, True, 1)
        onward(1, False, 1)
        arrive([to_twin(j, mates[j + 1]) for j in evens])

        def widen(d, _):
            rows = jnp.concatenate([x_got[j, d] for j in range(N_TP)], axis=0)
            x_out[aligned(d * tokens, tokens, tokens)] = (rows * w_ref[...]).astype(BF16)
            return 0

        lax.fori_loop(0, N_DP, widen, 0)
        arrive(dp_came)
        row = lax.broadcasted_iota(jnp.int32, (few, LANES), 0)
        lanes = lax.broadcasted_iota(jnp.int32, (few, LANES), 1)
        for d in range(N_DP):
            block = all_ref[d]
            safe = jnp.where((row < AWAY) & (lanes < tokens), block, 1.0)
            rel[d * few:(d + 1) * few] = jnp.where(row < AWAY, 1.0 / safe, block / count)
        for k, (dz, dy) in enumerate(OFFSETS):
            square[k * few:(k + 1) * few] = rel[aligned(at[-dz, -dy] * few, few, few)]
        coef_ref[...] = jnp.transpose(square[...])

        own_tab.wait()
        for j, path in enumerate(PATHS):
            hop(j, len(path) - 1, 0).wait_recv()
        for j, level, w in COPIES:
            if level == 0:
                hop(j, level, w).wait_send()

        def block(b, _):
            @pl.when(b == 1)
            def _():
                came(2, 1)
                onward(DOWN, True, 1)

            grad_block(at, got_soon, x_out, tab_out[aligned(b * sub, sub)], coef_ref, sends, raw, blocks_ref, b)
            return 0

        lax.fori_loop(0, 2, block, 0)
        arrive(gn_came)
        gg_ref[...] = added(gn_got, slice(1))
        for j, path in enumerate(PATHS):
            hop(j, len(path) - 1, 1).wait_recv()
        for j, level, w in COPIES:
            if level:
                hop(j, level, w).wait_send()
        for cp in (*pay_sends, *mask_sends, *tp_sends, *dp_sends, *xt_sends, *twin_sends, *rs_sends, *ag_sends, *gn_sends):
            cp.wait_send()

    dma = pltpu.SemaphoreType.DMA
    wide, flat = (tokens, dim), (few, LANES)
    return pl.pallas_call(
        kern,
        out_shape=tuple(jax.ShapeDtypeStruct(shape, kind) for shape, kind in (
            ((N_DP, tokens, part // 2), F32), ((2, sub, dim), F32), ((N_DP * tokens, dim), BF16), ((part, dim), BF16), ((LANES, LANES), F32), ((N_DP, *flat), F32), (wide, F32),
            ((1, dim), F32))),
        in_specs=[HB] * 5, out_specs=(VM,) * 8,
        scratch_shapes=[pltpu.VMEM(shape, kind) for shape, kind in (
            (wide, BF16), ((dim // LANES, LANES), F32), ((1, tokens), F32), ((1, dim), F32), ((N_DP * tokens, part), BF16), ((N_DP * tokens, part), F32),
            ((len(MIDDLE), half, part), F32), ((N_DP, tokens, part // 2), F32),
            ((depth, sub, dim), BF16), (wide, F32), (wide, BF16), ((tokens, LANES), F32), ((LANES, LANES), F32), ((few, dim), F32),
            ((N_DP, few, dim), F32), (flat, F32), ((N_DP, *flat), F32), ((N_TP, N_DP, few, dim), F32), ((N_TP, tokens, LANES), F32),
            ((tokens, LANES), F32), (flat, F32), ((LANES, LANES), F32), (wide, F32), ((N_TP, few, dim), F32), ((2 * few, dim), F32),
            ((N_TP, 2 * few, dim), F32), ((few, dim), F32), ((N_DP, few, dim), F32))] + [
            dma((N_DP,)), dma((depth,)), dma((5,)), dma((2, len(COPIES))), dma((SIDE, 2, N_DP)), dma((SIDE, 2, N_TP))],
        compiler_params=pltpu.CompilerParams(collective_id=0, has_side_effects=True, vmem_limit_bytes=L_FRONT * MIB),
        cost_estimate=pl.CostEstimate(flops=3 * 10 ** 9, bytes_accessed=100 * MIB, transcendentals=0), name='front')(
            *(pltpu.with_memory_space_constraint(a, pltpu.HBM) for a in (hidden, gain_row, mask_row, teacher, table)))


def finish(teas, x_all, tab_part, coef):
    n, tokens, late = teas.shape
    dim = x_all.shape[1]
    span = late // 2

    def kern(tea_ref, x_ref, tab_ref, coef_ref, out_ref, z_buf, g_buf):
        at = peers()[1]

        def block(b, _):
            grad_block(at, tea_ref, x_ref, tab_ref[aligned(late + b * span, span)], coef_ref, z_buf, g_buf, out_ref, b)
            return 0

        lax.fori_loop(0, 2, block, 0)

    return pl.pallas_call(kern, out_shape=jax.ShapeDtypeStruct((2, span, dim), F32), in_specs=[VM] * 4, out_specs=VM,
        scratch_shapes=[pltpu.VMEM((n * tokens, span), F32), pltpu.VMEM((n * tokens, span), BF16)], name='finish',
        compiler_params=pltpu.CompilerParams(vmem_limit_bytes=22 * MIB),
        cost_estimate=pl.CostEstimate(flops=10 ** 9, bytes_accessed=8 * MIB, transcendentals=0))(teas, x_all, tab_part, coef)


def place(table, pieces, vocab):
    arrays = [p[0] for p in pieces]
    n = len(arrays)
    dim = arrays[0].shape[1]
    rows = vocab // N_DP
    quarter = rows // SIDE
    cut = 256
    chunks = [(i, r) for i in range(n) for r in range(0, arrays[i].shape[0], cut)]

    def kern(*refs):
        dst, buf, sem = refs[-DOWN:]
        at = peers()[1]
        reads, writes = [], []
        for k, (i, r) in enumerate(chunks):
            _, dz, dy, kind, half = pieces[i]
            first = (2 * (half + r // quarter) + kind) * quarter + r % quarter
            there = aligned(at[dz, dy] * rows + first, cut, cut)
            reads.append(pltpu.make_async_copy(refs[i].at[pl.ds(r, cut)], buf.at[k], sem.at[0, k]))
            writes.append(pltpu.make_async_copy(buf.at[k], dst.at[there], sem.at[1, k]))
        for cp in reads:
            cp.start()
        for read, write in zip(reads, writes):
            read.wait()
            write.start()
        for cp in writes:
            cp.wait()

    args = arrays if table is None else [*arrays, table]
    size = len(chunks) * cut * dim
    return pl.pallas_call(kern, out_shape=jax.ShapeDtypeStruct((vocab, dim), F32), in_specs=[pl.BlockSpec(memory_space=pl.ANY)] * n + [HB] * (len(args) - n),
        out_specs=HB, scratch_shapes=[pltpu.VMEM((len(chunks), cut, dim), F32), pltpu.SemaphoreType.DMA((2, len(chunks)))],
        input_output_aliases={} if table is None else {n: 0}, name='place', compiler_params=pltpu.CompilerParams(vmem_limit_bytes=4 * size + MIB),
        cost_estimate=pl.CostEstimate(flops=10 * MIB, bytes_accessed=8 * size, transcendentals=0))(*args)


def gather(first, rest, vocab):
    quarter = first[0].shape[0]
    sets, ways = range(2), (UP, DOWN)
    table, event = None, 0

    def send(pair, axis, step):
        out = []
        for k in sets:
            dz, dy = (step, 0) if axis == k else (0, step)
            out.append(lax.ppermute(pair[k], 'dp', [(d, shift(d, dz, dy)) for d in range(N_DP)]))
        return out

    def put(pair, a, b, c=0):
        return [(pair[k], *((b, a) if k else (a, b)), k, c) for k in sets]

    def settle(*pieces):
        nonlocal table
        table = place(table, [p for ps in pieces for p in ps], vocab)

    def wait(*pairs):
        nonlocal table, event
        event += 1
        table, *flat = lax.optimization_barrier((table, *(x for pair in pairs for x in pair)))
        return [flat[2 * i:2 * i + 2] for i in range(len(pairs))]

    def join(one, other):
        return [jnp.concatenate(pair) for pair in zip(one, other)]

    own = [first]
    low, high = ([send(own[0], 0, way)] for way in ways)
    later = rest()
    event = 1
    own.append([later[k] for k in sets])
    low.append(send(own[1], 0, UP))
    high.append(send(own[1], 0, DOWN))
    whole = join(*own)
    side = {way: send(whole, 1, way) for way in ways}
    settle(put(own[0], 0, 0, 0), put(own[1], 0, 0, 1))

    low[0], high[0] = wait(low[0], high[0])
    far_low = send(low[0], 0, UP)
    settle(put(low[0], DOWN, 0, 0), put(high[0], UP, 0, 0))

    low[1], high[1] = wait(low[1], high[1])
    far_high = send(high[1], 0, DOWN)
    low_whole, high_whole = join(*low), join(*high)
    low_side = {way: send(low_whole, 1, way) for way in ways}
    settle(put(low[1], DOWN, 0, 1), put(high[1], UP, 0, 1))

    side[UP], side[DOWN], high_whole = wait(side[UP], side[DOWN], high_whole)
    high_side = {way: send(high_whole, 1, way) for way in ways}
    side_far = send(side[UP], 1, UP)
    settle(put(side[UP], 0, DOWN))
    settle(put(side[DOWN], 0, UP))

    far_low, far_high = wait(far_low, far_high)
    far_side = {(c, way): send(pair, 1, way) for way in ways for c, pair in enumerate((far_low, far_high))}
    settle(put(far_low, AWAY, 0, 0), put(far_high, AWAY, 0, 1))

    low_side[UP], low_side[DOWN] = wait(low_side[UP], low_side[DOWN])
    low_far = send(low_side[DOWN], 1, DOWN)
    settle(put(low_side[UP], DOWN, DOWN))
    settle(put(low_side[DOWN], DOWN, UP))

    high_side[UP], high_side[DOWN] = wait(high_side[UP], high_side[DOWN])
    high_far = [send([x[:quarter] for x in high_side[UP]], 1, UP), send([x[quarter:] for x in high_side[DOWN]], 1, DOWN)]
    settle(put(high_side[UP], UP, DOWN))
    settle(put(high_side[DOWN], UP, UP))

    far_side[0, DOWN], far_side[1, DOWN], side_far = wait(far_side[0, DOWN], far_side[1, DOWN], side_far)
    last_down = send(far_side[1, DOWN], 1, DOWN)
    settle(put(far_side[0, DOWN], AWAY, UP, 0), put(far_side[1, DOWN], AWAY, UP, 1))
    settle(put(side_far, 0, AWAY))

    far_side[0, UP], = wait(far_side[0, UP])
    last_up = send(far_side[0, UP], 1, UP)
    settle(put(far_side[0, UP], AWAY, DOWN, 0))

    far_side[1, UP], low_far = wait(far_side[1, UP], low_far)
    settle(put(far_side[1, UP], AWAY, DOWN, 1))
    settle(put(low_far, DOWN, AWAY))

    high_far = wait(*high_far)
    settle(put(high_far[0], UP, AWAY, 0), put(high_far[1], UP, AWAY, 1))
    last_up, last_down = wait(last_up, last_down)
    settle(put(last_up, AWAY, AWAY, 0), put(last_down, AWAY, AWAY, 1))
    return table


def solution(mesh):
    def local_step(hid_rows, w_final, tab_rows, tea_rows, mask_rows):
        tokens = hid_rows.shape[0]
        late, soon, x_all, tab_part, coef, stats, grad_h, gain_line = front(hid_rows, w_final.reshape(-1, LANES), mask_rows[None], tea_rows, tab_rows)
        coef, *first = lax.optimization_barrier((coef, soon[0], soon[1]))
        table = gather(first, lambda: finish(late, x_all, tab_part, coef), tab_rows.shape[0])
        s_sum, t_sum, k_sum, masks = (stats[:, i, :tokens] for i in range(SIDE))
        all_kl = k_sum / t_sum + jnp.log(s_sum) - jnp.log(t_sum)
        loss_val = jnp.sum(masks * all_kl) / jnp.sum(masks)
        return loss_val, grad_h.astype(BF16), gain_line[0], table

    return jax.shard_map(local_step, mesh=mesh, in_specs=(P('dp', None), P(None), P('tp', None), P('dp', 'tp'), P('dp')), out_specs=(P(), P('dp', None), P(None), P('tp', None)), check_vma=False)
```

```python
import jax
import jax.numpy as jnp
from jax import lax
from jax.experimental import pallas as pl
from jax.experimental.pallas import tpu as pltpu
from jax.sharding import PartitionSpec as P


SOFT_CAP = 30.0
INV_CAP = 1.0 / SOFT_CAP
NORM_EPS = 1e-6
SIDE, N_DP, N_TP, LANES = 4, 16, 8, 128
UP, DOWN, AWAY = 1, 3, 2
MIB = 2 ** 20
L_FRONT = 41
MESH = pl.DeviceIdType.MESH
VM = pl.BlockSpec(memory_space=pltpu.VMEM)
HB = pl.BlockSpec(memory_space=pltpu.HBM)
F32, BF16 = jnp.float32, jnp.bfloat16
ROWS_BY_ROWS = (((1,), (1,)), ((), ()))
COLS_BY_COLS = (((0,), (0,)), ((), ()))

OFFSETS = tuple((dz, dy) for dz in range(SIDE) for dy in range(SIDE))
ORDER = tuple(sorted(OFFSETS, key=lambda o: -sum(min(d, SIDE - d) for d in o)))


def shift(dp, dz, dy):
    return (dp // SIDE + dz + SIDE) % SIDE * SIDE + (dp % SIDE + dy + SIDE) % SIDE


def peers():
    me = lax.axis_index('dp')
    z, y = lax.div(me, SIDE), lax.rem(me, SIDE)
    zs = [lax.rem(z + d, SIDE) * SIDE for d in range(SIDE)]
    ys = [lax.rem(y + d, SIDE) for d in range(SIDE)]
    return me, {(dz, dy): zs[dz] + ys[dy] for dz in range(-DOWN, SIDE) for dy in range(-DOWN, SIDE)}


def aligned(start, size, unit=LANES):
    return pl.ds(pl.multiple_of(start, unit), size)


def hops(kind, dz, dy):
    along_z = [(dz, 0)] if dz % 2 else [(UP if dy < AWAY else DOWN, 0)] * dz
    along_y = [(0, dy)] if dy % 2 else [(0, UP if dz < AWAY else DOWN)] * dy
    return along_y + along_z if kind else along_z + along_y


JOBS = tuple((kind, o) for o in ORDER[:-1] for kind in range(2))
PATHS = tuple(hops(kind, *o) for kind, o in JOBS)
MIDDLE = tuple((j, level) for level in range(SIDE) for j, path in enumerate(PATHS) if len(path) > level + 1)


def waves(j, level):
    return (None,) if (j, level) in MIDDLE and level < 2 else (0, 1)


COPIES = tuple((j, level, w) for j, path in enumerate(PATHS) for level in range(len(path)) for w in waves(j, level))


def grad_block(at, tea_ref, x_ref, tab_rows, coef_ref, z_buf, g_buf, out_ref, block):
    tokens = tea_ref.shape[1]
    span = tab_rows.shape[0]
    few = LANES // N_DP
    cols = aligned(block * span, span)
    z_buf[:, :span] = lax.dot_general(x_ref[...], tab_rows, ROWS_BY_ROWS, preferred_element_type=F32)
    for k, (dz, dy) in enumerate(OFFSETS):
        here = aligned(at[-dz, -dy] * tokens, tokens, tokens)
        ratio = jnp.tanh(z_buf[here, :span] * INV_CAP)
        stu = jnp.exp(SOFT_CAP * ratio - SOFT_CAP)
        inv_s, inv_t, _, weight = (coef_ref[0:tokens, k * few + i:k * few + i + 1] for i in range(SIDE))
        diff = (stu * inv_s - tea_ref[k, :, cols] * inv_t) * weight
        g_buf[here, :span] = (diff * (1.0 - ratio * ratio)).astype(BF16)
    out_ref[block] = lax.dot_general(g_buf[:, :span], x_ref[...], COLS_BY_COLS, preferred_element_type=F32)


def front(hidden, gain_row, mask_row, teacher, table):
    tokens, vocab = teacher.shape
    dim = hidden.shape[1]
    part = vocab // N_DP
    half = tokens // 2
    few = tokens // N_TP
    pack = 16
    sub = 512
    per = part // sub
    tiles = vocab // sub
    depth = 2 * per
    ring = N_DP // 2
    few_first = 3

    def kern(hid_hbm, gain_hbm, mask_hbm, tea_ref, tab_ref, got_late, blocks_ref, x_out, tab_out, coef_ref, all_ref, gh_ref, gg_ref,
             hid_ref, gain_ref, mask_in, w_ref, raw, sends, stage, got_soon, g_buf, t_acc, c_acc, tabs, n_buf, x_buf, inv_buf, square, pay, pay_got, mask_own, mask_got, x_got, tp_got, own_col,
             own_row, rel, dx, rs_got, ag_own, ag_got, gn_own, gn_got, raw_sem, tab_sem, in_sem, hop_sem, dp_sem, tp_sem):
        me, at = peers()
        col = lax.axis_index('tp')
        mates = [lax.rem(col + j, N_TP) for j in range(N_TP)]
        my_few = aligned(col * few, few, few)

        def fetch(k):
            d = at[ORDER[k]]
            return pltpu.make_async_copy(tea_ref.at[:, aligned(d * part, part)], raw.at[pl.ds(k % ring * tokens, tokens)], raw_sem.at[k])

        def tab_copy(i):
            slot = lax.rem(i, depth)
            return pltpu.make_async_copy(tab_ref.at[aligned(lax.rem(i, tiles) * sub, sub)], tabs.at[slot], tab_sem.at[slot])

        inputs = [pltpu.make_async_copy(src, dst, in_sem.at[2 + i])
                  for i, (src, dst) in enumerate(((hid_hbm, hid_ref), (gain_hbm, gain_ref), (mask_hbm, mask_in)))]
        own_tab = pltpu.make_async_copy(tab_ref.at[aligned(me * part, part)], tab_out, in_sem.at[1])
        for cp in inputs:
            cp.start()
        for k in range(ring):
            fetch(k).start()
        for i in range(per):
            tab_copy(i).start()
        own_tab.start()
        barrier = pltpu.get_barrier_semaphore()
        for dz, dy in ORDER[:-1]:
            pl.semaphore_signal(barrier, inc=1, device_id=(at[dz, dy], col), device_id_type=MESH)
        for j in range(1, N_TP):
            pl.semaphore_signal(barrier, inc=1, device_id=(me, mates[j]), device_id_type=MESH)

        def fold(v):
            total = v[:, :LANES]
            for c in range(LANES, v.shape[1], LANES):
                total = total + v[:, c:c + LANES]
            return total

        def weigh(k):
            fetch(k).wait()
            d = at[ORDER[k]]

            def rows(r, _):
                here = aligned(r * pack, pack, pack)
                cap = jnp.tanh(raw[aligned(k % ring * tokens + r * pack, pack, pack)].astype(F32) * INV_CAP)
                tea = jnp.exp(SOFT_CAP * cap - SOFT_CAP)
                sends[aligned(d * tokens + r * pack, pack, pack)] = tea
                t_acc[here] += fold(tea)
                c_acc[here] += fold(tea * cap)
                return 0

            lax.fori_loop(0, tokens // pack, rows, 0)
            if k + ring < N_DP:
                fetch(k + ring).start()

        t_acc[...] = jnp.zeros((tokens, LANES), F32)
        c_acc[...] = jnp.zeros((tokens, LANES), F32)
        weigh(0)
        pl.semaphore_wait(barrier, N_DP + N_TP - 2)

        def remote(src, dst, out, into, dp, tp):
            return pltpu.make_async_remote_copy(src_ref=src, dst_ref=dst, send_sem=out, recv_sem=into, device_id=(dp, tp), device_id_type=MESH)

        def to_dp(src, dst, x, rows=slice(None)):
            def send(o):
                d = at[o]
                return remote(src.at[rows], dst.at[me, rows], dp_sem.at[x, 0, d], dp_sem.at[x, 1, me], d, col)

            def into(o):
                d = at[o]
                return remote(src.at[rows], dst.at[d, rows], dp_sem.at[x, 0, d], dp_sem.at[x, 1, d], d, col)

            return [send(o) for o in ORDER[:-1]], [into(o) for o in ORDER[:-1]]

        def to_tp(srcs, dst, x):
            def send(j):
                c = mates[j]
                return remote(srcs(c), dst.at[col], tp_sem.at[x, 0, c], tp_sem.at[x, 1, col], me, c)

            def into(j):
                c = mates[j]
                return remote(srcs(c), dst.at[c], tp_sem.at[x, 0, c], tp_sem.at[x, 1, c], me, c)

            return [send(j) for j in range(1, N_TP)], [into(j) for j in range(1, N_TP)]

        def start(copies):
            for cp in copies:
                cp.start()

        def arrive(copies):
            for cp in copies:
                cp.wait_recv()

        def added(ref, here=slice(None)):
            total = ref[0, here]
            for d in range(1, ref.shape[0]):
                total = total + ref[d, here]
            return total

        gots = (got_soon, got_late)
        late = part // 2

        def hop(j, level, w):
            kind, (dz, dy) = JOBS[j]
            tok = pl.ds(kind * half, half)
            rows = slice(None) if w is None else pl.ds(w * late, late)
            src = stage.at[MIDDLE.index((j, level - 1)), :, rows] if level else sends.at[aligned(at[dz, dy] * tokens + kind * half, half, half), rows]
            dst = stage.at[MIDDLE.index((j, level)), :, rows] if (j, level) in MIDDLE else gots[w].at[dz * SIDE + dy, tok]
            k = COPIES.index((j, level, w))
            return remote(src, dst, hop_sem.at[0, k], hop_sem.at[1, k], at[PATHS[j][level]], col)

        def came(level, w=None):
            for j, at in MIDDLE:
                if at == level:
                    hop(j, level, w).wait_recv()

        def onward(level, far, *ws):
            for w in ws:
                for j, at in MIDDLE:
                    if at == level - 1 and far == (len(PATHS[j]) > 2):
                        hop(j, level, w).start()

        def issue(k):
            for j, (_, to) in enumerate(JOBS):
                if to == ORDER[k]:
                    for w in waves(j, 0):
                        hop(j, 0, w).start()

        issue(0)
        for k in range(1, few_first):
            weigh(k)
            issue(k)
        for cp in inputs:
            cp.wait()
        w_ref[...] = 1.0 + jnp.concatenate([gain_ref[i:i + 1] for i in range(dim // LANES)], axis=1)
        hid = hid_ref[...].astype(F32)
        inv = lax.rsqrt(jnp.mean(hid * hid, axis=1, keepdims=True) + NORM_EPS)
        n_buf[...] = hid * inv
        x_buf[...] = (n_buf[...] * w_ref[...]).astype(BF16)
        inv_buf[...] = jnp.broadcast_to(inv, (tokens, LANES))
        pay[...] = n_buf[my_few]
        square[...] = jnp.zeros((LANES, LANES), F32)
        square[0:1, 0:tokens] = mask_in[...]
        mask_own[...] = square[0:few]
        mask_col = jnp.transpose(square[...])[0:tokens, 0:1]
        pay_sends, pay_came = to_dp(pay, pay_got, 0)
        start(pay_sends)
        pay_got[me] = pay[...]
        mask_sends, mask_came = to_dp(mask_own, mask_got, 1, pl.ds(0, 1))
        start(mask_sends)
        mask_got[me] = mask_own[...]
        for k in range(few_first, N_DP):
            weigh(k)
            issue(k)

        def keep(r, _):
            here, there = aligned(me * tokens + r * pack, pack, pack), aligned(r * pack, pack, pack)
            got_soon[0, there] = sends[here, :late]
            got_late[0, there] = sends[here, late:]
            return 0

        lax.fori_loop(0, tokens // pack, keep, 0)

        def student(slot):
            z = lax.dot_general(x_buf[...], tabs[slot], ROWS_BY_ROWS, preferred_element_type=F32)
            ratio = jnp.tanh(z * INV_CAP)
            return ratio, jnp.exp(SOFT_CAP * ratio - SOFT_CAP)

        def next_tiles(i):
            for c in range(per):
                tab_copy(i * per + c).wait()

            @pl.when(i + 1 < 2 * N_DP)
            def _():
                for c in range(per):
                    tab_copy((i + 1) * per + c).start()

            return [lax.rem(i, 2) * per + c for c in range(per)]

        def forward(i, sums):
            s_sum, k_sum = sums
            slots = next_tiles(i)
            for c in range(per):
                ratio, stu = student(slots[c])
                tea = sends[aligned(i * tokens, tokens, tokens), pl.ds(c * sub, sub)]
                s_sum, k_sum = s_sum + fold(stu), k_sum + fold(tea * ratio)
            return s_sum, k_sum

        zero = jnp.zeros((tokens, LANES), F32)
        s_sum, k_sum = lax.fori_loop(0, N_DP, forward, (zero, zero))
        lane = lax.broadcasted_iota(jnp.int32, (tokens, LANES), 1)
        sums = jnp.where(lane == 0, jnp.sum(s_sum, axis=1, keepdims=True), 0.0)
        sums = jnp.where(lane == 1, jnp.sum(t_acc[...], axis=1, keepdims=True), sums)
        sums = jnp.where(lane == AWAY, SOFT_CAP * jnp.sum(c_acc[...] - k_sum, axis=1, keepdims=True), sums)
        own_col[...] = sums
        tp_got[col] = sums
        tp_sends, tp_came = to_tp(lambda c: own_col, tp_got, 0)
        start(tp_sends)
        arrive(tp_came)
        total = added(tp_got)
        square[0:tokens] = jnp.where(lane == DOWN, mask_col, total)
        line = jnp.transpose(square[...])[0:few]
        own_row[...] = line
        all_ref[me] = line
        dp_sends, dp_came = to_dp(own_row, all_ref, 2)
        start(dp_sends)
        twin = col + 1 - 2 * lax.rem(col, 2)
        arrive((*pay_came, *mask_came))
        x_got[col] = pay_got[...]

        def across(j, origin):
            return remote(pay_got, x_got.at[origin], tp_sem.at[1, 0, mates[j]], tp_sem.at[1, 1, origin], me, mates[j])

        def to_twin(j, origin):
            return remote(x_got.at[origin], x_got.at[origin], tp_sem.at[1, 0, mates[j + 1]], tp_sem.at[1, 1, origin], me, twin)

        evens = range(0, N_TP, 2)
        xt_sends = [across(j, col) for j in evens[1:]]
        start(xt_sends)
        came(0)
        onward(1, True, None)
        onward(1, False, 0)

        count = jnp.sum(added(mask_got, slice(1)), axis=1, keepdims=True)
        inv_s, inv_t, weight = 1.0 / total[:, 0:1], 1.0 / total[:, 1:2], mask_col / count
        dx[...] = jnp.zeros((tokens, dim), F32)

        def backward(i, _):
            slots = next_tiles(i)
            total = dx[...]
            for c in range(per):
                ratio, stu = student(slots[c])
                tea = sends[aligned((i - N_DP) * tokens, tokens, tokens), pl.ds(c * sub, sub)]
                diff = (stu * inv_s - tea * inv_t) * weight
                g = (diff * (1.0 - ratio * ratio)).astype(BF16)
                total = total + jnp.dot(g, tabs[slots[c]], preferred_element_type=F32)
            dx[...] = total
            return 0

        lax.fori_loop(N_DP, 2 * N_DP, backward, 0)
        came(1)
        onward(2, True, 0)
        onward(1, False, 1)
        arrive([across(j, mates[j]) for j in evens[1:]])
        twin_sends = [to_twin(j, mates[j]) for j in evens]
        start(twin_sends)

        rs_got[col] = dx[my_few]
        rs_sends, rs_came = to_tp(lambda c: dx.at[aligned(c * few, few, few)], rs_got, 2)
        start(rs_sends)
        arrive(rs_came)
        my_x = added(rs_got)
        my_n = n_buf[my_few]
        grad_n = my_x * w_ref[...]
        my_h = inv_buf[my_few, 0:1] * (grad_n - my_n * jnp.mean(grad_n * my_n, axis=1, keepdims=True))
        ag_own[...] = jnp.zeros((2 * few, dim), F32)
        ag_own[0:few] = my_h
        ag_own[few:few + 1] = jnp.sum(my_x * my_n, axis=0, keepdims=True)
        ag_got[col] = ag_own[...]
        ag_sends, ag_came = to_tp(lambda c: ag_own, ag_got, DOWN)
        start(ag_sends)
        arrive(ag_came)
        gh_ref[...] = jnp.concatenate([ag_got[j, 0:few] for j in range(N_TP)], axis=0)
        line = added(ag_got, slice(few, few + 1))
        gn_own[0:1] = line
        gn_got[me, 0:1] = line
        gn_sends, gn_came = to_dp(gn_own, gn_got, DOWN, pl.ds(0, 1))
        start(gn_sends)

        came(2, 0)
        onward(DOWN, True, 0)
        onward(2, True, 1)
        arrive([to_twin(j, mates[j + 1]) for j in evens])

        def widen(d, _):
            rows = jnp.concatenate([x_got[j, d] for j in range(N_TP)], axis=0)
            x_out[aligned(d * tokens, tokens, tokens)] = (rows * w_ref[...]).astype(BF16)
            return 0

        lax.fori_loop(0, N_DP, widen, 0)
        arrive(dp_came)
        row = lax.broadcasted_iota(jnp.int32, (few, LANES), 0)
        lanes = lax.broadcasted_iota(jnp.int32, (few, LANES), 1)
        for d in range(N_DP):
            block = all_ref[d]
            safe = jnp.where((row < AWAY) & (lanes < tokens), block, 1.0)
            rel[d * few:(d + 1) * few] = jnp.where(row < AWAY, 1.0 / safe, block / count)
        for k, (dz, dy) in enumerate(OFFSETS):
            square[k * few:(k + 1) * few] = rel[aligned(at[-dz, -dy] * few, few, few)]
        coef_ref[...] = jnp.transpose(square[...])

        own_tab.wait()
        for j, path in enumerate(PATHS):
            hop(j, len(path) - 1, 0).wait_recv()
        for j, level, w in COPIES:
            if level == 0:
                hop(j, level, w).wait_send()

        def block(b, _):
            @pl.when(b == 1)
            def _():
                came(2, 1)
                onward(DOWN, True, 1)

            grad_block(at, got_soon, x_out, tab_out[aligned(b * sub, sub)], coef_ref, sends, g_buf, blocks_ref, b)
            return 0

        lax.fori_loop(0, 2, block, 0)
        arrive(gn_came)
        gg_ref[...] = added(gn_got, slice(1))
        for j, path in enumerate(PATHS):
            hop(j, len(path) - 1, 1).wait_recv()
        for j, level, w in COPIES:
            if level:
                hop(j, level, w).wait_send()
        for cp in (*pay_sends, *mask_sends, *tp_sends, *dp_sends, *xt_sends, *twin_sends, *rs_sends, *ag_sends, *gn_sends):
            cp.wait_send()

    dma = pltpu.SemaphoreType.DMA
    wide, flat = (tokens, dim), (few, LANES)
    return pl.pallas_call(
        kern,
        out_shape=tuple(jax.ShapeDtypeStruct(shape, kind) for shape, kind in (
            ((N_DP, tokens, part // 2), F32), ((2, sub, dim), F32), ((N_DP * tokens, dim), BF16), ((part, dim), BF16), ((LANES, LANES), F32), ((N_DP, *flat), F32), (wide, F32),
            ((1, dim), F32))),
        in_specs=[HB] * 5, out_specs=(VM,) * 8,
        scratch_shapes=[pltpu.VMEM(shape, kind) for shape, kind in (
            (wide, BF16), ((dim // LANES, LANES), F32), ((1, tokens), F32), ((1, dim), F32), ((ring * tokens, part), BF16), ((N_DP * tokens, part), F32),
            ((len(MIDDLE), half, part), F32), ((N_DP, tokens, part // 2), F32), ((N_DP * tokens, sub), BF16), ((tokens, LANES), F32), ((tokens, LANES), F32),
            ((depth, sub, dim), BF16), (wide, F32), (wide, BF16), ((tokens, LANES), F32), ((LANES, LANES), F32), ((few, dim), F32),
            ((N_DP, few, dim), F32), (flat, F32), ((N_DP, *flat), F32), ((N_TP, N_DP, few, dim), F32), ((N_TP, tokens, LANES), F32),
            ((tokens, LANES), F32), (flat, F32), ((LANES, LANES), F32), (wide, F32), ((N_TP, few, dim), F32), ((2 * few, dim), F32),
            ((N_TP, 2 * few, dim), F32), ((few, dim), F32), ((N_DP, few, dim), F32))] + [
            dma((N_DP,)), dma((depth,)), dma((5,)), dma((2, len(COPIES))), dma((SIDE, 2, N_DP)), dma((SIDE, 2, N_TP))],
        compiler_params=pltpu.CompilerParams(collective_id=0, has_side_effects=True, vmem_limit_bytes=L_FRONT * MIB),
        cost_estimate=pl.CostEstimate(flops=3 * 10 ** 9, bytes_accessed=100 * MIB, transcendentals=0), name='front')(
            *(pltpu.with_memory_space_constraint(a, pltpu.HBM) for a in (hidden, gain_row, mask_row, teacher, table)))


def finish(teas, x_all, tab_part, coef):
    n, tokens, late = teas.shape
    dim = x_all.shape[1]
    span = late // 2

    def kern(tea_ref, x_ref, tab_ref, coef_ref, out_ref, z_buf, g_buf):
        at = peers()[1]

        def block(b, _):
            grad_block(at, tea_ref, x_ref, tab_ref[aligned(late + b * span, span)], coef_ref, z_buf, g_buf, out_ref, b)
            return 0

        lax.fori_loop(0, 2, block, 0)

    return pl.pallas_call(kern, out_shape=jax.ShapeDtypeStruct((2, span, dim), F32), in_specs=[VM] * 4, out_specs=VM,
        scratch_shapes=[pltpu.VMEM((n * tokens, span), F32), pltpu.VMEM((n * tokens, span), BF16)], name='finish',
        compiler_params=pltpu.CompilerParams(vmem_limit_bytes=22 * MIB),
        cost_estimate=pl.CostEstimate(flops=10 ** 9, bytes_accessed=8 * MIB, transcendentals=0))(teas, x_all, tab_part, coef)


def place(table, pieces, vocab):
    arrays = [p[0] for p in pieces]
    n = len(arrays)
    dim = arrays[0].shape[1]
    rows = vocab // N_DP
    quarter = rows // SIDE
    cut = 256
    chunks = [(i, r) for i in range(n) for r in range(0, arrays[i].shape[0], cut)]

    def kern(*refs):
        dst, buf, sem = refs[-DOWN:]
        at = peers()[1]
        reads, writes = [], []
        for k, (i, r) in enumerate(chunks):
            _, dz, dy, kind, half = pieces[i]
            first = (2 * (half + r // quarter) + kind) * quarter + r % quarter
            there = aligned(at[dz, dy] * rows + first, cut, cut)
            reads.append(pltpu.make_async_copy(refs[i].at[pl.ds(r, cut)], buf.at[k], sem.at[0, k]))
            writes.append(pltpu.make_async_copy(buf.at[k], dst.at[there], sem.at[1, k]))
        for cp in reads:
            cp.start()
        for read, write in zip(reads, writes):
            read.wait()
            write.start()
        for cp in writes:
            cp.wait()

    args = arrays if table is None else [*arrays, table]
    size = len(chunks) * cut * dim
    return pl.pallas_call(kern, out_shape=jax.ShapeDtypeStruct((vocab, dim), F32), in_specs=[pl.BlockSpec(memory_space=pl.ANY)] * n + [HB] * (len(args) - n),
        out_specs=HB, scratch_shapes=[pltpu.VMEM((len(chunks), cut, dim), F32), pltpu.SemaphoreType.DMA((2, len(chunks)))],
        input_output_aliases={} if table is None else {n: 0}, name='place', compiler_params=pltpu.CompilerParams(vmem_limit_bytes=4 * size + MIB),
        cost_estimate=pl.CostEstimate(flops=10 * MIB, bytes_accessed=8 * size, transcendentals=0))(*args)


def gather(first, rest, vocab):
    quarter = first[0].shape[0]
    sets, ways = range(2), (UP, DOWN)
    table, event = None, 0

    def send(pair, axis, step):
        out = []
        for k in sets:
            dz, dy = (step, 0) if axis == k else (0, step)
            out.append(lax.ppermute(pair[k], 'dp', [(d, shift(d, dz, dy)) for d in range(N_DP)]))
        return out

    def put(pair, a, b, c=0):
        return [(pair[k], *((b, a) if k else (a, b)), k, c) for k in sets]

    def settle(*pieces):
        nonlocal table
        table = place(table, [p for ps in pieces for p in ps], vocab)

    def wait(*pairs):
        nonlocal table, event
        event += 1
        table, *flat = lax.optimization_barrier((table, *(x for pair in pairs for x in pair)))
        return [flat[2 * i:2 * i + 2] for i in range(len(pairs))]

    def join(one, other):
        return [jnp.concatenate(pair) for pair in zip(one, other)]

    own = [first]
    low, high = ([send(own[0], 0, way)] for way in ways)
    later = rest()
    event = 1
    own.append([later[k] for k in sets])
    low.append(send(own[1], 0, UP))
    high.append(send(own[1], 0, DOWN))
    whole = join(*own)
    side = {way: send(whole, 1, way) for way in ways}
    settle(put(own[0], 0, 0, 0), put(own[1], 0, 0, 1))

    low[0], high[0] = wait(low[0], high[0])
    far_low = send(low[0], 0, UP)
    settle(put(low[0], DOWN, 0, 0), put(high[0], UP, 0, 0))

    low[1], high[1] = wait(low[1], high[1])
    far_high = send(high[1], 0, DOWN)
    low_whole, high_whole = join(*low), join(*high)
    low_side = {way: send(low_whole, 1, way) for way in ways}
    settle(put(low[1], DOWN, 0, 1), put(high[1], UP, 0, 1))

    side[UP], side[DOWN], high_whole = wait(side[UP], side[DOWN], high_whole)
    high_side = {way: send(high_whole, 1, way) for way in ways}
    side_far = send(side[UP], 1, UP)
    settle(put(side[UP], 0, DOWN))
    settle(put(side[DOWN], 0, UP))

    far_low, far_high = wait(far_low, far_high)
    far_side = {(c, way): send(pair, 1, way) for way in ways for c, pair in enumerate((far_low, far_high))}
    settle(put(far_low, AWAY, 0, 0), put(far_high, AWAY, 0, 1))

    low_side[UP], low_side[DOWN] = wait(low_side[UP], low_side[DOWN])
    low_far = send(low_side[DOWN], 1, DOWN)
    settle(put(low_side[UP], DOWN, DOWN))
    settle(put(low_side[DOWN], DOWN, UP))

    high_side[UP], high_side[DOWN] = wait(high_side[UP], high_side[DOWN])
    high_far = [send([x[:quarter] for x in high_side[UP]], 1, UP), send([x[quarter:] for x in high_side[DOWN]], 1, DOWN)]
    settle(put(high_side[UP], UP, DOWN))
    settle(put(high_side[DOWN], UP, UP))

    far_side[0, DOWN], far_side[1, DOWN], side_far = wait(far_side[0, DOWN], far_side[1, DOWN], side_far)
    last_down = send(far_side[1, DOWN], 1, DOWN)
    settle(put(far_side[0, DOWN], AWAY, UP, 0), put(far_side[1, DOWN], AWAY, UP, 1))
    settle(put(side_far, 0, AWAY))

    far_side[0, UP], = wait(far_side[0, UP])
    last_up = send(far_side[0, UP], 1, UP)
    settle(put(far_side[0, UP], AWAY, DOWN, 0))

    far_side[1, UP], low_far = wait(far_side[1, UP], low_far)
    settle(put(far_side[1, UP], AWAY, DOWN, 1))
    settle(put(low_far, DOWN, AWAY))

    high_far = wait(*high_far)
    settle(put(high_far[0], UP, AWAY, 0), put(high_far[1], UP, AWAY, 1))
    last_up, last_down = wait(last_up, last_down)
    settle(put(last_up, AWAY, AWAY, 0), put(last_down, AWAY, AWAY, 1))
    return table


def solution(mesh):
    def local_step(hid_rows, w_final, tab_rows, tea_rows, mask_rows):
        tokens = hid_rows.shape[0]
        late, soon, x_all, tab_part, coef, stats, grad_h, gain_line = front(hid_rows, w_final.reshape(-1, LANES), mask_rows[None], tea_rows, tab_rows)
        coef, *first = lax.optimization_barrier((coef, soon[0], soon[1]))
        table = gather(first, lambda: finish(late, x_all, tab_part, coef), tab_rows.shape[0])
        s_sum, t_sum, k_sum, masks = (stats[:, i, :tokens] for i in range(SIDE))
        all_kl = k_sum / t_sum + jnp.log(s_sum) - jnp.log(t_sum)
        loss_val = jnp.sum(masks * all_kl) / jnp.sum(masks)
        return loss_val, grad_h.astype(BF16), gain_line[0], table

    return jax.shard_map(local_step, mesh=mesh, in_specs=(P('dp', None), P(None), P('tp', None), P('dp', 'tp'), P('dp')), out_specs=(P(), P('dp', None), P(None), P('tp', None)), check_vma=False)
```

```python
import jax
import jax.numpy as jnp
from jax import lax
from jax.experimental import pallas as pl
from jax.experimental.pallas import tpu as pltpu
from jax.sharding import PartitionSpec as P


SOFT_CAP = 30.0
INV_CAP = 1.0 / SOFT_CAP
NORM_EPS = 1e-6
SIDE, N_DP, N_TP, LANES = 4, 16, 8, 128
UP, DOWN, AWAY = 1, 3, 2
MIB = 2 ** 20
L_FRONT = 41
MESH = pl.DeviceIdType.MESH
VM = pl.BlockSpec(memory_space=pltpu.VMEM)
HB = pl.BlockSpec(memory_space=pltpu.HBM)
F32, BF16 = jnp.float32, jnp.bfloat16
ROWS_BY_ROWS = (((1,), (1,)), ((), ()))
COLS_BY_COLS = (((0,), (0,)), ((), ()))

OFFSETS = tuple((dz, dy) for dz in range(SIDE) for dy in range(SIDE))
ORDER = tuple(sorted(OFFSETS, key=lambda o: -sum(min(d, SIDE - d) for d in o)))


def shift(dp, dz, dy):
    return (dp // SIDE + dz + SIDE) % SIDE * SIDE + (dp % SIDE + dy + SIDE) % SIDE


def peers():
    me = lax.axis_index('dp')
    z, y = lax.div(me, SIDE), lax.rem(me, SIDE)
    zs = [lax.rem(z + d, SIDE) * SIDE for d in range(SIDE)]
    ys = [lax.rem(y + d, SIDE) for d in range(SIDE)]
    return me, {(dz, dy): zs[dz] + ys[dy] for dz in range(-DOWN, SIDE) for dy in range(-DOWN, SIDE)}


def aligned(start, size, unit=LANES):
    return pl.ds(pl.multiple_of(start, unit), size)


def hops(kind, dz, dy):
    along_z = [(dz, 0)] if dz % 2 else [(UP if dy < AWAY else DOWN, 0)] * dz
    along_y = [(0, dy)] if dy % 2 else [(0, UP if dz < AWAY else DOWN)] * dy
    return along_y + along_z if kind else along_z + along_y


JOBS = tuple((kind, o) for o in ORDER[:-1] for kind in range(2))
PATHS = tuple(hops(kind, *o) for kind, o in JOBS)
MIDDLE = tuple((j, level) for level in range(SIDE) for j, path in enumerate(PATHS) if len(path) > level + 1)


def waves(j, level):
    return (None,) if (j, level) in MIDDLE and level < 2 else (0, 1)


def grad_block(at, tea_ref, x_ref, tab_rows, coef_ref, z_buf, g_buf, out_ref, block):
    tokens = tea_ref.shape[1]
    span = tab_rows.shape[0]
    few = LANES // N_DP
    cols = aligned(block * span, span)
    z_buf[:, :span] = lax.dot_general(x_ref[...], tab_rows, ROWS_BY_ROWS, preferred_element_type=F32)
    for k, (dz, dy) in enumerate(OFFSETS):
        here = aligned(at[-dz, -dy] * tokens, tokens, tokens)
        ratio = jnp.tanh(z_buf[here, :span] * INV_CAP)
        stu = jnp.exp(SOFT_CAP * ratio - SOFT_CAP)
        inv_s, inv_t, _, weight = (coef_ref[0:tokens, k * few + i:k * few + i + 1] for i in range(SIDE))
        diff = (stu * inv_s - tea_ref[k, :, cols] * inv_t) * weight
        g_buf[here, :span] = (diff * (1.0 - ratio * ratio)).astype(BF16)
    out_ref[block] = lax.dot_general(g_buf[:, :span], x_ref[...], COLS_BY_COLS, preferred_element_type=F32)


def front(hidden, gain_row, mask_row, teacher, table):
    tokens, vocab = teacher.shape
    dim = hidden.shape[1]
    part = vocab // N_DP
    half = tokens // 2
    few = tokens // N_TP
    pack = 16
    sub = 512
    per = part // sub
    tiles = vocab // sub
    depth = 2 * per
    ring = N_DP // 2
    few_first = 3

    def kern(hid_hbm, gain_hbm, mask_hbm, tea_ref, tab_ref, got_late, blocks_ref, x_out, tab_out, coef_ref, all_ref, gh_ref, gg_ref,
             hid_ref, gain_ref, mask_in, w_ref, raw, sends, stage, got_soon, g_buf, t_acc, c_acc, tabs, n_buf, x_buf, inv_buf, square, pay, pay_got, mask_own, mask_got, x_got, tp_got, own_col,
             own_row, rel, dx, rs_got, ag_own, ag_got, gn_own, gn_got, raw_sem, tab_sem, in_sem, hop_out, hop_in, dp_sem, tp_sem):
        me, at = peers()
        col = lax.axis_index('tp')
        mates = [lax.rem(col + j, N_TP) for j in range(N_TP)]
        my_few = aligned(col * few, few, few)

        def fetch(k):
            d = at[ORDER[k]]
            return pltpu.make_async_copy(tea_ref.at[:, aligned(d * part, part)], raw.at[pl.ds(k % ring * tokens, tokens)], raw_sem.at[k % ring])

        def tab_copy(i):
            slot = lax.rem(i, depth)
            return pltpu.make_async_copy(tab_ref.at[aligned(lax.rem(i, tiles) * sub, sub)], tabs.at[slot], tab_sem.at[slot])

        inputs = [pltpu.make_async_copy(src, dst, in_sem.at[2 + i])
                  for i, (src, dst) in enumerate(((hid_hbm, hid_ref), (gain_hbm, gain_ref), (mask_hbm, mask_in)))]
        own_tab = pltpu.make_async_copy(tab_ref.at[aligned(me * part, part)], tab_out, in_sem.at[1])
        for cp in inputs:
            cp.start()
        for k in range(ring):
            fetch(k).start()
        for i in range(per):
            tab_copy(i).start()
        own_tab.start()
        barrier = pltpu.get_barrier_semaphore()
        for dz, dy in ORDER[:-1]:
            pl.semaphore_signal(barrier, inc=1, device_id=(at[dz, dy], col), device_id_type=MESH)
        for j in range(1, N_TP):
            pl.semaphore_signal(barrier, inc=1, device_id=(me, mates[j]), device_id_type=MESH)

        def fold(v):
            total = v[:, :LANES]
            for c in range(LANES, v.shape[1], LANES):
                total = total + v[:, c:c + LANES]
            return total

        def weigh(k):
            fetch(k).wait()
            d = at[ORDER[k]]

            def rows(r, _):
                here = aligned(r * pack, pack, pack)
                cap = jnp.tanh(raw[aligned(k % ring * tokens + r * pack, pack, pack)].astype(F32) * INV_CAP)
                tea = jnp.exp(SOFT_CAP * cap - SOFT_CAP)
                sends[aligned(d * tokens + r * pack, pack, pack)] = tea
                t_acc[here] += fold(tea)
                c_acc[here] += fold(tea * cap)
                return 0

            lax.fori_loop(0, tokens // pack, rows, 0)
            if k + ring < N_DP:
                fetch(k + ring).start()

        t_acc[...] = jnp.zeros((tokens, LANES), F32)
        c_acc[...] = jnp.zeros((tokens, LANES), F32)
        weigh(0)
        pl.semaphore_wait(barrier, N_DP + N_TP - 2)

        def remote(src, dst, out, into, dp, tp):
            return pltpu.make_async_remote_copy(src_ref=src, dst_ref=dst, send_sem=out, recv_sem=into, device_id=(dp, tp), device_id_type=MESH)

        def whole(ref, sem):
            pltpu.make_async_copy(ref, ref, sem).wait()

        def to_dp(src, dst, x, rows=slice(None)):
            for o in ORDER[:-1]:
                remote(src.at[rows], dst.at[me, rows], dp_sem.at[x, 0], dp_sem.at[x, 1], at[o], col).start()
            others = dst.at[pl.ds(0, N_DP - 1), rows]
            return [(others, dp_sem.at[x, 0])], lambda: whole(others, dp_sem.at[x, 1])

        def to_tp(srcs, dst, x):
            for c in mates[1:]:
                remote(srcs(c), dst.at[col], tp_sem.at[x, 0], tp_sem.at[x, 1], me, c).start()
            others = dst.at[pl.ds(0, N_TP - 1)]
            return [(others, tp_sem.at[x, 0])], lambda: whole(others, tp_sem.at[x, 1])

        def added(ref, here=slice(None)):
            total = ref[0, here]
            for d in range(1, ref.shape[0]):
                total = total + ref[d, here]
            return total

        gots = (got_soon, got_late)
        late = part // 2

        def hop(j, level, w):
            kind, (dz, dy) = JOBS[j]
            tok = pl.ds(kind * half, half)
            rows = slice(None) if w is None else pl.ds(w * late, late)
            src = stage.at[MIDDLE.index((j, level - 1)), :, rows] if level else sends.at[aligned(at[dz, dy] * tokens + kind * half, half, half), rows]
            dst = stage.at[MIDDLE.index((j, level)), :, rows] if (j, level) in MIDDLE else gots[w].at[dz * SIDE + dy, tok]
            into = (level if w is None else level + w) if (j, level) in MIDDLE else SIDE + w
            return remote(src, dst, hop_out.at[min(level, 1)], hop_in.at[into], at[PATHS[j][level]], col)

        def came(level, w=None):
            n = sum(at == level for _, at in MIDDLE)
            rows = slice(None) if w is None else pl.ds(0, late)
            whole(stage.at[pl.ds(0, n), :, rows], hop_in.at[level + (w or 0)])

        def onward(level, far, *ws):
            for w in ws:
                for j, at in MIDDLE:
                    if at == level - 1 and far == (len(PATHS[j]) > 2):
                        hop(j, level, w).start()

        def issue(k):
            for j, (_, to) in enumerate(JOBS):
                if to == ORDER[k]:
                    for w in waves(j, 0):
                        hop(j, 0, w).start()

        issue(0)
        for k in range(1, few_first):
            weigh(k)
            issue(k)
        for cp in inputs:
            cp.wait()
        w_ref[...] = 1.0 + jnp.concatenate([gain_ref[i:i + 1] for i in range(dim // LANES)], axis=1)
        hid = hid_ref[...].astype(F32)
        inv = lax.rsqrt(jnp.mean(hid * hid, axis=1, keepdims=True) + NORM_EPS)
        n_buf[...] = hid * inv
        x_buf[...] = (n_buf[...] * w_ref[...]).astype(BF16)
        inv_buf[...] = jnp.broadcast_to(inv, (tokens, LANES))
        pay[...] = n_buf[my_few]
        square[...] = jnp.zeros((LANES, LANES), F32)
        square[0:1, 0:tokens] = mask_in[...]
        mask_own[...] = square[0:few]
        mask_col = jnp.transpose(square[...])[0:tokens, 0:1]
        pay_sent, pay_came = to_dp(pay, pay_got, 0)
        pay_got[me] = pay[...]
        mask_sent, mask_came = to_dp(mask_own, mask_got, 1, pl.ds(0, 1))
        mask_got[me] = mask_own[...]
        for k in range(few_first, N_DP):
            weigh(k)
            issue(k)

        def keep(r, _):
            here, there = aligned(me * tokens + r * pack, pack, pack), aligned(r * pack, pack, pack)
            got_soon[0, there] = sends[here, :late]
            got_late[0, there] = sends[here, late:]
            return 0

        lax.fori_loop(0, tokens // pack, keep, 0)

        def student(slot):
            z = lax.dot_general(x_buf[...], tabs[slot], ROWS_BY_ROWS, preferred_element_type=F32)
            ratio = jnp.tanh(z * INV_CAP)
            return ratio, jnp.exp(SOFT_CAP * ratio - SOFT_CAP)

        def next_tiles(i):
            for c in range(per):
                tab_copy(i * per + c).wait()

            @pl.when(i + 1 < 2 * N_DP)
            def _():
                for c in range(per):
                    tab_copy((i + 1) * per + c).start()

            return [lax.rem(i, 2) * per + c for c in range(per)]

        def forward(i, sums):
            s_sum, k_sum = sums
            slots = next_tiles(i)
            for c in range(per):
                ratio, stu = student(slots[c])
                tea = sends[aligned(i * tokens, tokens, tokens), pl.ds(c * sub, sub)]
                s_sum, k_sum = s_sum + fold(stu), k_sum + fold(tea * ratio)
            return s_sum, k_sum

        zero = jnp.zeros((tokens, LANES), F32)
        s_sum, k_sum = lax.fori_loop(0, N_DP, forward, (zero, zero))
        lane = lax.broadcasted_iota(jnp.int32, (tokens, LANES), 1)
        sums = jnp.where(lane == 0, jnp.sum(s_sum, axis=1, keepdims=True), 0.0)
        sums = jnp.where(lane == 1, jnp.sum(t_acc[...], axis=1, keepdims=True), sums)
        sums = jnp.where(lane == AWAY, SOFT_CAP * jnp.sum(c_acc[...] - k_sum, axis=1, keepdims=True), sums)
        own_col[...] = sums
        tp_got[col] = sums
        tp_sent, tp_came = to_tp(lambda c: own_col, tp_got, 0)
        tp_came()
        total = added(tp_got)
        square[0:tokens] = jnp.where(lane == DOWN, mask_col, total)
        line = jnp.transpose(square[...])[0:few]
        own_row[...] = line
        all_ref[me] = line
        dp_sent, dp_came = to_dp(own_row, all_ref, 2)
        twin = col + 1 - 2 * lax.rem(col, 2)
        pay_came()
        mask_came()
        x_got[col] = pay_got[...]

        evens = range(0, N_TP, 2)
        for j in evens[1:]:
            remote(pay_got, x_got.at[col], tp_sem.at[1, 0], tp_sem.at[1, 1], me, mates[j]).start()
        came(0)
        onward(1, True, None)
        onward(1, False, 0)

        count = jnp.sum(added(mask_got, slice(1)), axis=1, keepdims=True)
        inv_s, inv_t, weight = 1.0 / total[:, 0:1], 1.0 / total[:, 1:2], mask_col / count
        dx[...] = jnp.zeros((tokens, dim), F32)

        def backward(i, _):
            slots = next_tiles(i)
            total = dx[...]
            for c in range(per):
                ratio, stu = student(slots[c])
                tea = sends[aligned((i - N_DP) * tokens, tokens, tokens), pl.ds(c * sub, sub)]
                diff = (stu * inv_s - tea * inv_t) * weight
                g = (diff * (1.0 - ratio * ratio)).astype(BF16)
                total = total + jnp.dot(g, tabs[slots[c]], preferred_element_type=F32)
            dx[...] = total
            return 0

        lax.fori_loop(N_DP, 2 * N_DP, backward, 0)
        came(1)
        onward(2, True, 0)
        onward(1, False, 1)
        whole(x_got.at[pl.ds(0, SIDE - 1)], tp_sem.at[1, 1])
        for j in evens:
            remote(x_got.at[mates[j]], x_got.at[mates[j]], tp_sem.at[SIDE, 0], tp_sem.at[SIDE, 1], me, twin).start()

        rs_got[col] = dx[my_few]
        rs_sent, rs_came = to_tp(lambda c: dx.at[aligned(c * few, few, few)], rs_got, 2)
        rs_came()
        my_x = added(rs_got)
        my_n = n_buf[my_few]
        grad_n = my_x * w_ref[...]
        my_h = inv_buf[my_few, 0:1] * (grad_n - my_n * jnp.mean(grad_n * my_n, axis=1, keepdims=True))
        ag_own[...] = jnp.zeros((2 * few, dim), F32)
        ag_own[0:few] = my_h
        ag_own[few:few + 1] = jnp.sum(my_x * my_n, axis=0, keepdims=True)
        ag_got[col] = ag_own[...]
        ag_sent, ag_came = to_tp(lambda c: ag_own, ag_got, DOWN)
        ag_came()
        gh_ref[...] = jnp.concatenate([ag_got[j, 0:few] for j in range(N_TP)], axis=0)
        line = added(ag_got, slice(few, few + 1))
        gn_own[0:1] = line
        gn_got[me, 0:1] = line
        gn_sent, gn_came = to_dp(gn_own, gn_got, DOWN, pl.ds(0, 1))

        came(2, 0)
        onward(DOWN, True, 0)
        onward(2, True, 1)
        whole(x_got.at[pl.ds(0, SIDE)], tp_sem.at[SIDE, 1])

        def widen(d, _):
            rows = jnp.concatenate([x_got[j, d] for j in range(N_TP)], axis=0)
            x_out[aligned(d * tokens, tokens, tokens)] = (rows * w_ref[...]).astype(BF16)
            return 0

        lax.fori_loop(0, N_DP, widen, 0)
        dp_came()
        row = lax.broadcasted_iota(jnp.int32, (few, LANES), 0)
        lanes = lax.broadcasted_iota(jnp.int32, (few, LANES), 1)
        for d in range(N_DP):
            block = all_ref[d]
            safe = jnp.where((row < AWAY) & (lanes < tokens), block, 1.0)
            rel[d * few:(d + 1) * few] = jnp.where(row < AWAY, 1.0 / safe, block / count)
        for k, (dz, dy) in enumerate(OFFSETS):
            square[k * few:(k + 1) * few] = rel[aligned(at[-dz, -dy] * few, few, few)]
        coef_ref[...] = jnp.transpose(square[...])

        own_tab.wait()
        whole(got_soon.at[pl.ds(0, N_DP - 1)], hop_in.at[SIDE])
        whole(sends.at[pl.ds(0, len(JOBS) * half)], hop_out.at[0])

        def block(b, _):
            @pl.when(b == 1)
            def _():
                came(2, 1)
                onward(DOWN, True, 1)

            grad_block(at, got_soon, x_out, tab_out[aligned(b * sub, sub)], coef_ref, sends, g_buf, blocks_ref, b)
            return 0

        lax.fori_loop(0, 2, block, 0)
        gn_came()
        gg_ref[...] = added(gn_got, slice(1))
        whole(got_late.at[pl.ds(0, N_DP - 1)], hop_in.at[SIDE + 1])
        whole(stage, hop_out.at[1])
        for ref, sem in (*pay_sent, *mask_sent, *tp_sent, *dp_sent, *rs_sent, *ag_sent, *gn_sent):
            whole(ref, sem)
        whole(x_got.at[pl.ds(0, SIDE - 1)], tp_sem.at[1, 0])
        whole(x_got.at[pl.ds(0, SIDE)], tp_sem.at[SIDE, 0])

    dma = pltpu.SemaphoreType.DMA
    wide, flat = (tokens, dim), (few, LANES)
    return pl.pallas_call(
        kern,
        out_shape=tuple(jax.ShapeDtypeStruct(shape, kind) for shape, kind in (
            ((N_DP, tokens, part // 2), F32), ((2, sub, dim), F32), ((N_DP * tokens, dim), BF16), ((part, dim), BF16), ((LANES, LANES), F32), ((N_DP, *flat), F32), (wide, F32),
            ((1, dim), F32))),
        in_specs=[HB] * 5, out_specs=(VM,) * 8,
        scratch_shapes=[pltpu.VMEM(shape, kind) for shape, kind in (
            (wide, BF16), ((dim // LANES, LANES), F32), ((1, tokens), F32), ((1, dim), F32), ((ring * tokens, part), BF16), ((N_DP * tokens, part), F32),
            ((len(MIDDLE), half, part), F32), ((N_DP, tokens, part // 2), F32), ((N_DP * tokens, sub), BF16), ((tokens, LANES), F32), ((tokens, LANES), F32),
            ((depth, sub, dim), BF16), (wide, F32), (wide, BF16), ((tokens, LANES), F32), ((LANES, LANES), F32), ((few, dim), F32),
            ((N_DP, few, dim), F32), (flat, F32), ((N_DP, *flat), F32), ((N_TP, N_DP, few, dim), F32), ((N_TP, tokens, LANES), F32),
            ((tokens, LANES), F32), (flat, F32), ((LANES, LANES), F32), (wide, F32), ((N_TP, few, dim), F32), ((2 * few, dim), F32),
            ((N_TP, 2 * few, dim), F32), ((few, dim), F32), ((N_DP, few, dim), F32))] + [
            dma((ring,)), dma((depth,)), dma((5,)), dma((2,)), dma((SIDE + 2,)), dma((SIDE, 2)), dma((SIDE + 1, 2))],
        compiler_params=pltpu.CompilerParams(collective_id=0, has_side_effects=True, vmem_limit_bytes=L_FRONT * MIB),
        cost_estimate=pl.CostEstimate(flops=3 * 10 ** 9, bytes_accessed=100 * MIB, transcendentals=0), name='front')(
            *(pltpu.with_memory_space_constraint(a, pltpu.HBM) for a in (hidden, gain_row, mask_row, teacher, table)))


def finish(teas, x_all, tab_part, coef):
    n, tokens, late = teas.shape
    dim = x_all.shape[1]
    span = late // 2

    def kern(tea_ref, x_ref, tab_ref, coef_ref, out_ref, z_buf, g_buf):
        at = peers()[1]

        def block(b, _):
            grad_block(at, tea_ref, x_ref, tab_ref[aligned(late + b * span, span)], coef_ref, z_buf, g_buf, out_ref, b)
            return 0

        lax.fori_loop(0, 2, block, 0)

    return pl.pallas_call(kern, out_shape=jax.ShapeDtypeStruct((2, span, dim), F32), in_specs=[VM] * 4, out_specs=VM,
        scratch_shapes=[pltpu.VMEM((n * tokens, span), F32), pltpu.VMEM((n * tokens, span), BF16)], name='finish',
        compiler_params=pltpu.CompilerParams(vmem_limit_bytes=22 * MIB),
        cost_estimate=pl.CostEstimate(flops=10 ** 9, bytes_accessed=8 * MIB, transcendentals=0))(teas, x_all, tab_part, coef)


def place(table, pieces, vocab):
    arrays = [p[0] for p in pieces]
    n = len(arrays)
    dim = arrays[0].shape[1]
    rows = vocab // N_DP
    quarter = rows // SIDE
    cut = 256
    chunks = [(i, r) for i in range(n) for r in range(0, arrays[i].shape[0], cut)]

    def kern(*refs):
        dst, buf, sem = refs[-DOWN:]
        at = peers()[1]
        reads, writes = [], []
        for k, (i, r) in enumerate(chunks):
            _, dz, dy, kind, half = pieces[i]
            first = (2 * (half + r // quarter) + kind) * quarter + r % quarter
            there = aligned(at[dz, dy] * rows + first, cut, cut)
            reads.append(pltpu.make_async_copy(refs[i].at[pl.ds(r, cut)], buf.at[k], sem.at[0, k]))
            writes.append(pltpu.make_async_copy(buf.at[k], dst.at[there], sem.at[1, k]))
        for cp in reads:
            cp.start()
        for read, write in zip(reads, writes):
            read.wait()
            write.start()
        for cp in writes:
            cp.wait()

    args = arrays if table is None else [*arrays, table]
    size = len(chunks) * cut * dim
    return pl.pallas_call(kern, out_shape=jax.ShapeDtypeStruct((vocab, dim), F32), in_specs=[pl.BlockSpec(memory_space=pl.ANY)] * n + [HB] * (len(args) - n),
        out_specs=HB, scratch_shapes=[pltpu.VMEM((len(chunks), cut, dim), F32), pltpu.SemaphoreType.DMA((2, len(chunks)))],
        input_output_aliases={} if table is None else {n: 0}, name='place', compiler_params=pltpu.CompilerParams(vmem_limit_bytes=4 * size + MIB),
        cost_estimate=pl.CostEstimate(flops=10 * MIB, bytes_accessed=8 * size, transcendentals=0))(*args)


def gather(first, rest, vocab):
    quarter = first[0].shape[0]
    sets, ways = range(2), (UP, DOWN)
    table, event = None, 0

    def send(pair, axis, step):
        out = []
        for k in sets:
            dz, dy = (step, 0) if axis == k else (0, step)
            out.append(lax.ppermute(pair[k], 'dp', [(d, shift(d, dz, dy)) for d in range(N_DP)]))
        return out

    def put(pair, a, b, c=0):
        return [(pair[k], *((b, a) if k else (a, b)), k, c) for k in sets]

    def settle(*pieces):
        nonlocal table
        table = place(table, [p for ps in pieces for p in ps], vocab)

    def wait(*pairs):
        nonlocal table, event
        event += 1
        table, *flat = lax.optimization_barrier((table, *(x for pair in pairs for x in pair)))
        return [flat[2 * i:2 * i + 2] for i in range(len(pairs))]

    def join(one, other):
        return [jnp.concatenate(pair) for pair in zip(one, other)]

    own = [first]
    low, high = ([send(own[0], 0, way)] for way in ways)
    later = rest()
    event = 1
    own.append([later[k] for k in sets])
    low.append(send(own[1], 0, UP))
    high.append(send(own[1], 0, DOWN))
    whole = join(*own)
    side = {way: send(whole, 1, way) for way in ways}
    settle(put(own[0], 0, 0, 0), put(own[1], 0, 0, 1))

    low[0], high[0] = wait(low[0], high[0])
    far_low = send(low[0], 0, UP)
    settle(put(low[0], DOWN, 0, 0), put(high[0], UP, 0, 0))

    low[1], high[1] = wait(low[1], high[1])
    far_high = send(high[1], 0, DOWN)
    low_whole, high_whole = join(*low), join(*high)
    low_side = {way: send(low_whole, 1, way) for way in ways}
    settle(put(low[1], DOWN, 0, 1), put(high[1], UP, 0, 1))

    side[UP], side[DOWN], high_whole = wait(side[UP], side[DOWN], high_whole)
    high_side = {way: send(high_whole, 1, way) for way in ways}
    side_far = send(side[UP], 1, UP)
    settle(put(side[UP], 0, DOWN))
    settle(put(side[DOWN], 0, UP))

    far_low, far_high = wait(far_low, far_high)
    far_side = {(c, way): send(pair, 1, way) for way in ways for c, pair in enumerate((far_low, far_high))}
    settle(put(far_low, AWAY, 0, 0), put(far_high, AWAY, 0, 1))

    low_side[UP], low_side[DOWN] = wait(low_side[UP], low_side[DOWN])
    low_far = send(low_side[DOWN], 1, DOWN)
    settle(put(low_side[UP], DOWN, DOWN))
    settle(put(low_side[DOWN], DOWN, UP))

    high_side[UP], high_side[DOWN] = wait(high_side[UP], high_side[DOWN])
    high_far = [send([x[:quarter] for x in high_side[UP]], 1, UP), send([x[quarter:] for x in high_side[DOWN]], 1, DOWN)]
    settle(put(high_side[UP], UP, DOWN))
    settle(put(high_side[DOWN], UP, UP))

    far_side[0, DOWN], far_side[1, DOWN], side_far = wait(far_side[0, DOWN], far_side[1, DOWN], side_far)
    last_down = send(far_side[1, DOWN], 1, DOWN)
    settle(put(far_side[0, DOWN], AWAY, UP, 0), put(far_side[1, DOWN], AWAY, UP, 1))
    settle(put(side_far, 0, AWAY))

    far_side[0, UP], = wait(far_side[0, UP])
    last_up = send(far_side[0, UP], 1, UP)
    settle(put(far_side[0, UP], AWAY, DOWN, 0))

    far_side[1, UP], low_far = wait(far_side[1, UP], low_far)
    settle(put(far_side[1, UP], AWAY, DOWN, 1))
    settle(put(low_far, DOWN, AWAY))

    high_far = wait(*high_far)
    settle(put(high_far[0], UP, AWAY, 0), put(high_far[1], UP, AWAY, 1))
    last_up, last_down = wait(last_up, last_down)
    settle(put(last_up, AWAY, AWAY, 0), put(last_down, AWAY, AWAY, 1))
    return table


def solution(mesh):
    def local_step(hid_rows, w_final, tab_rows, tea_rows, mask_rows):
        tokens = hid_rows.shape[0]
        late, soon, x_all, tab_part, coef, stats, grad_h, gain_line = front(hid_rows, w_final.reshape(-1, LANES), mask_rows[None], tea_rows, tab_rows)
        coef, *first = lax.optimization_barrier((coef, soon[0], soon[1]))
        table = gather(first, lambda: finish(late, x_all, tab_part, coef), tab_rows.shape[0])
        s_sum, t_sum, k_sum, masks = (stats[:, i, :tokens] for i in range(SIDE))
        all_kl = k_sum / t_sum + jnp.log(s_sum) - jnp.log(t_sum)
        loss_val = jnp.sum(masks * all_kl) / jnp.sum(masks)
        return loss_val, grad_h.astype(BF16), gain_line[0], table

    return jax.shard_map(local_step, mesh=mesh, in_specs=(P('dp', None), P(None), P('tp', None), P('dp', 'tp'), P('dp')), out_specs=(P(), P('dp', None), P(None), P('tp', None)), check_vma=False)
```

```python
import jax
import jax.numpy as jnp
from jax import lax
from jax.experimental import pallas as pl
from jax.experimental.pallas import tpu as pltpu
from jax.sharding import PartitionSpec as P


SOFT_CAP = 30.0
INV_CAP = 1.0 / SOFT_CAP
NORM_EPS = 1e-6
SIDE, N_DP, N_TP, LANES = 4, 16, 8, 128
UP, DOWN, AWAY = 1, 3, 2
MIB = 2 ** 20
L_FRONT = 41
MESH = pl.DeviceIdType.MESH
VM = pl.BlockSpec(memory_space=pltpu.VMEM)
HB = pl.BlockSpec(memory_space=pltpu.HBM)
F32, BF16 = jnp.float32, jnp.bfloat16
ROWS_BY_ROWS = (((1,), (1,)), ((), ()))
COLS_BY_COLS = (((0,), (0,)), ((), ()))

OFFSETS = tuple((dz, dy) for dz in range(SIDE) for dy in range(SIDE))
ORDER = tuple(sorted(OFFSETS, key=lambda o: -sum(min(d, SIDE - d) for d in o)))


def shift(dp, dz, dy):
    return (dp // SIDE + dz + SIDE) % SIDE * SIDE + (dp % SIDE + dy + SIDE) % SIDE


def peers():
    me = lax.axis_index('dp')
    z, y = lax.div(me, SIDE), lax.rem(me, SIDE)
    zs = [lax.rem(z + d, SIDE) * SIDE for d in range(SIDE)]
    ys = [lax.rem(y + d, SIDE) for d in range(SIDE)]
    return me, {(dz, dy): zs[dz] + ys[dy] for dz in range(-DOWN, SIDE) for dy in range(-DOWN, SIDE)}


def aligned(start, size, unit=LANES):
    return pl.ds(pl.multiple_of(start, unit), size)


def hops(kind, dz, dy):
    along_z = [(dz, 0)] if dz % 2 else [(UP if dy < AWAY else DOWN, 0)] * dz
    along_y = [(0, dy)] if dy % 2 else [(0, UP if dz < AWAY else DOWN)] * dy
    return along_y + along_z if kind else along_z + along_y


JOBS = tuple((kind, o) for o in ORDER[:-1] for kind in range(2))
PATHS = tuple(hops(kind, *o) for kind, o in JOBS)
MIDDLE = tuple((j, level) for level in range(SIDE) for j, path in enumerate(PATHS) if len(path) > level + 1)


def waves(j, level):
    return (None,) if (j, level) in MIDDLE and level < 2 else (0, 1)


def grad_block(at, tea_ref, x_ref, tab_rows, coef_ref, z_buf, g_buf, out_ref, block):
    tokens = tea_ref.shape[1]
    span = tab_rows.shape[0]
    few = LANES // N_DP
    cols = aligned(block * span, span)
    z_buf[:, :span] = lax.dot_general(x_ref[...], tab_rows, ROWS_BY_ROWS, preferred_element_type=F32)
    for k, (dz, dy) in enumerate(OFFSETS):
        here = aligned(at[-dz, -dy] * tokens, tokens, tokens)
        ratio = jnp.tanh(z_buf[here, :span] * INV_CAP)
        stu = jnp.exp(SOFT_CAP * ratio - SOFT_CAP)
        inv_s, inv_t, _, weight = (coef_ref[0:tokens, k * few + i:k * few + i + 1] for i in range(SIDE))
        diff = (stu * inv_s - tea_ref[k, :, cols] * inv_t) * weight
        g_buf[here, :span] = (diff * (1.0 - ratio * ratio)).astype(BF16)
    out_ref[block] = lax.dot_general(g_buf[:, :span], x_ref[...], COLS_BY_COLS, preferred_element_type=F32)


def front(hidden, gain_row, mask_row, teacher, table):
    tokens, vocab = teacher.shape
    dim = hidden.shape[1]
    part = vocab // N_DP
    half = tokens // 2
    few = tokens // N_TP
    pack = 16
    sub = 512
    per = part // sub
    tiles = vocab // sub
    depth = 2 * per
    ring = N_DP // 2
    few_first = 3

    def kern(hid_hbm, gain_hbm, mask_hbm, tea_ref, tab_ref, got_late, blocks_ref, x_out, tab_out, coef_ref, all_ref, gh_ref, gg_ref,
             hid_ref, gain_ref, mask_in, w_ref, raw, sends, stage, got_soon, g_buf, t_acc, c_acc, tabs, n_buf, x_buf, inv_buf, square, pay, pay_got, mask_own, mask_got, x_got, tp_got, own_col,
             own_row, rel, dx, rs_got, ag_own, ag_got, gn_own, gn_got, raw_sem, tab_sem, in_sem, hop_out, hop_in, dp_sem, tp_sem):
        me, at = peers()
        col = lax.axis_index('tp')
        mates = [lax.rem(col + j, N_TP) for j in range(N_TP)]
        my_few = aligned(col * few, few, few)

        def fetch(k):
            d = at[ORDER[k]]
            return pltpu.make_async_copy(tea_ref.at[:, aligned(d * part, part)], raw.at[pl.ds(k % ring * tokens, tokens)], raw_sem.at[k % ring])

        def tab_copy(i):
            slot = lax.rem(i, depth)
            return pltpu.make_async_copy(tab_ref.at[aligned(lax.rem(i, tiles) * sub, sub)], tabs.at[slot], tab_sem.at[slot])

        inputs = [pltpu.make_async_copy(src, dst, in_sem.at[2 + i])
                  for i, (src, dst) in enumerate(((hid_hbm, hid_ref), (gain_hbm, gain_ref), (mask_hbm, mask_in)))]
        own_tab = pltpu.make_async_copy(tab_ref.at[aligned(me * part, part)], tab_out, in_sem.at[1])
        for cp in inputs:
            cp.start()
        for k in range(ring):
            fetch(k).start()
        for i in range(per):
            tab_copy(i).start()
        own_tab.start()
        barrier = pltpu.get_barrier_semaphore()
        for dz, dy in ORDER[:-1]:
            pl.semaphore_signal(barrier, inc=1, device_id=(at[dz, dy], col), device_id_type=MESH)
        for j in range(1, N_TP):
            pl.semaphore_signal(barrier, inc=1, device_id=(me, mates[j]), device_id_type=MESH)

        def fold(v):
            total = v[:, :LANES]
            for c in range(LANES, v.shape[1], LANES):
                total = total + v[:, c:c + LANES]
            return total

        def weigh(k):
            fetch(k).wait()
            d = at[ORDER[k]]

            def rows(r, _):
                here = aligned(r * pack, pack, pack)
                cap = jnp.tanh(raw[aligned(k % ring * tokens + r * pack, pack, pack)].astype(F32) * INV_CAP)
                tea = jnp.exp(SOFT_CAP * cap - SOFT_CAP)
                sends[aligned(d * tokens + r * pack, pack, pack)] = tea
                t_acc[here] += fold(tea)
                c_acc[here] += fold(tea * cap)
                return 0

            lax.fori_loop(0, tokens // pack, rows, 0)
            if k + ring < N_DP:
                fetch(k + ring).start()

        t_acc[...] = jnp.zeros((tokens, LANES), F32)
        c_acc[...] = jnp.zeros((tokens, LANES), F32)
        weigh(0)
        pl.semaphore_wait(barrier, N_DP + N_TP - 2)

        def remote(src, dst, out, into, dp, tp):
            return pltpu.make_async_remote_copy(src_ref=src, dst_ref=dst, send_sem=out, recv_sem=into, device_id=(dp, tp), device_id_type=MESH)

        def whole(ref, sem):
            pltpu.make_async_copy(ref, ref, sem).wait()

        def to_dp(src, dst, x, rows=slice(None)):
            for o in ORDER[:-1]:
                remote(src.at[rows], dst.at[me, rows], dp_sem.at[x, 0], dp_sem.at[x, 1], at[o], col).start()
            others = dst.at[pl.ds(0, N_DP - 1), rows]
            return [(others, dp_sem.at[x, 0])], lambda: whole(others, dp_sem.at[x, 1])

        def to_tp(srcs, dst, x):
            for c in mates[1:]:
                remote(srcs(c), dst.at[col], tp_sem.at[x, 0], tp_sem.at[x, 1], me, c).start()
            others = dst.at[pl.ds(0, N_TP - 1)]
            return [(others, tp_sem.at[x, 0])], lambda: whole(others, tp_sem.at[x, 1])

        def added(ref, here=slice(None)):
            total = ref[0, here]
            for d in range(1, ref.shape[0]):
                total = total + ref[d, here]
            return total

        gots = (got_soon, got_late)
        late = part // 2

        def hop(j, level, w):
            kind, (dz, dy) = JOBS[j]
            tok = pl.ds(kind * half, half)
            rows = slice(None) if w is None else pl.ds(w * late, late)
            src = stage.at[MIDDLE.index((j, level - 1)), :, rows] if level else sends.at[aligned(at[dz, dy] * tokens + kind * half, half, half), rows]
            dst = stage.at[MIDDLE.index((j, level)), :, rows] if (j, level) in MIDDLE else gots[w].at[dz * SIDE + dy, tok]
            into = (level if w is None else level + w) if (j, level) in MIDDLE else SIDE + w
            return remote(src, dst, hop_out.at[min(level, 1)], hop_in.at[into], at[PATHS[j][level]], col)

        def came(level, w=None):
            n = sum(at == level for _, at in MIDDLE)
            rows = slice(None) if w is None else pl.ds(0, late)
            whole(stage.at[pl.ds(0, n), :, rows], hop_in.at[level + (w or 0)])

        def onward(level, far, *ws):
            for w in ws:
                for j, at in MIDDLE:
                    if at == level - 1 and far == (len(PATHS[j]) > 2):
                        hop(j, level, w).start()

        def issue(k):
            for j, (_, to) in enumerate(JOBS):
                if to == ORDER[k]:
                    for w in waves(j, 0):
                        hop(j, 0, w).start()

        issue(0)
        for k in range(1, few_first):
            weigh(k)
            issue(k)
        for cp in inputs:
            cp.wait()
        w_ref[...] = 1.0 + jnp.concatenate([gain_ref[i:i + 1] for i in range(dim // LANES)], axis=1)
        hid = hid_ref[...].astype(F32)
        inv = lax.rsqrt(jnp.mean(hid * hid, axis=1, keepdims=True) + NORM_EPS)
        n_buf[...] = hid * inv
        x_buf[...] = (n_buf[...] * w_ref[...]).astype(BF16)
        inv_buf[...] = jnp.broadcast_to(inv, (tokens, LANES))
        pay[...] = n_buf[my_few]
        square[...] = jnp.zeros((LANES, LANES), F32)
        square[0:1, 0:tokens] = mask_in[...]
        mask_own[...] = square[0:few]
        mask_col = jnp.transpose(square[...])[0:tokens, 0:1]
        my_z, my_y = lax.div(me, SIDE), lax.rem(me, SIDE)
        for d in range(1, SIDE):
            remote(pay, pay_got.at[my_z, my_y], dp_sem.at[0, 0], dp_sem.at[0, 1], at[d, 0], col).start()
        pay_got[my_z, my_y] = pay[...]
        mask_sent, mask_came = to_dp(mask_own, mask_got, 1, pl.ds(0, 1))
        mask_got[me] = mask_own[...]
        for k in range(few_first, N_DP):
            weigh(k)
            issue(k)

        def keep(r, _):
            here, there = aligned(me * tokens + r * pack, pack, pack), aligned(r * pack, pack, pack)
            got_soon[0, there] = sends[here, :late]
            got_late[0, there] = sends[here, late:]
            return 0

        lax.fori_loop(0, tokens // pack, keep, 0)

        def student(slot):
            z = lax.dot_general(x_buf[...], tabs[slot], ROWS_BY_ROWS, preferred_element_type=F32)
            ratio = jnp.tanh(z * INV_CAP)
            return ratio, jnp.exp(SOFT_CAP * ratio - SOFT_CAP)

        def next_tiles(i):
            for c in range(per):
                tab_copy(i * per + c).wait()

            @pl.when(i + 1 < 2 * N_DP)
            def _():
                for c in range(per):
                    tab_copy((i + 1) * per + c).start()

            return [lax.rem(i, 2) * per + c for c in range(per)]

        def forward(i, sums):
            s_sum, k_sum = sums
            slots = next_tiles(i)
            for c in range(per):
                ratio, stu = student(slots[c])
                tea = sends[aligned(i * tokens, tokens, tokens), pl.ds(c * sub, sub)]
                s_sum, k_sum = s_sum + fold(stu), k_sum + fold(tea * ratio)
            return s_sum, k_sum

        zero = jnp.zeros((tokens, LANES), F32)
        s_sum, k_sum = lax.fori_loop(0, N_DP, forward, (zero, zero))
        lane = lax.broadcasted_iota(jnp.int32, (tokens, LANES), 1)
        sums = jnp.where(lane == 0, jnp.sum(s_sum, axis=1, keepdims=True), 0.0)
        sums = jnp.where(lane == 1, jnp.sum(t_acc[...], axis=1, keepdims=True), sums)
        sums = jnp.where(lane == AWAY, SOFT_CAP * jnp.sum(c_acc[...] - k_sum, axis=1, keepdims=True), sums)
        own_col[...] = sums
        tp_got[col] = sums
        tp_sent, tp_came = to_tp(lambda c: own_col, tp_got, 0)
        tp_came()
        total = added(tp_got)
        square[0:tokens] = jnp.where(lane == DOWN, mask_col, total)
        line = jnp.transpose(square[...])[0:few]
        own_row[...] = line
        all_ref[me] = line
        dp_sent, dp_came = to_dp(own_row, all_ref, 2)
        whole(pay_got.at[0, pl.ds(0, SIDE - 1)], dp_sem.at[0, 1])
        line = pay_got.at[:, my_y]
        for d in range(1, SIDE):
            remote(line, line, dp_sem.at[SIDE, 0], dp_sem.at[SIDE, 1], at[0, d], col).start()
        mask_came()
        came(0)
        onward(1, True, None)
        onward(1, False, 0)

        count = jnp.sum(added(mask_got, slice(1)), axis=1, keepdims=True)
        inv_s, inv_t, weight = 1.0 / total[:, 0:1], 1.0 / total[:, 1:2], mask_col / count
        dx[...] = jnp.zeros((tokens, dim), F32)

        def backward(i, _):
            slots = next_tiles(i)
            total = dx[...]
            for c in range(per):
                ratio, stu = student(slots[c])
                tea = sends[aligned((i - N_DP) * tokens, tokens, tokens), pl.ds(c * sub, sub)]
                diff = (stu * inv_s - tea * inv_t) * weight
                g = (diff * (1.0 - ratio * ratio)).astype(BF16)
                total = total + jnp.dot(g, tabs[slots[c]], preferred_element_type=F32)
            dx[...] = total
            return 0

        lax.fori_loop(N_DP, N_DP + SIDE, backward, 0)
        lines = pay_got.at[pl.ds(0, SIDE - 1)]
        whole(lines, dp_sem.at[SIDE, 1])
        twin = col + 1 - 2 * lax.rem(col, 2)
        x_got[col] = pay_got[...]
        for j in range(2, N_TP, 2):
            remote(pay_got, x_got.at[col], tp_sem.at[1, 0], tp_sem.at[1, 1], me, mates[j]).start()
        lax.fori_loop(N_DP + SIDE, 2 * N_DP, backward, 0)
        came(1)
        onward(2, True, 0)
        onward(1, False, 1)

        rs_got[col] = dx[my_few]
        rs_sent, rs_came = to_tp(lambda c: dx.at[aligned(c * few, few, few)], rs_got, 2)
        rs_came()
        my_x = added(rs_got)
        my_n = n_buf[my_few]
        grad_n = my_x * w_ref[...]
        my_h = inv_buf[my_few, 0:1] * (grad_n - my_n * jnp.mean(grad_n * my_n, axis=1, keepdims=True))
        ag_own[...] = jnp.zeros((2 * few, dim), F32)
        ag_own[0:few] = my_h
        ag_own[few:few + 1] = jnp.sum(my_x * my_n, axis=0, keepdims=True)
        ag_got[col] = ag_own[...]
        ag_sent, ag_came = to_tp(lambda c: ag_own, ag_got, DOWN)
        ag_came()
        gh_ref[...] = jnp.concatenate([ag_got[j, 0:few] for j in range(N_TP)], axis=0)
        line = added(ag_got, slice(few, few + 1))
        gn_own[0:1] = line
        gn_got[me, 0:1] = line
        gn_sent, gn_came = to_dp(gn_own, gn_got, DOWN, pl.ds(0, 1))

        came(2, 0)
        onward(DOWN, True, 0)
        onward(2, True, 1)
        whole(x_got.at[pl.ds(0, SIDE - 1)], tp_sem.at[1, 1])
        for j in range(0, N_TP, 2):
            remote(x_got.at[mates[j]], x_got.at[mates[j]], tp_sem.at[SIDE, 0], tp_sem.at[SIDE, 1], me, twin).start()
        whole(x_got.at[pl.ds(0, SIDE)], tp_sem.at[SIDE, 1])

        def widen(d, _):
            rows = jnp.concatenate([x_got[j, lax.div(d, SIDE), lax.rem(d, SIDE)] for j in range(N_TP)], axis=0)
            x_out[aligned(d * tokens, tokens, tokens)] = (rows * w_ref[...]).astype(BF16)
            return 0

        lax.fori_loop(0, N_DP, widen, 0)
        dp_came()
        row = lax.broadcasted_iota(jnp.int32, (few, LANES), 0)
        lanes = lax.broadcasted_iota(jnp.int32, (few, LANES), 1)
        for d in range(N_DP):
            block = all_ref[d]
            safe = jnp.where((row < AWAY) & (lanes < tokens), block, 1.0)
            rel[d * few:(d + 1) * few] = jnp.where(row < AWAY, 1.0 / safe, block / count)
        for k, (dz, dy) in enumerate(OFFSETS):
            square[k * few:(k + 1) * few] = rel[aligned(at[-dz, -dy] * few, few, few)]
        coef_ref[...] = jnp.transpose(square[...])

        own_tab.wait()
        whole(got_soon.at[pl.ds(0, N_DP - 1)], hop_in.at[SIDE])
        whole(sends.at[pl.ds(0, len(JOBS) * half)], hop_out.at[0])

        def block(b, _):
            @pl.when(b == 1)
            def _():
                came(2, 1)
                onward(DOWN, True, 1)

            grad_block(at, got_soon, x_out, tab_out[aligned(b * sub, sub)], coef_ref, sends, g_buf, blocks_ref, b)
            return 0

        lax.fori_loop(0, 2, block, 0)
        gn_came()
        gg_ref[...] = added(gn_got, slice(1))
        whole(got_late.at[pl.ds(0, N_DP - 1)], hop_in.at[SIDE + 1])
        whole(stage, hop_out.at[1])
        for ref, sem in (*mask_sent, *tp_sent, *dp_sent, *rs_sent, *ag_sent, *gn_sent):
            whole(ref, sem)
        whole(pay_got.at[0, pl.ds(0, SIDE - 1)], dp_sem.at[0, 0])
        whole(lines, dp_sem.at[SIDE, 0])
        whole(x_got.at[pl.ds(0, SIDE - 1)], tp_sem.at[1, 0])
        whole(x_got.at[pl.ds(0, SIDE)], tp_sem.at[SIDE, 0])

    dma = pltpu.SemaphoreType.DMA
    wide, flat = (tokens, dim), (few, LANES)
    return pl.pallas_call(
        kern,
        out_shape=tuple(jax.ShapeDtypeStruct(shape, kind) for shape, kind in (
            ((N_DP, tokens, part // 2), F32), ((2, sub, dim), F32), ((N_DP * tokens, dim), BF16), ((part, dim), BF16), ((LANES, LANES), F32), ((N_DP, *flat), F32), (wide, F32),
            ((1, dim), F32))),
        in_specs=[HB] * 5, out_specs=(VM,) * 8,
        scratch_shapes=[pltpu.VMEM(shape, kind) for shape, kind in (
            (wide, BF16), ((dim // LANES, LANES), F32), ((1, tokens), F32), ((1, dim), F32), ((ring * tokens, part), BF16), ((N_DP * tokens, part), F32),
            ((len(MIDDLE), half, part), F32), ((N_DP, tokens, part // 2), F32), ((N_DP * tokens, sub), BF16), ((tokens, LANES), F32), ((tokens, LANES), F32),
            ((depth, sub, dim), BF16), (wide, F32), (wide, BF16), ((tokens, LANES), F32), ((LANES, LANES), F32), ((few, dim), F32),
            ((SIDE, SIDE, few, dim), F32), (flat, F32), ((N_DP, *flat), F32), ((N_TP, SIDE, SIDE, few, dim), F32), ((N_TP, tokens, LANES), F32),
            ((tokens, LANES), F32), (flat, F32), ((LANES, LANES), F32), (wide, F32), ((N_TP, few, dim), F32), ((2 * few, dim), F32),
            ((N_TP, 2 * few, dim), F32), ((few, dim), F32), ((N_DP, few, dim), F32))] + [
            dma((ring,)), dma((depth,)), dma((5,)), dma((2,)), dma((SIDE + 2,)), dma((SIDE + 1, 2)), dma((SIDE + 1, 2))],
        compiler_params=pltpu.CompilerParams(collective_id=0, has_side_effects=True, vmem_limit_bytes=L_FRONT * MIB),
        cost_estimate=pl.CostEstimate(flops=3 * 10 ** 9, bytes_accessed=100 * MIB, transcendentals=0), name='front')(
            *(pltpu.with_memory_space_constraint(a, pltpu.HBM) for a in (hidden, gain_row, mask_row, teacher, table)))


def finish(teas, x_all, tab_part, coef):
    n, tokens, late = teas.shape
    dim = x_all.shape[1]
    span = late // 2

    def kern(tea_ref, x_ref, tab_ref, coef_ref, out_ref, z_buf, g_buf):
        at = peers()[1]

        def block(b, _):
            grad_block(at, tea_ref, x_ref, tab_ref[aligned(late + b * span, span)], coef_ref, z_buf, g_buf, out_ref, b)
            return 0

        lax.fori_loop(0, 2, block, 0)

    return pl.pallas_call(kern, out_shape=jax.ShapeDtypeStruct((2, span, dim), F32), in_specs=[VM] * 4, out_specs=VM,
        scratch_shapes=[pltpu.VMEM((n * tokens, span), F32), pltpu.VMEM((n * tokens, span), BF16)], name='finish',
        compiler_params=pltpu.CompilerParams(vmem_limit_bytes=22 * MIB),
        cost_estimate=pl.CostEstimate(flops=10 ** 9, bytes_accessed=8 * MIB, transcendentals=0))(teas, x_all, tab_part, coef)


def place(table, pieces, vocab):
    arrays = [p[0] for p in pieces]
    n = len(arrays)
    dim = arrays[0].shape[1]
    rows = vocab // N_DP
    quarter = rows // SIDE
    cut = 256
    chunks = []
    for i, (array, dz, dy, kind, start) in enumerate(pieces):
        r = 0
        while r < array.shape[0]:
            half, row = divmod(start + r, quarter)
            size = min(cut, array.shape[0] - r, quarter - row)
            chunks.append((i, r, size, dz, dy, (2 * half + kind) * quarter + row))
            r += size

    def kern(*refs):
        dst, buf, sem = refs[-DOWN:]
        at = peers()[1]
        reads, writes = [], []
        for k, (i, r, size, dz, dy, first) in enumerate(chunks):
            held = buf.at[k, pl.ds(0, size)]
            there = aligned(at[dz, dy] * rows + first, size, 16)
            reads.append(pltpu.make_async_copy(refs[i].at[pl.ds(r, size)], held, sem.at[0, k]))
            writes.append(pltpu.make_async_copy(held, dst.at[there], sem.at[1, k]))
        for cp in reads:
            cp.start()
        for read, write in zip(reads, writes):
            read.wait()
            write.start()
        for cp in writes:
            cp.wait()

    args = arrays if table is None else [*arrays, table]
    size = len(chunks) * cut * dim
    return pl.pallas_call(kern, out_shape=jax.ShapeDtypeStruct((vocab, dim), F32), in_specs=[pl.BlockSpec(memory_space=pl.ANY)] * n + [HB] * (len(args) - n),
        out_specs=HB, scratch_shapes=[pltpu.VMEM((len(chunks), cut, dim), F32), pltpu.SemaphoreType.DMA((2, len(chunks)))],
        input_output_aliases={} if table is None else {n: 0}, name='place', compiler_params=pltpu.CompilerParams(vmem_limit_bytes=4 * size + MIB),
        cost_estimate=pl.CostEstimate(flops=10 * MIB, bytes_accessed=8 * size, transcendentals=0))(*args)


def gather(first, rest, vocab):
    quarter = first[0].shape[0]
    sets, ways = range(2), (UP, DOWN)
    table, event = None, 0

    def send(pair, axis, step):
        out = []
        for k in sets:
            dz, dy = (step, 0) if axis == k else (0, step)
            out.append(lax.ppermute(pair[k], 'dp', [(d, shift(d, dz, dy)) for d in range(N_DP)]))
        return out

    def put(pair, a, b, start=0):
        return [(pair[k], *((b, a) if k else (a, b)), k, start) for k in sets]

    def settle(*pieces):
        nonlocal table
        table = place(table, [p for ps in pieces for p in ps], vocab)

    def wait(*pairs):
        nonlocal table, event
        event += 1
        table, *flat = lax.optimization_barrier((table, *(x for pair in pairs for x in pair)))
        return [flat[2 * i:2 * i + 2] for i in range(len(pairs))]

    def join(one, other):
        return [jnp.concatenate(pair) for pair in zip(one, other)]

    own = [first]
    low, high = ([send(own[0], 0, way)] for way in ways)
    later = rest()
    event = 1
    own.append([later[k] for k in sets])
    low.append(send(own[1], 0, UP))
    high.append(send(own[1], 0, DOWN))
    whole = join(*own)
    side = {way: send(whole, 1, way) for way in ways}
    settle(put(own[0], 0, 0, 0), put(own[1], 0, 0, quarter))

    low[0], high[0] = wait(low[0], high[0])
    far_low = send(low[0], 0, UP)
    settle(put(low[0], DOWN, 0, 0), put(high[0], UP, 0, 0))

    low[1], high[1] = wait(low[1], high[1])
    far_high = send(high[1], 0, DOWN)
    low_whole, high_whole = join(*low), join(*high)
    low_side = {way: send(low_whole, 1, way) for way in ways}
    settle(put(low[1], DOWN, 0, quarter), put(high[1], UP, 0, quarter))

    side[UP], side[DOWN], high_whole = wait(side[UP], side[DOWN], high_whole)
    high_side = {way: send(high_whole, 1, way) for way in ways}
    side_far = send(side[UP], 1, UP)
    settle(put(side[UP], 0, DOWN))
    settle(put(side[DOWN], 0, UP))

    far_low, far_high = wait(far_low, far_high)
    far_side = {(c, way): send(pair, 1, way) for way in ways for c, pair in enumerate((far_low, far_high))}
    settle(put(far_low, AWAY, 0, 0), put(far_high, AWAY, 0, quarter))

    low_side[UP], low_side[DOWN] = wait(low_side[UP], low_side[DOWN])
    low_far = send(low_side[DOWN], 1, DOWN)
    settle(put(low_side[UP], DOWN, DOWN))
    settle(put(low_side[DOWN], DOWN, UP))

    high_side[UP], high_side[DOWN] = wait(high_side[UP], high_side[DOWN])
    cut = quarter + 16
    high_far = [send([x[:cut] for x in high_side[UP]], 1, UP), send([x[cut:] for x in high_side[DOWN]], 1, DOWN)]
    settle(put(high_side[UP], UP, DOWN))
    settle(put(high_side[DOWN], UP, UP))

    far_side[0, DOWN], far_side[1, DOWN], side_far = wait(far_side[0, DOWN], far_side[1, DOWN], side_far)
    last_down = send(far_side[1, DOWN], 1, DOWN)
    settle(put(far_side[0, DOWN], AWAY, UP, 0), put(far_side[1, DOWN], AWAY, UP, quarter))
    settle(put(side_far, 0, AWAY))

    far_side[0, UP], = wait(far_side[0, UP])
    last_up = send(far_side[0, UP], 1, UP)
    settle(put(far_side[0, UP], AWAY, DOWN, 0))

    far_side[1, UP], low_far = wait(far_side[1, UP], low_far)
    settle(put(far_side[1, UP], AWAY, DOWN, quarter))
    settle(put(low_far, DOWN, AWAY))

    high_far = wait(*high_far)
    settle(put(high_far[0], UP, AWAY, 0), put(high_far[1], UP, AWAY, cut))
    for k in reversed(sets):
        table, up, down = lax.optimization_barrier((table, last_up[k], last_down[k]))
        table = place(table, [put([up] * 2, AWAY, AWAY)[k], put([down] * 2, AWAY, AWAY, quarter)[k]], vocab)
    return table


def solution(mesh):
    def local_step(hid_rows, w_final, tab_rows, tea_rows, mask_rows):
        tokens = hid_rows.shape[0]
        late, soon, x_all, tab_part, coef, stats, grad_h, gain_line = front(hid_rows, w_final.reshape(-1, LANES), mask_rows[None], tea_rows, tab_rows)
        coef, *first = lax.optimization_barrier((coef, soon[0], soon[1]))
        table = gather(first, lambda: finish(late, x_all, tab_part, coef), tab_rows.shape[0])
        s_sum, t_sum, k_sum, masks = (stats[:, i, :tokens] for i in range(SIDE))
        all_kl = k_sum / t_sum + jnp.log(s_sum) - jnp.log(t_sum)
        loss_val = jnp.sum(masks * all_kl) / jnp.sum(masks)
        return loss_val, grad_h.astype(BF16), gain_line[0], table

    return jax.shard_map(local_step, mesh=mesh, in_specs=(P('dp', None), P(None), P('tp', None), P('dp', 'tp'), P('dp')), out_specs=(P(), P('dp', None), P(None), P('tp', None)), check_vma=False)
```

```python
import jax
import jax.numpy as jnp
from jax import lax
from jax.experimental import pallas as pl
from jax.experimental.pallas import tpu as pltpu
from jax.sharding import PartitionSpec as P


SOFT_CAP = 30.0
INV_CAP = 1.0 / SOFT_CAP
NORM_EPS = 1e-6
SIDE, N_DP, N_TP, LANES = 4, 16, 8, 128
UP, DOWN, AWAY = 1, 3, 2
TILT = 8
MIB = 2 ** 20
L_FRONT = 41
MESH = pl.DeviceIdType.MESH
VM = pl.BlockSpec(memory_space=pltpu.VMEM)
HB = pl.BlockSpec(memory_space=pltpu.HBM)
F32, BF16 = jnp.float32, jnp.bfloat16
ROWS_BY_ROWS = (((1,), (1,)), ((), ()))
COLS_BY_COLS = (((0,), (0,)), ((), ()))

OFFSETS = tuple((dz, dy) for dz in range(SIDE) for dy in range(SIDE))
ORDER = tuple(sorted(OFFSETS, key=lambda o: -sum(min(d, SIDE - d) for d in o)))


def shift(dp, dz, dy):
    return (dp // SIDE + dz + SIDE) % SIDE * SIDE + (dp % SIDE + dy + SIDE) % SIDE


def peers():
    me = lax.axis_index('dp')
    z, y = lax.div(me, SIDE), lax.rem(me, SIDE)
    zs = [lax.rem(z + d, SIDE) * SIDE for d in range(SIDE)]
    ys = [lax.rem(y + d, SIDE) for d in range(SIDE)]
    return me, {(dz, dy): zs[dz] + ys[dy] for dz in range(-DOWN, SIDE) for dy in range(-DOWN, SIDE)}


def aligned(start, size, unit=LANES):
    return pl.ds(pl.multiple_of(start, unit), size)


def hops(kind, dz, dy):
    along_z = [(dz, 0)] if dz % 2 else [(UP if dy < AWAY else DOWN, 0)] * dz
    along_y = [(0, dy)] if dy % 2 else [(0, UP if dz < AWAY else DOWN)] * dy
    return along_y + along_z if kind else along_z + along_y


JOBS = tuple((kind, o) for o in ORDER[:-1] for kind in range(2))
PATHS = tuple(hops(kind, *o) for kind, o in JOBS)
MIDDLE = tuple((j, level) for level in range(SIDE) for j, path in enumerate(PATHS) if len(path) > level + 1)


def waves(j, level):
    return (None,) if (j, level) in MIDDLE and level < 2 else (0, 1)


def grad_block(at, tea_ref, x_ref, tab_rows, coef_ref, z_buf, g_buf, out_ref, block):
    tokens = tea_ref.shape[1]
    span = tab_rows.shape[0]
    few = LANES // N_DP
    cols = aligned(block * span, span)
    z_buf[:, :span] = lax.dot_general(x_ref[...], tab_rows, ROWS_BY_ROWS, preferred_element_type=F32)
    for k, (dz, dy) in enumerate(OFFSETS):
        here = aligned(at[-dz, -dy] * tokens, tokens, tokens)
        ratio = jnp.tanh(z_buf[here, :span] * INV_CAP)
        stu = jnp.exp(SOFT_CAP * ratio - SOFT_CAP)
        inv_s, inv_t, _, weight = (coef_ref[0:tokens, k * few + i:k * few + i + 1] for i in range(SIDE))
        diff = (stu * inv_s - tea_ref[k, :, cols] * inv_t) * weight
        g_buf[here, :span] = (diff * (1.0 - ratio * ratio)).astype(BF16)
    out_ref[block] = lax.dot_general(g_buf[:, :span], x_ref[...], COLS_BY_COLS, preferred_element_type=F32)


def front(hidden, gain_row, mask_row, teacher, table):
    tokens, vocab = teacher.shape
    dim = hidden.shape[1]
    part = vocab // N_DP
    half = tokens // 2
    few = tokens // N_TP
    pack = 16
    sub = 512
    per = part // sub
    tiles = vocab // sub
    depth = 2 * per
    ring = N_DP // 2
    few_first = 3

    def kern(hid_hbm, gain_hbm, mask_hbm, tea_ref, tab_ref, got_late, blocks_ref, x_out, tab_out, coef_ref, all_ref, gh_ref, gg_ref,
             hid_ref, gain_ref, mask_in, w_ref, raw, sends, stage, got_soon, g_buf, t_acc, c_acc, tabs, n_buf, x_buf, inv_buf, square, pay, pay_got, mask_own, mask_got, x_got, tp_got, own_col,
             own_row, rel, dx, rs_got, ag_own, ag_got, gn_own, gn_got, raw_sem, tab_sem, in_sem, hop_out, hop_in, dp_sem, tp_sem):
        me, at = peers()
        col = lax.axis_index('tp')
        mates = [lax.rem(col + j, N_TP) for j in range(N_TP)]
        my_few = aligned(col * few, few, few)

        def fetch(k):
            d = at[ORDER[k]]
            return pltpu.make_async_copy(tea_ref.at[:, aligned(d * part, part)], raw.at[pl.ds(k % ring * tokens, tokens)], raw_sem.at[k % ring])

        def tab_copy(i):
            slot = lax.rem(i, depth)
            return pltpu.make_async_copy(tab_ref.at[aligned(lax.rem(i, tiles) * sub, sub)], tabs.at[slot], tab_sem.at[slot])

        inputs = [pltpu.make_async_copy(src, dst, in_sem.at[2 + i])
                  for i, (src, dst) in enumerate(((hid_hbm, hid_ref), (gain_hbm, gain_ref), (mask_hbm, mask_in)))]
        own_tab = pltpu.make_async_copy(tab_ref.at[aligned(me * part, part)], tab_out, in_sem.at[1])
        for cp in inputs:
            cp.start()
        for k in range(ring):
            fetch(k).start()
        for i in range(per):
            tab_copy(i).start()
        own_tab.start()
        barrier = pltpu.get_barrier_semaphore()
        for dz, dy in ORDER[:-1]:
            pl.semaphore_signal(barrier, inc=1, device_id=(at[dz, dy], col), device_id_type=MESH)
        for j in range(1, N_TP):
            pl.semaphore_signal(barrier, inc=1, device_id=(me, mates[j]), device_id_type=MESH)

        def fold(v):
            total = v[:, :LANES]
            for c in range(LANES, v.shape[1], LANES):
                total = total + v[:, c:c + LANES]
            return total

        def weigh(k):
            fetch(k).wait()
            d = at[ORDER[k]]

            def rows(r, _):
                here = aligned(r * pack, pack, pack)
                cap = jnp.tanh(raw[aligned(k % ring * tokens + r * pack, pack, pack)].astype(F32) * INV_CAP)
                tea = jnp.exp(SOFT_CAP * cap - SOFT_CAP)
                sends[aligned(d * tokens + r * pack, pack, pack)] = tea
                t_acc[here] += fold(tea)
                c_acc[here] += fold(tea * cap)
                return 0

            lax.fori_loop(0, tokens // pack, rows, 0)
            if k + ring < N_DP:
                fetch(k + ring).start()

        t_acc[...] = jnp.zeros((tokens, LANES), F32)
        c_acc[...] = jnp.zeros((tokens, LANES), F32)
        weigh(0)
        pl.semaphore_wait(barrier, N_DP + N_TP - 2)

        def remote(src, dst, out, into, dp, tp):
            return pltpu.make_async_remote_copy(src_ref=src, dst_ref=dst, send_sem=out, recv_sem=into, device_id=(dp, tp), device_id_type=MESH)

        def whole(ref, sem):
            pltpu.make_async_copy(ref, ref, sem).wait()

        def to_dp(src, dst, x, rows=slice(None)):
            for o in ORDER[:-1]:
                remote(src.at[rows], dst.at[me, rows], dp_sem.at[x, 0], dp_sem.at[x, 1], at[o], col).start()
            others = dst.at[pl.ds(0, N_DP - 1), rows]
            return [(others, dp_sem.at[x, 0])], lambda: whole(others, dp_sem.at[x, 1])

        def to_tp(srcs, dst, x):
            for c in mates[1:]:
                remote(srcs(c), dst.at[col], tp_sem.at[x, 0], tp_sem.at[x, 1], me, c).start()
            others = dst.at[pl.ds(0, N_TP - 1)]
            return [(others, tp_sem.at[x, 0])], lambda: whole(others, tp_sem.at[x, 1])

        def added(ref, here=slice(None)):
            total = ref[0, here]
            for d in range(1, ref.shape[0]):
                total = total + ref[d, here]
            return total

        gots = (got_soon, got_late)
        late = part // 2

        def hop(j, level, w):
            kind, (dz, dy) = JOBS[j]
            tok = pl.ds(kind * half, half)
            rows = slice(None) if w is None else pl.ds(w * late, late)
            src = stage.at[MIDDLE.index((j, level - 1)), :, rows] if level else sends.at[aligned(at[dz, dy] * tokens + kind * half, half, half), rows]
            dst = stage.at[MIDDLE.index((j, level)), :, rows] if (j, level) in MIDDLE else gots[w].at[dz * SIDE + dy, tok]
            into = (level if w is None else level + w) if (j, level) in MIDDLE else SIDE + w
            return remote(src, dst, hop_out.at[min(level, 1)], hop_in.at[into], at[PATHS[j][level]], col)

        def came(level, w=None):
            n = sum(at == level for _, at in MIDDLE)
            rows = slice(None) if w is None else pl.ds(0, late)
            whole(stage.at[pl.ds(0, n), :, rows], hop_in.at[level + (w or 0)])

        def onward(level, far, *ws):
            for w in ws:
                for j, at in MIDDLE:
                    if at == level - 1 and far == (len(PATHS[j]) > 2):
                        hop(j, level, w).start()

        def issue(k):
            for j, (_, to) in enumerate(JOBS):
                if to == ORDER[k]:
                    for w in waves(j, 0):
                        hop(j, 0, w).start()

        issue(0)
        for k in range(1, few_first):
            weigh(k)
            issue(k)
        for cp in inputs:
            cp.wait()
        w_ref[...] = 1.0 + jnp.concatenate([gain_ref[i:i + 1] for i in range(dim // LANES)], axis=1)
        hid = hid_ref[...].astype(F32)
        inv = lax.rsqrt(jnp.mean(hid * hid, axis=1, keepdims=True) + NORM_EPS)
        n_buf[...] = hid * inv
        x_buf[...] = (n_buf[...] * w_ref[...]).astype(BF16)
        inv_buf[...] = jnp.broadcast_to(inv, (tokens, LANES))
        pay[...] = n_buf[my_few]
        square[...] = jnp.zeros((LANES, LANES), F32)
        square[0:1, 0:tokens] = mask_in[...]
        mask_own[...] = square[0:few]
        mask_col = jnp.transpose(square[...])[0:tokens, 0:1]
        pay_sent, pay_came = to_dp(pay, pay_got, 0)
        pay_got[me] = pay[...]
        mask_sent, mask_came = to_dp(mask_own, mask_got, 1, pl.ds(0, 1))
        mask_got[me] = mask_own[...]
        for k in range(few_first, N_DP):
            weigh(k)
            issue(k)

        def keep(r, _):
            here, there = aligned(me * tokens + r * pack, pack, pack), aligned(r * pack, pack, pack)
            got_soon[0, there] = sends[here, :late]
            got_late[0, there] = sends[here, late:]
            return 0

        lax.fori_loop(0, tokens // pack, keep, 0)

        def student(slot):
            z = lax.dot_general(x_buf[...], tabs[slot], ROWS_BY_ROWS, preferred_element_type=F32)
            ratio = jnp.tanh(z * INV_CAP)
            return ratio, jnp.exp(SOFT_CAP * ratio - SOFT_CAP)

        def next_tiles(i):
            for c in range(per):
                tab_copy(i * per + c).wait()

            @pl.when(i + 1 < 2 * N_DP)
            def _():
                for c in range(per):
                    tab_copy((i + 1) * per + c).start()

            return [lax.rem(i, 2) * per + c for c in range(per)]

        def forward(i, sums):
            s_sum, k_sum = sums
            slots = next_tiles(i)
            for c in range(per):
                ratio, stu = student(slots[c])
                tea = sends[aligned(i * tokens, tokens, tokens), pl.ds(c * sub, sub)]
                s_sum, k_sum = s_sum + fold(stu), k_sum + fold(tea * ratio)
            return s_sum, k_sum

        zero = jnp.zeros((tokens, LANES), F32)
        s_sum, k_sum = lax.fori_loop(0, N_DP, forward, (zero, zero))
        lane = lax.broadcasted_iota(jnp.int32, (tokens, LANES), 1)
        sums = jnp.where(lane == 0, jnp.sum(s_sum, axis=1, keepdims=True), 0.0)
        sums = jnp.where(lane == 1, jnp.sum(t_acc[...], axis=1, keepdims=True), sums)
        sums = jnp.where(lane == AWAY, SOFT_CAP * jnp.sum(c_acc[...] - k_sum, axis=1, keepdims=True), sums)
        own_col[...] = sums
        tp_got[col] = sums
        tp_sent, tp_came = to_tp(lambda c: own_col, tp_got, 0)
        tp_came()
        total = added(tp_got)
        square[0:tokens] = jnp.where(lane == DOWN, mask_col, total)
        line = jnp.transpose(square[...])[0:few]
        own_row[...] = line
        all_ref[me] = line
        dp_sent, dp_came = to_dp(own_row, all_ref, 2)
        twin = col + 1 - 2 * lax.rem(col, 2)
        pay_came()
        mask_came()
        x_got[col] = pay_got[...]

        evens = range(0, N_TP, 2)
        for j in evens[1:]:
            remote(pay_got, x_got.at[col], tp_sem.at[1, 0], tp_sem.at[1, 1], me, mates[j]).start()
        came(0)
        onward(1, True, None)
        onward(1, False, 0)

        count = jnp.sum(added(mask_got, slice(1)), axis=1, keepdims=True)
        inv_s, inv_t, weight = 1.0 / total[:, 0:1], 1.0 / total[:, 1:2], mask_col / count
        dx[...] = jnp.zeros((tokens, dim), F32)

        def backward(i, _):
            slots = next_tiles(i)
            total = dx[...]
            for c in range(per):
                ratio, stu = student(slots[c])
                tea = sends[aligned((i - N_DP) * tokens, tokens, tokens), pl.ds(c * sub, sub)]
                diff = (stu * inv_s - tea * inv_t) * weight
                g = (diff * (1.0 - ratio * ratio)).astype(BF16)
                total = total + jnp.dot(g, tabs[slots[c]], preferred_element_type=F32)
            dx[...] = total
            return 0

        lax.fori_loop(N_DP, 2 * N_DP, backward, 0)
        came(1)
        onward(2, True, 0)
        onward(1, False, 1)
        whole(x_got.at[pl.ds(0, SIDE - 1)], tp_sem.at[1, 1])
        for j in evens:
            remote(x_got.at[mates[j]], x_got.at[mates[j]], tp_sem.at[SIDE, 0], tp_sem.at[SIDE, 1], me, twin).start()

        rs_got[col] = dx[my_few]
        rs_sent, rs_came = to_tp(lambda c: dx.at[aligned(c * few, few, few)], rs_got, 2)
        rs_came()
        my_x = added(rs_got)
        my_n = n_buf[my_few]
        grad_n = my_x * w_ref[...]
        my_h = inv_buf[my_few, 0:1] * (grad_n - my_n * jnp.mean(grad_n * my_n, axis=1, keepdims=True))
        ag_own[...] = jnp.zeros((2 * few, dim), F32)
        ag_own[0:few] = my_h
        ag_own[few:few + 1] = jnp.sum(my_x * my_n, axis=0, keepdims=True)
        ag_got[col] = ag_own[...]
        ag_sent, ag_came = to_tp(lambda c: ag_own, ag_got, DOWN)
        ag_came()
        gh_ref[...] = jnp.concatenate([ag_got[j, 0:few] for j in range(N_TP)], axis=0)
        line = added(ag_got, slice(few, few + 1))
        gn_own[0:1] = line
        gn_got[me, 0:1] = line
        gn_sent, gn_came = to_dp(gn_own, gn_got, DOWN, pl.ds(0, 1))

        came(2, 0)
        onward(DOWN, True, 0)
        onward(2, True, 1)
        whole(x_got.at[pl.ds(0, SIDE)], tp_sem.at[SIDE, 1])

        def widen(d, _):
            rows = jnp.concatenate([x_got[j, d] for j in range(N_TP)], axis=0)
            x_out[aligned(d * tokens, tokens, tokens)] = (rows * w_ref[...]).astype(BF16)
            return 0

        lax.fori_loop(0, N_DP, widen, 0)
        dp_came()
        row = lax.broadcasted_iota(jnp.int32, (few, LANES), 0)
        lanes = lax.broadcasted_iota(jnp.int32, (few, LANES), 1)
        for d in range(N_DP):
            block = all_ref[d]
            safe = jnp.where((row < AWAY) & (lanes < tokens), block, 1.0)
            rel[d * few:(d + 1) * few] = jnp.where(row < AWAY, 1.0 / safe, block / count)
        for k, (dz, dy) in enumerate(OFFSETS):
            square[k * few:(k + 1) * few] = rel[aligned(at[-dz, -dy] * few, few, few)]
        coef_ref[...] = jnp.transpose(square[...])

        own_tab.wait()
        whole(got_soon.at[pl.ds(0, N_DP - 1)], hop_in.at[SIDE])
        whole(sends.at[pl.ds(0, len(JOBS) * half)], hop_out.at[0])

        def block(b, _):
            @pl.when(b == 1)
            def _():
                came(2, 1)
                onward(DOWN, True, 1)

            grad_block(at, got_soon, x_out, tab_out[aligned(b * sub, sub)], coef_ref, sends, g_buf, blocks_ref, b)
            return 0

        lax.fori_loop(0, 2, block, 0)
        gn_came()
        gg_ref[...] = added(gn_got, slice(1))
        whole(got_late.at[pl.ds(0, N_DP - 1)], hop_in.at[SIDE + 1])
        whole(stage, hop_out.at[1])
        for ref, sem in (*pay_sent, *mask_sent, *tp_sent, *dp_sent, *rs_sent, *ag_sent, *gn_sent):
            whole(ref, sem)
        whole(x_got.at[pl.ds(0, SIDE - 1)], tp_sem.at[1, 0])
        whole(x_got.at[pl.ds(0, SIDE)], tp_sem.at[SIDE, 0])

    dma = pltpu.SemaphoreType.DMA
    wide, flat = (tokens, dim), (few, LANES)
    return pl.pallas_call(
        kern,
        out_shape=tuple(jax.ShapeDtypeStruct(shape, kind) for shape, kind in (
            ((N_DP, tokens, part // 2), F32), ((2, sub, dim), F32), ((N_DP * tokens, dim), BF16), ((part, dim), BF16), ((LANES, LANES), F32), ((N_DP, *flat), F32), (wide, F32),
            ((1, dim), F32))),
        in_specs=[HB] * 5, out_specs=(VM,) * 8,
        scratch_shapes=[pltpu.VMEM(shape, kind) for shape, kind in (
            (wide, BF16), ((dim // LANES, LANES), F32), ((1, tokens), F32), ((1, dim), F32), ((ring * tokens, part), BF16), ((N_DP * tokens, part), F32),
            ((len(MIDDLE), half, part), F32), ((N_DP, tokens, part // 2), F32), ((N_DP * tokens, sub), BF16), ((tokens, LANES), F32), ((tokens, LANES), F32),
            ((depth, sub, dim), BF16), (wide, F32), (wide, BF16), ((tokens, LANES), F32), ((LANES, LANES), F32), ((few, dim), F32),
            ((N_DP, few, dim), F32), (flat, F32), ((N_DP, *flat), F32), ((N_TP, N_DP, few, dim), F32), ((N_TP, tokens, LANES), F32),
            ((tokens, LANES), F32), (flat, F32), ((LANES, LANES), F32), (wide, F32), ((N_TP, few, dim), F32), ((2 * few, dim), F32),
            ((N_TP, 2 * few, dim), F32), ((few, dim), F32), ((N_DP, few, dim), F32))] + [
            dma((ring,)), dma((depth,)), dma((5,)), dma((2,)), dma((SIDE + 2,)), dma((SIDE, 2)), dma((SIDE + 1, 2))],
        compiler_params=pltpu.CompilerParams(collective_id=0, has_side_effects=True, vmem_limit_bytes=L_FRONT * MIB),
        cost_estimate=pl.CostEstimate(flops=3 * 10 ** 9, bytes_accessed=100 * MIB, transcendentals=0), name='front')(
            *(pltpu.with_memory_space_constraint(a, pltpu.HBM) for a in (hidden, gain_row, mask_row, teacher, table)))


def finish(teas, x_all, tab_part, coef):
    n, tokens, late = teas.shape
    dim = x_all.shape[1]
    span = late // 2

    def kern(tea_ref, x_ref, tab_ref, coef_ref, out_ref, z_buf, g_buf):
        at = peers()[1]

        def block(b, _):
            grad_block(at, tea_ref, x_ref, tab_ref[aligned(late + b * span, span)], coef_ref, z_buf, g_buf, out_ref, b)
            return 0

        lax.fori_loop(0, 2, block, 0)

    return pl.pallas_call(kern, out_shape=jax.ShapeDtypeStruct((2, span, dim), F32), in_specs=[VM] * 4, out_specs=VM,
        scratch_shapes=[pltpu.VMEM((n * tokens, span), F32), pltpu.VMEM((n * tokens, span), BF16)], name='finish',
        compiler_params=pltpu.CompilerParams(vmem_limit_bytes=22 * MIB),
        cost_estimate=pl.CostEstimate(flops=10 ** 9, bytes_accessed=8 * MIB, transcendentals=0))(teas, x_all, tab_part, coef)


def place(table, pieces, vocab):
    arrays = [p[0] for p in pieces]
    n = len(arrays)
    dim = arrays[0].shape[1]
    rows = vocab // N_DP
    quarter = rows // SIDE
    cut = 256
    chunks = []
    for i, (array, dz, dy, kind, start) in enumerate(pieces):
        r = 0
        while r < array.shape[0]:
            row = start + r
            size = min(cut, array.shape[0] - r, quarter - row if row < quarter else cut)
            chunks.append((i, r, size, dz, dy, row + kind * quarter if row < quarter else row + quarter + kind * (quarter - TILT)))
            r += size

    def kern(*refs):
        dst, buf, sem = refs[-DOWN:]
        at = peers()[1]
        reads, writes = [], []
        for k, (i, r, size, dz, dy, first) in enumerate(chunks):
            held = buf.at[k, pl.ds(0, size)]
            there = aligned(at[dz, dy] * rows + first, size, 8)
            reads.append(pltpu.make_async_copy(refs[i].at[pl.ds(r, size)], held, sem.at[0, k]))
            writes.append(pltpu.make_async_copy(held, dst.at[there], sem.at[1, k]))
        for cp in reads:
            cp.start()
        for read, write in zip(reads, writes):
            read.wait()
            write.start()
        for cp in writes:
            cp.wait()

    args = arrays if table is None else [*arrays, table]
    size = len(chunks) * cut * dim
    return pl.pallas_call(kern, out_shape=jax.ShapeDtypeStruct((vocab, dim), F32), in_specs=[pl.BlockSpec(memory_space=pl.ANY)] * n + [HB] * (len(args) - n),
        out_specs=HB, scratch_shapes=[pltpu.VMEM((len(chunks), cut, dim), F32), pltpu.SemaphoreType.DMA((2, len(chunks)))],
        input_output_aliases={} if table is None else {n: 0}, name='place', compiler_params=pltpu.CompilerParams(vmem_limit_bytes=4 * size + MIB),
        cost_estimate=pl.CostEstimate(flops=10 * MIB, bytes_accessed=8 * size, transcendentals=0))(*args)


def gather(first, rest, vocab):
    quarter = first[0].shape[0]
    sets, ways = range(2), (UP, DOWN)
    table, event = None, 0

    def send(pair, axis, step):
        out = []
        for k in sets:
            dz, dy = (step, 0) if axis == k else (0, step)
            out.append(lax.ppermute(pair[k], 'dp', [(d, shift(d, dz, dy)) for d in range(N_DP)]))
        return out

    def put(pair, a, b, start=0):
        starts = start if isinstance(start, tuple) else (start, start)
        return [(pair[k], *((b, a) if k else (a, b)), k, starts[k]) for k in sets]

    def settle(*pieces):
        nonlocal table
        table = place(table, [p for ps in pieces for p in ps], vocab)

    def wait(*pairs):
        nonlocal table, event
        event += 1
        table, *flat = lax.optimization_barrier((table, *(x for pair in pairs for x in pair)))
        return [flat[2 * i:2 * i + 2] for i in range(len(pairs))]

    def join(one, other):
        return [jnp.concatenate(pair) for pair in zip(one, other)]

    own = [first]
    low, high = ([send(own[0], 0, way)] for way in ways)
    later = rest()
    event = 1
    own.append([later[:quarter - TILT], later[quarter - TILT:]])
    low.append(send(own[1], 0, UP))
    high.append(send(own[1], 0, DOWN))
    whole = join(*own)
    side = {way: send(whole, 1, way) for way in ways}
    settle(put(own[0], 0, 0, 0), put(own[1], 0, 0, quarter))

    low[0], high[0] = wait(low[0], high[0])
    far_low = send(low[0], 0, UP)
    settle(put(low[0], DOWN, 0, 0), put(high[0], UP, 0, 0))

    low[1], high[1] = wait(low[1], high[1])
    far_high = send(high[1], 0, DOWN)
    low_whole, high_whole = join(*low), join(*high)
    low_side = {way: send(low_whole, 1, way) for way in ways}
    settle(put(low[1], DOWN, 0, quarter), put(high[1], UP, 0, quarter))

    side[UP], side[DOWN], high_whole = wait(side[UP], side[DOWN], high_whole)
    high_side = {way: send(high_whole, 1, way) for way in ways}
    side_far = send(side[UP], 1, UP)
    settle(put(side[UP], 0, DOWN))
    settle(put(side[DOWN], 0, UP))

    far_low, far_high = wait(far_low, far_high)
    far_side = {(c, way): send(pair, 1, way) for way in ways for c, pair in enumerate((far_low, far_high))}
    settle(put(far_low, AWAY, 0, 0), put(far_high, AWAY, 0, quarter))

    low_side[UP], low_side[DOWN] = wait(low_side[UP], low_side[DOWN])
    low_far = send(low_side[DOWN], 1, DOWN)
    settle(put(low_side[UP], DOWN, DOWN))
    settle(put(low_side[DOWN], DOWN, UP))

    high_side[UP], high_side[DOWN] = wait(high_side[UP], high_side[DOWN])
    cuts = quarter + TILT, quarter + 2 * TILT
    high_far = [send([x[:cut] for x, cut in zip(high_side[UP], cuts)], 1, UP), send([x[cut:] for x, cut in zip(high_side[DOWN], cuts)], 1, DOWN)]
    settle(put(high_side[UP], UP, DOWN))
    settle(put(high_side[DOWN], UP, UP))

    far_side[0, DOWN], far_side[1, DOWN], side_far = wait(far_side[0, DOWN], far_side[1, DOWN], side_far)
    last_down = send(far_side[1, DOWN], 1, DOWN)
    settle(put(far_side[0, DOWN], AWAY, UP, 0), put(far_side[1, DOWN], AWAY, UP, quarter))
    settle(put(side_far, 0, AWAY))

    far_side[0, UP], = wait(far_side[0, UP])
    last_up = send(far_side[0, UP], 1, UP)
    settle(put(far_side[0, UP], AWAY, DOWN, 0))

    far_side[1, UP], low_far = wait(far_side[1, UP], low_far)
    settle(put(far_side[1, UP], AWAY, DOWN, quarter))
    settle(put(low_far, DOWN, AWAY))

    high_far = wait(*high_far)
    settle(put(high_far[0], UP, AWAY, 0), put(high_far[1], UP, AWAY, cuts))
    last_up, last_down = wait(last_up, last_down)
    settle(put(last_up, AWAY, AWAY, 0), put(last_down, AWAY, AWAY, quarter))
    return table


def solution(mesh):
    def local_step(hid_rows, w_final, tab_rows, tea_rows, mask_rows):
        tokens = hid_rows.shape[0]
        late, soon, x_all, tab_part, coef, stats, grad_h, gain_line = front(hid_rows, w_final.reshape(-1, LANES), mask_rows[None], tea_rows, tab_rows)
        coef, *first = lax.optimization_barrier((coef, soon[0], soon[1]))
        table = gather(first, lambda: finish(late, x_all, tab_part, coef).reshape(-1, x_all.shape[1]), tab_rows.shape[0])
        s_sum, t_sum, k_sum, masks = (stats[:, i, :tokens] for i in range(SIDE))
        all_kl = k_sum / t_sum + jnp.log(s_sum) - jnp.log(t_sum)
        loss_val = jnp.sum(masks * all_kl) / jnp.sum(masks)
        return loss_val, grad_h.astype(BF16), gain_line[0], table

    return jax.shard_map(local_step, mesh=mesh, in_specs=(P('dp', None), P(None), P('tp', None), P('dp', 'tp'), P('dp')), out_specs=(P(), P('dp', None), P(None), P('tp', None)), check_vma=False)
```

```python
import jax
import jax.numpy as jnp
from jax import lax
from jax.experimental import pallas as pl
from jax.experimental.pallas import tpu as pltpu
from jax.sharding import PartitionSpec as P


SOFT_CAP = 30.0
INV_CAP = 1.0 / SOFT_CAP
NORM_EPS = 1e-6
SIDE, N_DP, N_TP, LANES = 4, 16, 8, 128
UP, DOWN, AWAY = 1, 3, 2
TILT = 8
LAST = 64
MIB = 2 ** 20
L_FRONT = 41
MESH = pl.DeviceIdType.MESH
VM = pl.BlockSpec(memory_space=pltpu.VMEM)
HB = pl.BlockSpec(memory_space=pltpu.HBM)
F32, BF16 = jnp.float32, jnp.bfloat16
ROWS_BY_ROWS = (((1,), (1,)), ((), ()))
COLS_BY_COLS = (((0,), (0,)), ((), ()))

OFFSETS = tuple((dz, dy) for dz in range(SIDE) for dy in range(SIDE))
ORDER = tuple(sorted(OFFSETS, key=lambda o: -sum(min(d, SIDE - d) for d in o)))


def shift(dp, dz, dy):
    return (dp // SIDE + dz + SIDE) % SIDE * SIDE + (dp % SIDE + dy + SIDE) % SIDE


def peers():
    me = lax.axis_index('dp')
    z, y = lax.div(me, SIDE), lax.rem(me, SIDE)
    zs = [lax.rem(z + d, SIDE) * SIDE for d in range(SIDE)]
    ys = [lax.rem(y + d, SIDE) for d in range(SIDE)]
    return me, {(dz, dy): zs[dz] + ys[dy] for dz in range(-DOWN, SIDE) for dy in range(-DOWN, SIDE)}


def aligned(start, size, unit=LANES):
    return pl.ds(pl.multiple_of(start, unit), size)


def hops(kind, dz, dy):
    along_z = [(dz, 0)] if dz % 2 else [(UP if dy < AWAY else DOWN, 0)] * dz
    along_y = [(0, dy)] if dy % 2 else [(0, UP if dz < AWAY else DOWN)] * dy
    return along_y + along_z if kind else along_z + along_y


JOBS = tuple((kind, o) for o in ORDER[:-1] for kind in range(2))
PATHS = tuple(hops(kind, *o) for kind, o in JOBS)
MIDDLE = tuple((j, level) for level in range(SIDE) for j, path in enumerate(PATHS) if len(path) > level + 1)


def waves(j, level):
    return (None,) if (j, level) in MIDDLE and level < 2 else (0, 1)


def grad_block(at, tea_ref, x_ref, tab_rows, coef_ref, z_buf, g_buf, out_ref, block):
    tokens = tea_ref.shape[1]
    span = tab_rows.shape[0]
    few = LANES // N_DP
    cols = aligned(block * span, span)
    z_buf[:, :span] = lax.dot_general(x_ref[...], tab_rows, ROWS_BY_ROWS, preferred_element_type=F32)
    for k, (dz, dy) in enumerate(OFFSETS):
        here = aligned(at[-dz, -dy] * tokens, tokens, tokens)
        ratio = jnp.tanh(z_buf[here, :span] * INV_CAP)
        stu = jnp.exp(SOFT_CAP * ratio - SOFT_CAP)
        inv_s, inv_t, _, weight = (coef_ref[0:tokens, k * few + i:k * few + i + 1] for i in range(SIDE))
        diff = (stu * inv_s - tea_ref[k, :, cols] * inv_t) * weight
        g_buf[here, :span] = (diff * (1.0 - ratio * ratio)).astype(BF16)
    out_ref[block] = lax.dot_general(g_buf[:, :span], x_ref[...], COLS_BY_COLS, preferred_element_type=F32)


def front(hidden, gain_row, mask_row, teacher, table):
    tokens, vocab = teacher.shape
    dim = hidden.shape[1]
    part = vocab // N_DP
    half = tokens // 2
    few = tokens // N_TP
    pack = 16
    sub = 512
    per = part // sub
    tiles = vocab // sub
    depth = 2 * per
    ring = N_DP // 2
    few_first = 3

    def kern(hid_hbm, gain_hbm, mask_hbm, tea_ref, tab_ref, got_late, blocks_ref, x_out, tab_out, coef_ref, all_ref, gh_ref, gg_ref,
             hid_ref, gain_ref, mask_in, w_ref, raw, sends, stage, got_soon, g_buf, t_acc, c_acc, tabs, n_buf, x_buf, inv_buf, square, pay, pay_got, mask_own, mask_got, x_got, tp_got, own_col,
             own_row, rel, dx, rs_got, ag_own, ag_got, gn_own, gn_got, raw_sem, tab_sem, in_sem, hop_out, hop_in, dp_sem, tp_sem):
        me, at = peers()
        col = lax.axis_index('tp')
        mates = [lax.rem(col + j, N_TP) for j in range(N_TP)]
        my_few = aligned(col * few, few, few)

        def fetch(k):
            d = at[ORDER[k]]
            return pltpu.make_async_copy(tea_ref.at[:, aligned(d * part, part)], raw.at[pl.ds(k % ring * tokens, tokens)], raw_sem.at[k % ring])

        def tab_copy(i):
            slot = lax.rem(i, depth)
            return pltpu.make_async_copy(tab_ref.at[aligned(lax.rem(i, tiles) * sub, sub)], tabs.at[slot], tab_sem.at[slot])

        inputs = [pltpu.make_async_copy(src, dst, in_sem.at[2 + i])
                  for i, (src, dst) in enumerate(((hid_hbm, hid_ref), (gain_hbm, gain_ref), (mask_hbm, mask_in)))]
        own_tab = pltpu.make_async_copy(tab_ref.at[aligned(me * part, part)], tab_out, in_sem.at[1])
        for cp in inputs:
            cp.start()
        for k in range(ring):
            fetch(k).start()
        for i in range(per):
            tab_copy(i).start()
        own_tab.start()
        barrier = pltpu.get_barrier_semaphore()
        for dz, dy in ORDER[:-1]:
            pl.semaphore_signal(barrier, inc=1, device_id=(at[dz, dy], col), device_id_type=MESH)
        for j in range(1, N_TP):
            pl.semaphore_signal(barrier, inc=1, device_id=(me, mates[j]), device_id_type=MESH)

        def fold(v):
            total = v[:, :LANES]
            for c in range(LANES, v.shape[1], LANES):
                total = total + v[:, c:c + LANES]
            return total

        def weigh(k):
            fetch(k).wait()
            d = at[ORDER[k]]

            def rows(r, _):
                here = aligned(r * pack, pack, pack)
                cap = jnp.tanh(raw[aligned(k % ring * tokens + r * pack, pack, pack)].astype(F32) * INV_CAP)
                tea = jnp.exp(SOFT_CAP * cap - SOFT_CAP)
                sends[aligned(d * tokens + r * pack, pack, pack)] = tea
                t_acc[here] += fold(tea)
                c_acc[here] += fold(tea * cap)
                return 0

            lax.fori_loop(0, tokens // pack, rows, 0)
            if k + ring < N_DP:
                fetch(k + ring).start()

        t_acc[...] = jnp.zeros((tokens, LANES), F32)
        c_acc[...] = jnp.zeros((tokens, LANES), F32)
        weigh(0)
        pl.semaphore_wait(barrier, N_DP + N_TP - 2)

        def remote(src, dst, out, into, dp, tp):
            return pltpu.make_async_remote_copy(src_ref=src, dst_ref=dst, send_sem=out, recv_sem=into, device_id=(dp, tp), device_id_type=MESH)

        def whole(ref, sem):
            pltpu.make_async_copy(ref, ref, sem).wait()

        def to_dp(src, dst, x, rows=slice(None)):
            for o in ORDER[:-1]:
                remote(src.at[rows], dst.at[me, rows], dp_sem.at[x, 0], dp_sem.at[x, 1], at[o], col).start()
            others = dst.at[pl.ds(0, N_DP - 1), rows]
            return [(others, dp_sem.at[x, 0])], lambda: whole(others, dp_sem.at[x, 1])

        def to_tp(srcs, dst, x):
            for c in mates[1:]:
                remote(srcs(c), dst.at[col], tp_sem.at[x, 0], tp_sem.at[x, 1], me, c).start()
            others = dst.at[pl.ds(0, N_TP - 1)]
            return [(others, tp_sem.at[x, 0])], lambda: whole(others, tp_sem.at[x, 1])

        def added(ref, here=slice(None)):
            total = ref[0, here]
            for d in range(1, ref.shape[0]):
                total = total + ref[d, here]
            return total

        gots = (got_soon, got_late)
        late = part // 2

        def hop(j, level, w):
            kind, (dz, dy) = JOBS[j]
            tok = pl.ds(kind * half, half)
            rows = slice(None) if w is None else pl.ds(w * late, late)
            src = stage.at[MIDDLE.index((j, level - 1)), :, rows] if level else sends.at[aligned(at[dz, dy] * tokens + kind * half, half, half), rows]
            dst = stage.at[MIDDLE.index((j, level)), :, rows] if (j, level) in MIDDLE else gots[w].at[dz * SIDE + dy, tok]
            into = (level if w is None else level + w) if (j, level) in MIDDLE else SIDE + w
            return remote(src, dst, hop_out.at[min(level, 1)], hop_in.at[into], at[PATHS[j][level]], col)

        def came(level, w=None):
            n = sum(at == level for _, at in MIDDLE)
            rows = slice(None) if w is None else pl.ds(0, late)
            whole(stage.at[pl.ds(0, n), :, rows], hop_in.at[level + (w or 0)])

        def onward(level, far, *ws):
            for w in ws:
                for j, at in MIDDLE:
                    if at == level - 1 and far == (len(PATHS[j]) > 2):
                        hop(j, level, w).start()

        def issue(k):
            for j, (_, to) in enumerate(JOBS):
                if to == ORDER[k]:
                    for w in waves(j, 0):
                        hop(j, 0, w).start()

        issue(0)
        for k in range(1, few_first):
            weigh(k)
            issue(k)
        for cp in inputs:
            cp.wait()
        w_ref[...] = 1.0 + jnp.concatenate([gain_ref[i:i + 1] for i in range(dim // LANES)], axis=1)
        hid = hid_ref[...].astype(F32)
        inv = lax.rsqrt(jnp.mean(hid * hid, axis=1, keepdims=True) + NORM_EPS)
        n_buf[...] = hid * inv
        x_buf[...] = (n_buf[...] * w_ref[...]).astype(BF16)
        inv_buf[...] = jnp.broadcast_to(inv, (tokens, LANES))
        pay[...] = n_buf[my_few]
        square[...] = jnp.zeros((LANES, LANES), F32)
        square[0:1, 0:tokens] = mask_in[...]
        mask_own[...] = square[0:few]
        mask_col = jnp.transpose(square[...])[0:tokens, 0:1]
        pay_sent, pay_came = to_dp(pay, pay_got, 0)
        pay_got[me] = pay[...]
        mask_sent, mask_came = to_dp(mask_own, mask_got, 1, pl.ds(0, 1))
        mask_got[me] = mask_own[...]
        for k in range(few_first, N_DP):
            weigh(k)
            issue(k)

        def keep(r, _):
            here, there = aligned(me * tokens + r * pack, pack, pack), aligned(r * pack, pack, pack)
            got_soon[0, there] = sends[here, :late]
            got_late[0, there] = sends[here, late:]
            return 0

        lax.fori_loop(0, tokens // pack, keep, 0)

        def student(slot):
            z = lax.dot_general(x_buf[...], tabs[slot], ROWS_BY_ROWS, preferred_element_type=F32)
            ratio = jnp.tanh(z * INV_CAP)
            return ratio, jnp.exp(SOFT_CAP * ratio - SOFT_CAP)

        def next_tiles(i):
            for c in range(per):
                tab_copy(i * per + c).wait()

            @pl.when(i + 1 < 2 * N_DP)
            def _():
                for c in range(per):
                    tab_copy((i + 1) * per + c).start()

            return [lax.rem(i, 2) * per + c for c in range(per)]

        def forward(i, sums):
            s_sum, k_sum = sums
            slots = next_tiles(i)
            for c in range(per):
                ratio, stu = student(slots[c])
                tea = sends[aligned(i * tokens, tokens, tokens), pl.ds(c * sub, sub)]
                s_sum, k_sum = s_sum + fold(stu), k_sum + fold(tea * ratio)
            return s_sum, k_sum

        zero = jnp.zeros((tokens, LANES), F32)
        s_sum, k_sum = lax.fori_loop(0, N_DP, forward, (zero, zero))
        lane = lax.broadcasted_iota(jnp.int32, (tokens, LANES), 1)
        sums = jnp.where(lane == 0, jnp.sum(s_sum, axis=1, keepdims=True), 0.0)
        sums = jnp.where(lane == 1, jnp.sum(t_acc[...], axis=1, keepdims=True), sums)
        sums = jnp.where(lane == AWAY, SOFT_CAP * jnp.sum(c_acc[...] - k_sum, axis=1, keepdims=True), sums)
        own_col[...] = sums
        tp_got[col] = sums
        tp_sent, tp_came = to_tp(lambda c: own_col, tp_got, 0)
        tp_came()
        total = added(tp_got)
        square[0:tokens] = jnp.where(lane == DOWN, mask_col, total)
        line = jnp.transpose(square[...])[0:few]
        own_row[...] = line
        all_ref[me] = line
        dp_sent, dp_came = to_dp(own_row, all_ref, 2)
        twin = col + 1 - 2 * lax.rem(col, 2)
        pay_came()
        mask_came()
        x_got[col] = pay_got[...]

        evens = range(0, N_TP, 2)
        for j in evens[1:]:
            remote(pay_got, x_got.at[col], tp_sem.at[1, 0], tp_sem.at[1, 1], me, mates[j]).start()
        came(0)
        onward(1, True, None)
        onward(1, False, 0)

        count = jnp.sum(added(mask_got, slice(1)), axis=1, keepdims=True)
        inv_s, inv_t, weight = 1.0 / total[:, 0:1], 1.0 / total[:, 1:2], mask_col / count
        dx[...] = jnp.zeros((tokens, dim), F32)

        def backward(i, _):
            slots = next_tiles(i)
            total = dx[...]
            for c in range(per):
                ratio, stu = student(slots[c])
                tea = sends[aligned((i - N_DP) * tokens, tokens, tokens), pl.ds(c * sub, sub)]
                diff = (stu * inv_s - tea * inv_t) * weight
                g = (diff * (1.0 - ratio * ratio)).astype(BF16)
                total = total + jnp.dot(g, tabs[slots[c]], preferred_element_type=F32)
            dx[...] = total
            return 0

        lax.fori_loop(N_DP, 2 * N_DP, backward, 0)
        came(1)
        onward(2, True, 0)
        onward(1, False, 1)
        whole(x_got.at[pl.ds(0, SIDE - 1)], tp_sem.at[1, 1])
        for j in evens:
            remote(x_got.at[mates[j]], x_got.at[mates[j]], tp_sem.at[SIDE, 0], tp_sem.at[SIDE, 1], me, twin).start()

        rs_got[col] = dx[my_few]
        rs_sent, rs_came = to_tp(lambda c: dx.at[aligned(c * few, few, few)], rs_got, 2)
        rs_came()
        my_x = added(rs_got)
        my_n = n_buf[my_few]
        grad_n = my_x * w_ref[...]
        my_h = inv_buf[my_few, 0:1] * (grad_n - my_n * jnp.mean(grad_n * my_n, axis=1, keepdims=True))
        ag_own[...] = jnp.zeros((2 * few, dim), F32)
        ag_own[0:few] = my_h
        ag_own[few:few + 1] = jnp.sum(my_x * my_n, axis=0, keepdims=True)
        ag_got[col] = ag_own[...]
        ag_sent, ag_came = to_tp(lambda c: ag_own, ag_got, DOWN)
        ag_came()
        gh_ref[...] = jnp.concatenate([ag_got[j, 0:few] for j in range(N_TP)], axis=0)
        line = added(ag_got, slice(few, few + 1))
        gn_own[0:1] = line
        gn_got[me, 0:1] = line
        gn_sent, gn_came = to_dp(gn_own, gn_got, DOWN, pl.ds(0, 1))

        came(2, 0)
        onward(DOWN, True, 0)
        onward(2, True, 1)
        whole(x_got.at[pl.ds(0, SIDE)], tp_sem.at[SIDE, 1])

        def widen(d, _):
            rows = jnp.concatenate([x_got[j, d] for j in range(N_TP)], axis=0)
            x_out[aligned(d * tokens, tokens, tokens)] = (rows * w_ref[...]).astype(BF16)
            return 0

        lax.fori_loop(0, N_DP, widen, 0)
        dp_came()
        row = lax.broadcasted_iota(jnp.int32, (few, LANES), 0)
        lanes = lax.broadcasted_iota(jnp.int32, (few, LANES), 1)
        for d in range(N_DP):
            block = all_ref[d]
            safe = jnp.where((row < AWAY) & (lanes < tokens), block, 1.0)
            rel[d * few:(d + 1) * few] = jnp.where(row < AWAY, 1.0 / safe, block / count)
        for k, (dz, dy) in enumerate(OFFSETS):
            square[k * few:(k + 1) * few] = rel[aligned(at[-dz, -dy] * few, few, few)]
        coef_ref[...] = jnp.transpose(square[...])

        own_tab.wait()
        whole(got_soon.at[pl.ds(0, N_DP - 1)], hop_in.at[SIDE])
        whole(sends.at[pl.ds(0, len(JOBS) * half)], hop_out.at[0])

        def block(b, _):
            @pl.when(b == 1)
            def _():
                came(2, 1)
                onward(DOWN, True, 1)

            grad_block(at, got_soon, x_out, tab_out[aligned(b * sub, sub)], coef_ref, sends, g_buf, blocks_ref, b)
            return 0

        lax.fori_loop(0, 2, block, 0)
        gn_came()
        gg_ref[...] = added(gn_got, slice(1))
        whole(got_late.at[pl.ds(0, N_DP - 1)], hop_in.at[SIDE + 1])
        whole(stage, hop_out.at[1])
        for ref, sem in (*pay_sent, *mask_sent, *tp_sent, *dp_sent, *rs_sent, *ag_sent, *gn_sent):
            whole(ref, sem)
        whole(x_got.at[pl.ds(0, SIDE - 1)], tp_sem.at[1, 0])
        whole(x_got.at[pl.ds(0, SIDE)], tp_sem.at[SIDE, 0])

    dma = pltpu.SemaphoreType.DMA
    wide, flat = (tokens, dim), (few, LANES)
    return pl.pallas_call(
        kern,
        out_shape=tuple(jax.ShapeDtypeStruct(shape, kind) for shape, kind in (
            ((N_DP, tokens, part // 2), F32), ((2, sub, dim), F32), ((N_DP * tokens, dim), BF16), ((part, dim), BF16), ((LANES, LANES), F32), ((N_DP, *flat), F32), (wide, F32),
            ((1, dim), F32))),
        in_specs=[HB] * 5, out_specs=(VM,) * 8,
        scratch_shapes=[pltpu.VMEM(shape, kind) for shape, kind in (
            (wide, BF16), ((dim // LANES, LANES), F32), ((1, tokens), F32), ((1, dim), F32), ((ring * tokens, part), BF16), ((N_DP * tokens, part), F32),
            ((len(MIDDLE), half, part), F32), ((N_DP, tokens, part // 2), F32), ((N_DP * tokens, sub), BF16), ((tokens, LANES), F32), ((tokens, LANES), F32),
            ((depth, sub, dim), BF16), (wide, F32), (wide, BF16), ((tokens, LANES), F32), ((LANES, LANES), F32), ((few, dim), F32),
            ((N_DP, few, dim), F32), (flat, F32), ((N_DP, *flat), F32), ((N_TP, N_DP, few, dim), F32), ((N_TP, tokens, LANES), F32),
            ((tokens, LANES), F32), (flat, F32), ((LANES, LANES), F32), (wide, F32), ((N_TP, few, dim), F32), ((2 * few, dim), F32),
            ((N_TP, 2 * few, dim), F32), ((few, dim), F32), ((N_DP, few, dim), F32))] + [
            dma((ring,)), dma((depth,)), dma((5,)), dma((2,)), dma((SIDE + 2,)), dma((SIDE, 2)), dma((SIDE + 1, 2))],
        compiler_params=pltpu.CompilerParams(collective_id=0, has_side_effects=True, vmem_limit_bytes=L_FRONT * MIB),
        cost_estimate=pl.CostEstimate(flops=3 * 10 ** 9, bytes_accessed=100 * MIB, transcendentals=0), name='front')(
            *(pltpu.with_memory_space_constraint(a, pltpu.HBM) for a in (hidden, gain_row, mask_row, teacher, table)))


def finish(teas, x_all, tab_part, coef):
    n, tokens, late = teas.shape
    dim = x_all.shape[1]
    span = late // 2

    def kern(tea_ref, x_ref, tab_ref, coef_ref, out_ref, z_buf, g_buf):
        at = peers()[1]

        def block(b, _):
            grad_block(at, tea_ref, x_ref, tab_ref[aligned(late + b * span, span)], coef_ref, z_buf, g_buf, out_ref, b)
            return 0

        lax.fori_loop(0, 2, block, 0)

    return pl.pallas_call(kern, out_shape=jax.ShapeDtypeStruct((2, span, dim), F32), in_specs=[VM] * 4, out_specs=VM,
        scratch_shapes=[pltpu.VMEM((n * tokens, span), F32), pltpu.VMEM((n * tokens, span), BF16)], name='finish',
        compiler_params=pltpu.CompilerParams(vmem_limit_bytes=22 * MIB),
        cost_estimate=pl.CostEstimate(flops=10 ** 9, bytes_accessed=8 * MIB, transcendentals=0))(teas, x_all, tab_part, coef)


def place(table, pieces, vocab):
    arrays = [p[0] for p in pieces]
    n = len(arrays)
    dim = arrays[0].shape[1]
    rows = vocab // N_DP
    quarter = rows // SIDE
    cut = 256
    chunks = []
    for i, (array, dz, dy, kind, start) in enumerate(pieces):
        r = 0
        while r < array.shape[0]:
            row = start + r
            size = min(cut, array.shape[0] - r, quarter - row % quarter)
            chunks.append((i, r, size, dz, dy, row + (row // quarter + kind) * quarter))
            r += size

    def kern(*refs):
        dst, buf, sem = refs[-DOWN:]
        at = peers()[1]
        reads, writes = [], []
        for k, (i, r, size, dz, dy, first) in enumerate(chunks):
            held = buf.at[k, pl.ds(0, size)]
            there = aligned(at[dz, dy] * rows + first, size, 8)
            reads.append(pltpu.make_async_copy(refs[i].at[pl.ds(r, size)], held, sem.at[0, k]))
            writes.append(pltpu.make_async_copy(held, dst.at[there], sem.at[1, k]))
        for cp in reads:
            cp.start()
        for read, write in zip(reads, writes):
            read.wait()
            write.start()
        for cp in writes:
            cp.wait()

    args = arrays if table is None else [*arrays, table]
    size = len(chunks) * cut * dim
    return pl.pallas_call(kern, out_shape=jax.ShapeDtypeStruct((vocab, dim), F32), in_specs=[pl.BlockSpec(memory_space=pl.ANY)] * n + [HB] * (len(args) - n),
        out_specs=HB, scratch_shapes=[pltpu.VMEM((len(chunks), cut, dim), F32), pltpu.SemaphoreType.DMA((2, len(chunks)))],
        input_output_aliases={} if table is None else {n: 0}, name='place', compiler_params=pltpu.CompilerParams(vmem_limit_bytes=4 * size + MIB),
        cost_estimate=pl.CostEstimate(flops=10 * MIB, bytes_accessed=8 * size, transcendentals=0))(*args)


def gather(first, rest, vocab):
    quarter = first[0].shape[0]
    sets, ways = range(2), (UP, DOWN)
    table, event = None, 0

    def send(pair, axis, step):
        out = []
        for k in sets:
            dz, dy = (step, 0) if axis == k else (0, step)
            out.append(lax.ppermute(pair[k], 'dp', [(d, shift(d, dz, dy)) for d in range(N_DP)]))
        return out

    def put(pair, a, b, start=0):
        return [(pair[k], *((b, a) if k else (a, b)), k, start) for k in sets]

    def settle(*pieces):
        nonlocal table
        table = place(table, [p for ps in pieces for p in ps], vocab)

    def wait(*pairs):
        nonlocal table, event
        event += 1
        table, *flat = lax.optimization_barrier((table, *(x for pair in pairs for x in pair)))
        return [flat[2 * i:2 * i + 2] for i in range(len(pairs))]

    def join(one, other):
        return [jnp.concatenate(pair) for pair in zip(one, other)]

    own = [first]
    low, high = ([send(own[0], 0, way)] for way in ways)
    later = rest()
    event = 1
    own.append([later[:quarter], later[quarter:]])
    low.append(send(own[1], 0, UP))
    high.append(send(own[1], 0, DOWN))
    whole = join(*own)
    side = {way: send(whole, 1, way) for way in ways}
    settle(put(own[0], 0, 0, 0), put(own[1], 0, 0, quarter))

    low[0], high[0] = wait(low[0], high[0])
    far_low = send(low[0], 0, UP)
    settle(put(low[0], DOWN, 0, 0), put(high[0], UP, 0, 0))

    low[1], high[1] = wait(low[1], high[1])
    far_high = send(high[1], 0, DOWN)
    low_whole, high_whole = join(*low), join(*high)
    low_side = {way: send(low_whole, 1, way) for way in ways}
    settle(put(low[1], DOWN, 0, quarter), put(high[1], UP, 0, quarter))

    side[UP], side[DOWN], high_whole = wait(side[UP], side[DOWN], high_whole)
    high_side = {way: send(high_whole, 1, way) for way in ways}
    side_far = send(side[UP], 1, UP)
    settle(put(side[UP], 0, DOWN))
    settle(put(side[DOWN], 0, UP))

    far_low, far_high = wait(far_low, far_high)
    far_side = {(c, way): send(pair, 1, way) for way in ways for c, pair in enumerate((far_low, far_high))}
    settle(put(far_low, AWAY, 0, 0), put(far_high, AWAY, 0, quarter))

    low_side[UP], low_side[DOWN] = wait(low_side[UP], low_side[DOWN])
    low_far = send(low_side[DOWN], 1, DOWN)
    settle(put(low_side[UP], DOWN, DOWN))
    settle(put(low_side[DOWN], DOWN, UP))

    high_side[UP], high_side[DOWN] = wait(high_side[UP], high_side[DOWN])
    cut = quarter + TILT
    high_far = [send([x[:cut] for x in high_side[UP]], 1, UP), send([x[cut:] for x in high_side[DOWN]], 1, DOWN)]
    settle(put(high_side[UP], UP, DOWN))
    settle(put(high_side[DOWN], UP, UP))

    far_side[0, DOWN], far_side[1, DOWN], side_far = wait(far_side[0, DOWN], far_side[1, DOWN], side_far)
    ends = slice(0, quarter - LAST), slice(quarter - LAST, quarter)
    last_down = [send([x[end] for x in far_side[1, DOWN]], 1, DOWN) for end in ends]
    settle(put(far_side[0, DOWN], AWAY, UP, 0), put(far_side[1, DOWN], AWAY, UP, quarter))
    settle(put(side_far, 0, AWAY))

    far_side[0, UP], = wait(far_side[0, UP])
    last_up = [send([x[end] for x in far_side[0, UP]], 1, UP) for end in ends]
    settle(put(far_side[0, UP], AWAY, DOWN, 0))

    far_side[1, UP], low_far = wait(far_side[1, UP], low_far)
    settle(put(far_side[1, UP], AWAY, DOWN, quarter))
    settle(put(low_far, DOWN, AWAY))

    high_far = wait(*high_far)
    settle(put(high_far[0], UP, AWAY, 0), put(high_far[1], UP, AWAY, cut))
    for up, down, end in zip(last_up, last_down, ends):
        up, down = wait(up, down)
        settle(put(up, AWAY, AWAY, end.start), put(down, AWAY, AWAY, quarter + end.start))
    return table


def solution(mesh):
    def local_step(hid_rows, w_final, tab_rows, tea_rows, mask_rows):
        tokens = hid_rows.shape[0]
        late, soon, x_all, tab_part, coef, stats, grad_h, gain_line = front(hid_rows, w_final.reshape(-1, LANES), mask_rows[None], tea_rows, tab_rows)
        coef, *first = lax.optimization_barrier((coef, soon[0], soon[1]))
        table = gather(first, lambda: finish(late, x_all, tab_part, coef).reshape(-1, x_all.shape[1]), tab_rows.shape[0])
        s_sum, t_sum, k_sum, masks = (stats[:, i, :tokens] for i in range(SIDE))
        all_kl = k_sum / t_sum + jnp.log(s_sum) - jnp.log(t_sum)
        loss_val = jnp.sum(masks * all_kl) / jnp.sum(masks)
        return loss_val, grad_h.astype(BF16), gain_line[0], table

    return jax.shard_map(local_step, mesh=mesh, in_specs=(P('dp', None), P(None), P('tp', None), P('dp', 'tp'), P('dp')), out_specs=(P(), P('dp', None), P(None), P('tp', None)), check_vma=False)
```

```python
import jax
import jax.numpy as jnp
from jax import lax
from jax.experimental import pallas as pl
from jax.experimental.pallas import tpu as pltpu
from jax.sharding import PartitionSpec as P


SOFT_CAP = 30.0
INV_CAP = 1.0 / SOFT_CAP
NORM_EPS = 1e-6
SIDE, N_DP, N_TP, LANES = 4, 16, 8, 128
UP, DOWN, AWAY = 1, 3, 2
LAST = 128
MIB = 2 ** 20
L_FRONT = 41
MESH = pl.DeviceIdType.MESH
VM = pl.BlockSpec(memory_space=pltpu.VMEM)
HB = pl.BlockSpec(memory_space=pltpu.HBM)
F32, BF16 = jnp.float32, jnp.bfloat16
ROWS_BY_ROWS = (((1,), (1,)), ((), ()))
COLS_BY_COLS = (((0,), (0,)), ((), ()))

OFFSETS = tuple((dz, dy) for dz in range(SIDE) for dy in range(SIDE))
ORDER = tuple(sorted(OFFSETS, key=lambda o: -sum(min(d, SIDE - d) for d in o)))


def shift(dp, dz, dy):
    return (dp // SIDE + dz + SIDE) % SIDE * SIDE + (dp % SIDE + dy + SIDE) % SIDE


def peers():
    me = lax.axis_index('dp')
    z, y = lax.div(me, SIDE), lax.rem(me, SIDE)
    zs = [lax.rem(z + d, SIDE) * SIDE for d in range(SIDE)]
    ys = [lax.rem(y + d, SIDE) for d in range(SIDE)]
    return me, {(dz, dy): zs[dz] + ys[dy] for dz in range(-DOWN, SIDE) for dy in range(-DOWN, SIDE)}


def aligned(start, size, unit=LANES):
    return pl.ds(pl.multiple_of(start, unit), size)


def hops(kind, dz, dy):
    along_z = [(dz, 0)] if dz % 2 else [(UP if dy < AWAY else DOWN, 0)] * dz
    along_y = [(0, dy)] if dy % 2 else [(0, UP if dz < AWAY else DOWN)] * dy
    return along_y + along_z if kind else along_z + along_y


JOBS = tuple((kind, o) for o in ORDER[:-1] for kind in range(2))
PATHS = tuple(hops(kind, *o) for kind, o in JOBS)
MIDDLE = tuple((j, level) for level in range(SIDE) for j, path in enumerate(PATHS) if len(path) > level + 1)


def waves(j, level):
    return (None,) if (j, level) in MIDDLE and level < 2 else (0, 1)


def grad_block(at, tea_ref, x_ref, tab_rows, coef_ref, z_buf, g_buf, out_ref, block):
    tokens = tea_ref.shape[1]
    span = tab_rows.shape[0]
    few = LANES // N_DP
    cols = aligned(block * span, span)
    z_buf[:, :span] = lax.dot_general(x_ref[...], tab_rows, ROWS_BY_ROWS, preferred_element_type=F32)
    for k, (dz, dy) in enumerate(OFFSETS):
        here = aligned(at[-dz, -dy] * tokens, tokens, tokens)
        ratio = jnp.tanh(z_buf[here, :span] * INV_CAP)
        stu = jnp.exp(SOFT_CAP * ratio - SOFT_CAP)
        inv_s, inv_t, _, weight = (coef_ref[0:tokens, k * few + i:k * few + i + 1] for i in range(SIDE))
        diff = (stu * inv_s - tea_ref[k, :, cols] * inv_t) * weight
        g_buf[here, :span] = (diff * (1.0 - ratio * ratio)).astype(BF16)
    out_ref[block] = lax.dot_general(g_buf[:, :span], x_ref[...], COLS_BY_COLS, preferred_element_type=F32)


def front(hidden, gain_row, mask_row, teacher, table):
    tokens, vocab = teacher.shape
    dim = hidden.shape[1]
    part = vocab // N_DP
    half = tokens // 2
    few = tokens // N_TP
    pack = 16
    sub = 512
    per = part // sub
    tiles = vocab // sub
    depth = 2 * per
    ring = N_DP // 2
    few_first = 3

    def kern(hid_hbm, gain_hbm, mask_hbm, tea_ref, tab_ref, got_late, blocks_ref, x_out, tab_out, coef_ref, all_ref, gh_ref, gg_ref,
             hid_ref, gain_ref, mask_in, w_ref, raw, sends, stage, got_soon, g_buf, t_acc, c_acc, tabs, n_buf, x_buf, inv_buf, square, pay, pay_got, mask_own, mask_got, x_got, tp_got, own_col,
             own_row, rel, dx, rs_got, ag_own, ag_got, gn_own, gn_got, raw_sem, tab_sem, in_sem, hop_out, hop_in, dp_sem, tp_sem):
        me, at = peers()
        col = lax.axis_index('tp')
        mates = [lax.rem(col + j, N_TP) for j in range(N_TP)]
        my_few = aligned(col * few, few, few)

        def fetch(k):
            d = at[ORDER[k]]
            return pltpu.make_async_copy(tea_ref.at[:, aligned(d * part, part)], raw.at[pl.ds(k % ring * tokens, tokens)], raw_sem.at[k % ring])

        def tab_copy(i):
            slot = lax.rem(i, depth)
            return pltpu.make_async_copy(tab_ref.at[aligned(lax.rem(i, tiles) * sub, sub)], tabs.at[slot], tab_sem.at[slot])

        inputs = [pltpu.make_async_copy(src, dst, in_sem.at[2 + i])
                  for i, (src, dst) in enumerate(((hid_hbm, hid_ref), (gain_hbm, gain_ref), (mask_hbm, mask_in)))]
        own_tab = pltpu.make_async_copy(tab_ref.at[aligned(me * part, part)], tab_out, in_sem.at[1])
        for cp in inputs:
            cp.start()
        for k in range(ring):
            fetch(k).start()
        for i in range(per):
            tab_copy(i).start()
        own_tab.start()
        all_ref[...] = jnp.zeros(all_ref.shape, F32)
        barrier = pltpu.get_barrier_semaphore()
        for dz, dy in ORDER[:-1]:
            pl.semaphore_signal(barrier, inc=1, device_id=(at[dz, dy], col), device_id_type=MESH)
        for j in range(1, N_TP):
            pl.semaphore_signal(barrier, inc=1, device_id=(me, mates[j]), device_id_type=MESH)

        def fold(v):
            total = v[:, :LANES]
            for c in range(LANES, v.shape[1], LANES):
                total = total + v[:, c:c + LANES]
            return total

        def weigh(k):
            fetch(k).wait()
            d = at[ORDER[k]]

            def rows(r, _):
                here = aligned(r * pack, pack, pack)
                cap = jnp.tanh(raw[aligned(k % ring * tokens + r * pack, pack, pack)].astype(F32) * INV_CAP)
                tea = jnp.exp(SOFT_CAP * cap - SOFT_CAP)
                sends[aligned(d * tokens + r * pack, pack, pack)] = tea
                t_acc[here] += fold(tea)
                c_acc[here] += fold(tea * cap)
                return 0

            lax.fori_loop(0, tokens // pack, rows, 0)
            if k + ring < N_DP:
                fetch(k + ring).start()

        t_acc[...] = jnp.zeros((tokens, LANES), F32)
        c_acc[...] = jnp.zeros((tokens, LANES), F32)
        weigh(0)
        pl.semaphore_wait(barrier, N_DP + N_TP - 2)

        def remote(src, dst, out, into, dp, tp):
            return pltpu.make_async_remote_copy(src_ref=src, dst_ref=dst, send_sem=out, recv_sem=into, device_id=(dp, tp), device_id_type=MESH)

        def whole(ref, sem):
            pltpu.make_async_copy(ref, ref, sem).wait()

        def to_dp(src, dst, x, rows=slice(None)):
            for o in ORDER[:-1]:
                remote(src.at[rows], dst.at[me, rows], dp_sem.at[x, 0], dp_sem.at[x, 1], at[o], col).start()
            others = dst.at[pl.ds(0, N_DP - 1), rows]
            return [(others, dp_sem.at[x, 0])], lambda: whole(others, dp_sem.at[x, 1])

        def to_tp(srcs, dst, x):
            for c in mates[1:]:
                remote(srcs(c), dst.at[col], tp_sem.at[x, 0], tp_sem.at[x, 1], me, c).start()
            others = dst.at[pl.ds(0, N_TP - 1)]
            return [(others, tp_sem.at[x, 0])], lambda: whole(others, tp_sem.at[x, 1])

        def added(ref, here=slice(None)):
            total = ref[0, here]
            for d in range(1, ref.shape[0]):
                total = total + ref[d, here]
            return total

        gots = (got_soon, got_late)
        late = part // 2

        def hop(j, level, w):
            kind, (dz, dy) = JOBS[j]
            tok = pl.ds(kind * half, half)
            rows = slice(None) if w is None else pl.ds(w * late, late)
            src = stage.at[MIDDLE.index((j, level - 1)), :, rows] if level else sends.at[aligned(at[dz, dy] * tokens + kind * half, half, half), rows]
            dst = stage.at[MIDDLE.index((j, level)), :, rows] if (j, level) in MIDDLE else gots[w].at[dz * SIDE + dy, tok]
            into = (level if w is None else level + w) if (j, level) in MIDDLE else SIDE + w
            return remote(src, dst, hop_out.at[min(level, 1)], hop_in.at[into], at[PATHS[j][level]], col)

        def came(level, w=None):
            n = sum(at == level for _, at in MIDDLE)
            rows = slice(None) if w is None else pl.ds(0, late)
            whole(stage.at[pl.ds(0, n), :, rows], hop_in.at[level + (w or 0)])

        def onward(level, far, *ws):
            for w in ws:
                for j, at in MIDDLE:
                    if at == level - 1 and far == (len(PATHS[j]) > 2):
                        hop(j, level, w).start()

        def issue(k):
            for j, (_, to) in enumerate(JOBS):
                if to == ORDER[k]:
                    for w in waves(j, 0):
                        hop(j, 0, w).start()

        issue(0)
        for k in range(1, few_first):
            weigh(k)
            issue(k)
        for cp in inputs:
            cp.wait()
        w_ref[...] = 1.0 + jnp.concatenate([gain_ref[i:i + 1] for i in range(dim // LANES)], axis=1)
        hid = hid_ref[...].astype(F32)
        inv = lax.rsqrt(jnp.mean(hid * hid, axis=1, keepdims=True) + NORM_EPS)
        n_buf[...] = hid * inv
        x_buf[...] = (n_buf[...] * w_ref[...]).astype(BF16)
        inv_buf[...] = jnp.broadcast_to(inv, (tokens, LANES))
        pay[...] = n_buf[my_few]
        square[...] = jnp.zeros((LANES, LANES), F32)
        square[0:1, 0:tokens] = mask_in[...]
        mask_own[...] = square[0:few]
        mask_col = jnp.transpose(square[...])[0:tokens, 0:1]
        pay_sent, pay_came = to_dp(pay, pay_got, 0)
        pay_got[me] = pay[...]
        mask_sent, mask_came = to_dp(mask_own, mask_got, 1, pl.ds(0, 1))
        mask_got[me] = mask_own[...]
        for k in range(few_first, N_DP):
            weigh(k)
            issue(k)

        def keep(r, _):
            here, there = aligned(me * tokens + r * pack, pack, pack), aligned(r * pack, pack, pack)
            got_soon[0, there] = sends[here, :late]
            got_late[0, there] = sends[here, late:]
            return 0

        lax.fori_loop(0, tokens // pack, keep, 0)

        def student(slot):
            z = lax.dot_general(x_buf[...], tabs[slot], ROWS_BY_ROWS, preferred_element_type=F32)
            ratio = jnp.tanh(z * INV_CAP)
            return ratio, jnp.exp(SOFT_CAP * ratio - SOFT_CAP)

        def next_tiles(i):
            for c in range(per):
                tab_copy(i * per + c).wait()

            @pl.when(i + 1 < 2 * N_DP)
            def _():
                for c in range(per):
                    tab_copy((i + 1) * per + c).start()

            return [lax.rem(i, 2) * per + c for c in range(per)]

        def forward(i, sums):
            s_sum, k_sum = sums
            slots = next_tiles(i)
            for c in range(per):
                ratio, stu = student(slots[c])
                tea = sends[aligned(i * tokens, tokens, tokens), pl.ds(c * sub, sub)]
                s_sum, k_sum = s_sum + fold(stu), k_sum + fold(tea * ratio)
            return s_sum, k_sum

        zero = jnp.zeros((tokens, LANES), F32)
        s_sum, k_sum = lax.fori_loop(0, N_DP, forward, (zero, zero))
        lane = lax.broadcasted_iota(jnp.int32, (tokens, LANES), 1)
        sums = jnp.where(lane == 0, jnp.sum(s_sum, axis=1, keepdims=True), 0.0)
        sums = jnp.where(lane == 1, jnp.sum(t_acc[...], axis=1, keepdims=True), sums)
        sums = jnp.where(lane == AWAY, SOFT_CAP * jnp.sum(c_acc[...] - k_sum, axis=1, keepdims=True), sums)
        own_col[...] = sums
        tp_got[col] = sums
        tp_sent, tp_came = to_tp(lambda c: own_col, tp_got, 0)
        tp_came()
        total = added(tp_got)
        square[0:tokens] = jnp.where(lane == DOWN, mask_col, total)
        line = jnp.transpose(square[...])[0:few]
        own_row[...] = line
        all_ref[me] = line
        dp_sent, dp_came = to_dp(own_row, all_ref, 2, pl.ds(0, SIDE))
        twin = col + 1 - 2 * lax.rem(col, 2)
        pay_came()
        mask_came()
        x_got[col] = pay_got[...]

        evens = range(0, N_TP, 2)
        for j in evens[1:]:
            remote(pay_got, x_got.at[col], tp_sem.at[1, 0], tp_sem.at[1, 1], me, mates[j]).start()
        came(0)
        onward(1, True, None)
        onward(1, False, 0)

        count = jnp.sum(added(mask_got, slice(1)), axis=1, keepdims=True)
        inv_s, inv_t, weight = 1.0 / total[:, 0:1], 1.0 / total[:, 1:2], mask_col / count
        dx[...] = jnp.zeros((tokens, dim), F32)

        def backward(i, _):
            slots = next_tiles(i)
            total = dx[...]
            for c in range(per):
                ratio, stu = student(slots[c])
                tea = sends[aligned((i - N_DP) * tokens, tokens, tokens), pl.ds(c * sub, sub)]
                diff = (stu * inv_s - tea * inv_t) * weight
                g = (diff * (1.0 - ratio * ratio)).astype(BF16)
                total = total + jnp.dot(g, tabs[slots[c]], preferred_element_type=F32)
            dx[...] = total
            return 0

        lax.fori_loop(N_DP, 2 * N_DP, backward, 0)
        came(1)
        onward(2, True, 0)
        onward(1, False, 1)
        whole(x_got.at[pl.ds(0, SIDE - 1)], tp_sem.at[1, 1])
        for j in evens:
            remote(x_got.at[mates[j]], x_got.at[mates[j]], tp_sem.at[SIDE, 0], tp_sem.at[SIDE, 1], me, twin).start()

        rs_got[col] = dx[my_few]
        rs_sent, rs_came = to_tp(lambda c: dx.at[aligned(c * few, few, few)], rs_got, 2)
        rs_came()
        my_x = added(rs_got)
        my_n = n_buf[my_few]
        grad_n = my_x * w_ref[...]
        my_h = inv_buf[my_few, 0:1] * (grad_n - my_n * jnp.mean(grad_n * my_n, axis=1, keepdims=True))
        ag_own[...] = jnp.zeros((2 * few, dim), F32)
        ag_own[0:few] = my_h
        ag_own[few:few + 1] = jnp.sum(my_x * my_n, axis=0, keepdims=True)
        ag_got[col] = ag_own[...]
        ag_sent, ag_came = to_tp(lambda c: ag_own, ag_got, DOWN)
        ag_came()
        gh_ref[...] = jnp.concatenate([ag_got[j, 0:few] for j in range(N_TP)], axis=0)
        line = added(ag_got, slice(few, few + 1))
        gn_own[0:1] = line
        gn_got[me, 0:1] = line
        gn_sent, gn_came = to_dp(gn_own, gn_got, DOWN, pl.ds(0, 1))

        came(2, 0)
        onward(DOWN, True, 0)
        onward(2, True, 1)
        whole(x_got.at[pl.ds(0, SIDE)], tp_sem.at[SIDE, 1])

        def widen(d, _):
            rows = jnp.concatenate([x_got[j, d] for j in range(N_TP)], axis=0)
            x_out[aligned(d * tokens, tokens, tokens)] = (rows * w_ref[...]).astype(BF16)
            return 0

        lax.fori_loop(0, N_DP, widen, 0)
        dp_came()
        row = lax.broadcasted_iota(jnp.int32, (few, LANES), 0)
        lanes = lax.broadcasted_iota(jnp.int32, (few, LANES), 1)
        for d in range(N_DP):
            block = all_ref[d]
            safe = jnp.where((row < AWAY) & (lanes < tokens), block, 1.0)
            rel[d * few:(d + 1) * few] = jnp.where(row < AWAY, 1.0 / safe, block / count)
        for k, (dz, dy) in enumerate(OFFSETS):
            square[k * few:(k + 1) * few] = rel[aligned(at[-dz, -dy] * few, few, few)]
        coef_ref[...] = jnp.transpose(square[...])

        own_tab.wait()
        whole(got_soon.at[pl.ds(0, N_DP - 1)], hop_in.at[SIDE])
        whole(sends.at[pl.ds(0, len(JOBS) * half)], hop_out.at[0])

        def block(b, _):
            @pl.when(b == 1)
            def _():
                came(2, 1)
                onward(DOWN, True, 1)

            grad_block(at, got_soon, x_out, tab_out[aligned(b * sub, sub)], coef_ref, sends, g_buf, blocks_ref, b)
            return 0

        lax.fori_loop(0, 2, block, 0)
        gn_came()
        gg_ref[...] = added(gn_got, slice(1))
        whole(got_late.at[pl.ds(0, N_DP - 1)], hop_in.at[SIDE + 1])
        whole(stage, hop_out.at[1])
        for ref, sem in (*pay_sent, *mask_sent, *tp_sent, *dp_sent, *rs_sent, *ag_sent, *gn_sent):
            whole(ref, sem)
        whole(x_got.at[pl.ds(0, SIDE - 1)], tp_sem.at[1, 0])
        whole(x_got.at[pl.ds(0, SIDE)], tp_sem.at[SIDE, 0])

    dma = pltpu.SemaphoreType.DMA
    wide, flat = (tokens, dim), (few, LANES)
    return pl.pallas_call(
        kern,
        out_shape=tuple(jax.ShapeDtypeStruct(shape, kind) for shape, kind in (
            ((N_DP, tokens, part // 2), F32), ((2, sub, dim), F32), ((N_DP * tokens, dim), BF16), ((part, dim), BF16), ((LANES, LANES), F32), ((N_DP, *flat), F32), (wide, F32),
            ((1, dim), F32))),
        in_specs=[HB] * 5, out_specs=(VM,) * 8,
        scratch_shapes=[pltpu.VMEM(shape, kind) for shape, kind in (
            (wide, BF16), ((dim // LANES, LANES), F32), ((1, tokens), F32), ((1, dim), F32), ((ring * tokens, part), BF16), ((N_DP * tokens, part), F32),
            ((len(MIDDLE), half, part), F32), ((N_DP, tokens, part // 2), F32), ((N_DP * tokens, sub), BF16), ((tokens, LANES), F32), ((tokens, LANES), F32),
            ((depth, sub, dim), BF16), (wide, F32), (wide, BF16), ((tokens, LANES), F32), ((LANES, LANES), F32), ((few, dim), F32),
            ((N_DP, few, dim), F32), (flat, F32), ((N_DP, *flat), F32), ((N_TP, N_DP, few, dim), F32), ((N_TP, tokens, LANES), F32),
            ((tokens, LANES), F32), (flat, F32), ((LANES, LANES), F32), (wide, F32), ((N_TP, few, dim), F32), ((2 * few, dim), F32),
            ((N_TP, 2 * few, dim), F32), ((few, dim), F32), ((N_DP, few, dim), F32))] + [
            dma((ring,)), dma((depth,)), dma((5,)), dma((2,)), dma((SIDE + 2,)), dma((SIDE, 2)), dma((SIDE + 1, 2))],
        compiler_params=pltpu.CompilerParams(collective_id=0, has_side_effects=True, vmem_limit_bytes=L_FRONT * MIB),
        cost_estimate=pl.CostEstimate(flops=3 * 10 ** 9, bytes_accessed=100 * MIB, transcendentals=0), name='front')(
            *(pltpu.with_memory_space_constraint(a, pltpu.HBM) for a in (hidden, gain_row, mask_row, teacher, table)))


def finish(teas, x_all, tab_part, coef):
    n, tokens, late = teas.shape
    dim = x_all.shape[1]
    span = late // 2

    def kern(tea_ref, x_ref, tab_ref, coef_ref, out_ref, z_buf, g_buf):
        at = peers()[1]

        def block(b, _):
            grad_block(at, tea_ref, x_ref, tab_ref[aligned(late + b * span, span)], coef_ref, z_buf, g_buf, out_ref, b)
            return 0

        lax.fori_loop(0, 2, block, 0)

    return pl.pallas_call(kern, out_shape=jax.ShapeDtypeStruct((2, span, dim), F32), in_specs=[VM] * 4, out_specs=VM,
        scratch_shapes=[pltpu.VMEM((n * tokens, span), F32), pltpu.VMEM((n * tokens, span), BF16)], name='finish',
        compiler_params=pltpu.CompilerParams(vmem_limit_bytes=22 * MIB),
        cost_estimate=pl.CostEstimate(flops=10 ** 9, bytes_accessed=8 * MIB, transcendentals=0))(teas, x_all, tab_part, coef)


def place(table, pieces, vocab):
    arrays = [p[0] for p in pieces]
    n = len(arrays)
    dim = arrays[0].shape[1]
    rows = vocab // N_DP
    quarter = rows // SIDE
    cut = 256
    chunks = []
    for i, (array, dz, dy, kind, start) in enumerate(pieces):
        r = 0
        while r < array.shape[0]:
            row = start + r
            size = min(cut, array.shape[0] - r, quarter - row % quarter)
            chunks.append((i, r, size, dz, dy, row + (row // quarter + kind) * quarter))
            r += size

    def kern(*refs):
        dst, buf, sem = refs[-DOWN:]
        at = peers()[1]
        reads, writes = [], []
        for k, (i, r, size, dz, dy, first) in enumerate(chunks):
            held = buf.at[k, pl.ds(0, size)]
            there = aligned(at[dz, dy] * rows + first, size, 8)
            reads.append(pltpu.make_async_copy(refs[i].at[pl.ds(r, size)], held, sem.at[0, k]))
            writes.append(pltpu.make_async_copy(held, dst.at[there], sem.at[1, k]))
        for cp in reads:
            cp.start()
        for read, write in zip(reads, writes):
            read.wait()
            write.start()
        for cp in writes:
            cp.wait()

    args = arrays if table is None else [*arrays, table]
    size = len(chunks) * cut * dim
    return pl.pallas_call(kern, out_shape=jax.ShapeDtypeStruct((vocab, dim), F32), in_specs=[pl.BlockSpec(memory_space=pl.ANY)] * n + [HB] * (len(args) - n),
        out_specs=HB, scratch_shapes=[pltpu.VMEM((len(chunks), cut, dim), F32), pltpu.SemaphoreType.DMA((2, len(chunks)))],
        input_output_aliases={} if table is None else {n: 0}, name='place', compiler_params=pltpu.CompilerParams(vmem_limit_bytes=4 * size + MIB),
        cost_estimate=pl.CostEstimate(flops=10 * MIB, bytes_accessed=8 * size, transcendentals=0))(*args)


def gather(first, rest, vocab):
    quarter = first[0].shape[0]
    sets, ways = range(2), (UP, DOWN)
    table, event = None, 0

    def send(pair, axis, step):
        out = []
        for k in sets:
            dz, dy = (step, 0) if axis == k else (0, step)
            out.append(lax.ppermute(pair[k], 'dp', [(d, shift(d, dz, dy)) for d in range(N_DP)]))
        return out

    def put(pair, a, b, start=0):
        return [(pair[k], *((b, a) if k else (a, b)), k, start) for k in sets]

    def settle(*pieces):
        nonlocal table
        table = place(table, [p for ps in pieces for p in ps], vocab)

    def wait(*pairs):
        nonlocal table, event
        event += 1
        table, *flat = lax.optimization_barrier((table, *(x for pair in pairs for x in pair)))
        return [flat[2 * i:2 * i + 2] for i in range(len(pairs))]

    def join(one, other):
        return [jnp.concatenate(pair) for pair in zip(one, other)]

    own = [first]
    low, high = ([send(own[0], 0, way)] for way in ways)
    later = rest()
    event = 1
    own.append([later[:quarter], later[quarter:]])
    low.append(send(own[1], 0, UP))
    high.append(send(own[1], 0, DOWN))
    whole = join(*own)
    side = {way: send(whole, 1, way) for way in ways}
    settle(put(own[0], 0, 0, 0), put(own[1], 0, 0, quarter))

    low[0], high[0] = wait(low[0], high[0])
    far_low = send(low[0], 0, UP)
    settle(put(low[0], DOWN, 0, 0), put(high[0], UP, 0, 0))

    low[1], high[1] = wait(low[1], high[1])
    far_high = send(high[1], 0, DOWN)
    low_whole, high_whole = join(*low), join(*high)
    low_side = {way: send(low_whole, 1, way) for way in ways}
    settle(put(low[1], DOWN, 0, quarter), put(high[1], UP, 0, quarter))

    side[UP], side[DOWN], high_whole = wait(side[UP], side[DOWN], high_whole)
    high_side = {way: send(high_whole, 1, way) for way in ways}
    side_far = send(side[UP], 1, UP)
    settle(put(side[UP], 0, DOWN))
    settle(put(side[DOWN], 0, UP))

    far_low, far_high = wait(far_low, far_high)
    far_side = {(c, way): send(pair, 1, way) for way in ways for c, pair in enumerate((far_low, far_high))}
    settle(put(far_low, AWAY, 0, 0), put(far_high, AWAY, 0, quarter))

    low_side[UP], low_side[DOWN] = wait(low_side[UP], low_side[DOWN])
    low_far = send(low_side[DOWN], 1, DOWN)
    settle(put(low_side[UP], DOWN, DOWN))
    settle(put(low_side[DOWN], DOWN, UP))

    high_side[UP], high_side[DOWN] = wait(high_side[UP], high_side[DOWN])
    high_far = [send([x[:quarter] for x in high_side[UP]], 1, UP), send([x[quarter:] for x in high_side[DOWN]], 1, DOWN)]
    settle(put(high_side[UP], UP, DOWN))
    settle(put(high_side[DOWN], UP, UP))

    far_side[0, DOWN], far_side[1, DOWN], side_far = wait(far_side[0, DOWN], far_side[1, DOWN], side_far)
    ends = slice(0, quarter - LAST), slice(quarter - LAST, quarter)
    last_down = [send([x[end] for x in far_side[1, DOWN]], 1, DOWN) for end in ends]
    settle(put(far_side[0, DOWN], AWAY, UP, 0), put(far_side[1, DOWN], AWAY, UP, quarter))
    settle(put(side_far, 0, AWAY))

    far_side[0, UP], = wait(far_side[0, UP])
    last_up = [send([x[end] for x in far_side[0, UP]], 1, UP) for end in ends]
    settle(put(far_side[0, UP], AWAY, DOWN, 0))

    far_side[1, UP], low_far = wait(far_side[1, UP], low_far)
    settle(put(far_side[1, UP], AWAY, DOWN, quarter))
    settle(put(low_far, DOWN, AWAY))

    high_far = wait(*high_far)
    settle(put(high_far[0], UP, AWAY, 0), put(high_far[1], UP, AWAY, quarter))
    for up, down, end in zip(last_up, last_down, ends):
        up, down = wait(up, down)
        settle(put(up, AWAY, AWAY, end.start), put(down, AWAY, AWAY, quarter + end.start))
    return table


def solution(mesh):
    def local_step(hid_rows, w_final, tab_rows, tea_rows, mask_rows):
        tokens = hid_rows.shape[0]
        late, soon, x_all, tab_part, coef, stats, grad_h, gain_line = front(hid_rows, w_final.reshape(-1, LANES), mask_rows[None], tea_rows, tab_rows)
        coef, *first = lax.optimization_barrier((coef, soon[0], soon[1]))
        table = gather(first, lambda: finish(late, x_all, tab_part, coef).reshape(-1, x_all.shape[1]), tab_rows.shape[0])
        s_sum, t_sum, k_sum, masks = (stats[:, i, :tokens] for i in range(SIDE))
        all_kl = k_sum / t_sum + jnp.log(s_sum) - jnp.log(t_sum)
        loss_val = jnp.sum(masks * all_kl) / jnp.sum(masks)
        return loss_val, grad_h.astype(BF16), gain_line[0], table

    return jax.shard_map(local_step, mesh=mesh, in_specs=(P('dp', None), P(None), P('tp', None), P('dp', 'tp'), P('dp')), out_specs=(P(), P('dp', None), P(None), P('tp', None)), check_vma=False)
```

```python
import jax
import jax.numpy as jnp
from jax import lax
from jax.experimental import pallas as pl
from jax.experimental.pallas import tpu as pltpu
from jax.sharding import PartitionSpec as P


SOFT_CAP = 30.0
INV_CAP = 1.0 / SOFT_CAP
NORM_EPS = 1e-6
SIDE, N_DP, N_TP, LANES = 4, 16, 8, 128
UP, DOWN, AWAY = 1, 3, 2
LAST = 128
MIB = 2 ** 20
L_FRONT = 41
MESH = pl.DeviceIdType.MESH
VM = pl.BlockSpec(memory_space=pltpu.VMEM)
HB = pl.BlockSpec(memory_space=pltpu.HBM)
F32, BF16 = jnp.float32, jnp.bfloat16
ROWS_BY_ROWS = (((1,), (1,)), ((), ()))
COLS_BY_COLS = (((0,), (0,)), ((), ()))

OFFSETS = tuple((dz, dy) for dz in range(SIDE) for dy in range(SIDE))
ORDER = tuple(sorted(OFFSETS, key=lambda o: -sum(min(d, SIDE - d) for d in o)))


def shift(dp, dz, dy):
    return (dp // SIDE + dz + SIDE) % SIDE * SIDE + (dp % SIDE + dy + SIDE) % SIDE


def peers():
    me = lax.axis_index('dp')
    z, y = lax.div(me, SIDE), lax.rem(me, SIDE)
    zs = [lax.rem(z + d, SIDE) * SIDE for d in range(SIDE)]
    ys = [lax.rem(y + d, SIDE) for d in range(SIDE)]
    return me, {(dz, dy): zs[dz] + ys[dy] for dz in range(-DOWN, SIDE) for dy in range(-DOWN, SIDE)}


def aligned(start, size, unit=LANES):
    return pl.ds(pl.multiple_of(start, unit), size)


def hops(kind, dz, dy):
    along_z = [(dz, 0)] if dz % 2 else [(UP if dy < AWAY else DOWN, 0)] * dz
    along_y = [(0, dy)] if dy % 2 else [(0, UP if dz < AWAY else DOWN)] * dy
    return along_y + along_z if kind else along_z + along_y


JOBS = tuple((kind, o) for o in ORDER[:-1] for kind in range(2))
PATHS = tuple(hops(kind, *o) for kind, o in JOBS)
MIDDLE = tuple((j, level) for level in range(SIDE) for j, path in enumerate(PATHS) if len(path) > level + 1)


def waves(j, level):
    return (None,) if (j, level) in MIDDLE else (0, 1)


def grad_block(at, tea_ref, x_ref, tab_rows, coef_ref, z_buf, g_buf, out_ref, block):
    tokens = tea_ref.shape[1]
    span = tab_rows.shape[0]
    few = LANES // N_DP
    cols = aligned(block * span, span)
    z_buf[:, :span] = lax.dot_general(x_ref[...], tab_rows, ROWS_BY_ROWS, preferred_element_type=F32)
    for k, (dz, dy) in enumerate(OFFSETS):
        here = aligned(at[-dz, -dy] * tokens, tokens, tokens)
        ratio = jnp.tanh(z_buf[here, :span] * INV_CAP)
        stu = jnp.exp(SOFT_CAP * ratio - SOFT_CAP)
        inv_s, inv_t, _, weight = (coef_ref[0:tokens, k * few + i:k * few + i + 1] for i in range(SIDE))
        diff = (stu * inv_s - tea_ref[k, :, cols] * inv_t) * weight
        g_buf[here, :span] = (diff * (1.0 - ratio * ratio)).astype(BF16)
    out_ref[block] = lax.dot_general(g_buf[:, :span], x_ref[...], COLS_BY_COLS, preferred_element_type=F32)


def front(hidden, gain_row, mask_row, teacher, table):
    tokens, vocab = teacher.shape
    dim = hidden.shape[1]
    part = vocab // N_DP
    half = tokens // 2
    few = tokens // N_TP
    pack = 16
    sub = 512
    per = part // sub
    tiles = vocab // sub
    depth = 2 * per
    ring = N_DP // 2
    few_first, before_lines = 2, 9

    def kern(hid_hbm, gain_hbm, mask_hbm, tea_ref, tab_ref, got_late, blocks_ref, x_out, tab_out, coef_ref, all_ref, gh_ref, gg_ref,
             hid_ref, gain_ref, mask_in, w_ref, raw, sends, stage, got_soon, g_buf, t_acc, c_acc, tabs, n_buf, x_buf, inv_buf, square, pay, pay_got, mask_own, mask_got, x_got, tp_got, own_col,
             own_row, rel, dx, rs_got, ag_own, ag_got, gn_own, gn_got, raw_sem, tab_sem, in_sem, hop_out, hop_in, dp_sem, tp_sem):
        me, at = peers()
        col = lax.axis_index('tp')
        mates = [lax.rem(col + j, N_TP) for j in range(N_TP)]
        my_few = aligned(col * few, few, few)

        def fetch(k):
            d = at[ORDER[k]]
            return pltpu.make_async_copy(tea_ref.at[:, aligned(d * part, part)], raw.at[pl.ds(k % ring * tokens, tokens)], raw_sem.at[k % ring])

        def tab_copy(i):
            slot = lax.rem(i, depth)
            return pltpu.make_async_copy(tab_ref.at[aligned(lax.rem(i, tiles) * sub, sub)], tabs.at[slot], tab_sem.at[slot])

        inputs = [pltpu.make_async_copy(src, dst, in_sem.at[2 + i])
                  for i, (src, dst) in enumerate(((hid_hbm, hid_ref), (gain_hbm, gain_ref), (mask_hbm, mask_in)))]
        own_tab = pltpu.make_async_copy(tab_ref.at[aligned(me * part, part)], tab_out, in_sem.at[1])
        for cp in inputs:
            cp.start()
        for k in range(ring):
            fetch(k).start()
        for i in range(per):
            tab_copy(i).start()
        own_tab.start()
        all_ref[...] = jnp.zeros(all_ref.shape, F32)
        barrier = pltpu.get_barrier_semaphore()
        for dz, dy in ORDER[:-1]:
            pl.semaphore_signal(barrier, inc=1, device_id=(at[dz, dy], col), device_id_type=MESH)
        for j in range(1, N_TP):
            pl.semaphore_signal(barrier, inc=1, device_id=(me, mates[j]), device_id_type=MESH)

        def fold(v):
            total = v[:, :LANES]
            for c in range(LANES, v.shape[1], LANES):
                total = total + v[:, c:c + LANES]
            return total

        def weigh(k):
            fetch(k).wait()
            d = at[ORDER[k]]

            def rows(r, _):
                here = aligned(r * pack, pack, pack)
                cap = jnp.tanh(raw[aligned(k % ring * tokens + r * pack, pack, pack)].astype(F32) * INV_CAP)
                tea = jnp.exp(SOFT_CAP * cap - SOFT_CAP)
                sends[aligned(d * tokens + r * pack, pack, pack)] = tea
                t_acc[here] += fold(tea)
                c_acc[here] += fold(tea * cap)
                return 0

            lax.fori_loop(0, tokens // pack, rows, 0)
            if k + ring < N_DP:
                fetch(k + ring).start()

        t_acc[...] = jnp.zeros((tokens, LANES), F32)
        c_acc[...] = jnp.zeros((tokens, LANES), F32)
        weigh(0)
        pl.semaphore_wait(barrier, N_DP + N_TP - 2)

        def remote(src, dst, out, into, dp, tp):
            return pltpu.make_async_remote_copy(src_ref=src, dst_ref=dst, send_sem=out, recv_sem=into, device_id=(dp, tp), device_id_type=MESH)

        def whole(ref, sem):
            pltpu.make_async_copy(ref, ref, sem).wait()

        def to_dp(src, dst, x, rows=slice(None)):
            for o in ORDER[:-1]:
                remote(src.at[rows], dst.at[me, rows], dp_sem.at[x, 0], dp_sem.at[x, 1], at[o], col).start()
            others = dst.at[pl.ds(0, N_DP - 1), rows]
            return [(others, dp_sem.at[x, 0])], lambda: whole(others, dp_sem.at[x, 1])

        def to_tp(srcs, dst, x):
            for c in mates[1:]:
                remote(srcs(c), dst.at[col], tp_sem.at[x, 0], tp_sem.at[x, 1], me, c).start()
            others = dst.at[pl.ds(0, N_TP - 1)]
            return [(others, tp_sem.at[x, 0])], lambda: whole(others, tp_sem.at[x, 1])

        def added(ref, here=slice(None)):
            total = ref[0, here]
            for d in range(1, ref.shape[0]):
                total = total + ref[d, here]
            return total

        gots = (got_soon, got_late)
        late = part // 2

        def hop(j, level, w):
            kind, (dz, dy) = JOBS[j]
            tok = pl.ds(kind * half, half)
            rows = slice(None) if w is None else pl.ds(w * late, late)
            src = stage.at[MIDDLE.index((j, level - 1)), :, rows] if level else sends.at[aligned(at[dz, dy] * tokens + kind * half, half, half), rows]
            dst = stage.at[MIDDLE.index((j, level)), :, rows] if (j, level) in MIDDLE else gots[w].at[dz * SIDE + dy, tok]
            into = level if (j, level) in MIDDLE else SIDE + w
            return remote(src, dst, hop_out.at[min(level, 1)], hop_in.at[into], at[PATHS[j][level]], col)

        def came(level):
            n = sum(at == level for _, at in MIDDLE)
            whole(stage.at[pl.ds(0, n)], hop_in.at[level])

        def onward(level, far, *ws):
            for w in ws:
                for j, at in MIDDLE:
                    if at == level - 1 and far == (len(PATHS[j]) > 2):
                        if (j, level) not in MIDDLE:
                            hop(j, level, w).start()
                        elif w != 1:
                            hop(j, level, None).start()

        def issue(k):
            for j, (_, to) in enumerate(JOBS):
                if to == ORDER[k]:
                    for w in waves(j, 0):
                        hop(j, 0, w).start()

        issue(0)
        for k in range(1, few_first):
            weigh(k)
            issue(k)
        for cp in inputs:
            cp.wait()
        w_ref[...] = 1.0 + jnp.concatenate([gain_ref[i:i + 1] for i in range(dim // LANES)], axis=1)
        hid = hid_ref[...].astype(F32)
        inv = lax.rsqrt(jnp.mean(hid * hid, axis=1, keepdims=True) + NORM_EPS)
        n_buf[...] = hid * inv
        x_buf[...] = (n_buf[...] * w_ref[...]).astype(BF16)
        inv_buf[...] = jnp.broadcast_to(inv, (tokens, LANES))
        pay[...] = n_buf[my_few]
        square[...] = jnp.zeros((LANES, LANES), F32)
        square[0:1, 0:tokens] = mask_in[...]
        mask_own[...] = square[0:few]
        mask_col = jnp.transpose(square[...])[0:tokens, 0:1]
        my_z, my_y = lax.div(me, SIDE), lax.rem(me, SIDE)
        for d in range(1, SIDE):
            remote(pay, pay_got.at[my_z, my_y], dp_sem.at[0, 0], dp_sem.at[0, 1], at[d, 0], col).start()
        pay_got[my_z, my_y] = pay[...]
        mask_sent, mask_came = to_dp(mask_own, mask_got, 1, pl.ds(0, 1))
        mask_got[me] = mask_own[...]
        for k in range(few_first, N_DP):
            weigh(k)
            if k < before_lines:
                issue(k)

        def keep(r, _):
            here, there = aligned(me * tokens + r * pack, pack, pack), aligned(r * pack, pack, pack)
            got_soon[0, there] = sends[here, :late]
            got_late[0, there] = sends[here, late:]
            return 0

        lax.fori_loop(0, tokens // pack, keep, 0)

        def student(slot):
            z = lax.dot_general(x_buf[...], tabs[slot], ROWS_BY_ROWS, preferred_element_type=F32)
            ratio = jnp.tanh(z * INV_CAP)
            return ratio, jnp.exp(SOFT_CAP * ratio - SOFT_CAP)

        def next_tiles(i):
            for c in range(per):
                tab_copy(i * per + c).wait()

            @pl.when(i + 1 < 2 * N_DP)
            def _():
                for c in range(per):
                    tab_copy((i + 1) * per + c).start()

            return [lax.rem(i, 2) * per + c for c in range(per)]

        def forward(i, sums):
            s_sum, k_sum = sums
            slots = next_tiles(i)
            for c in range(per):
                ratio, stu = student(slots[c])
                tea = sends[aligned(i * tokens, tokens, tokens), pl.ds(c * sub, sub)]
                s_sum, k_sum = s_sum + fold(stu), k_sum + fold(tea * ratio)
            return s_sum, k_sum

        zero = jnp.zeros((tokens, LANES), F32)
        s_sum, k_sum = lax.fori_loop(0, SIDE, forward, (zero, zero))
        whole(pay_got.at[0, pl.ds(0, SIDE - 1)], dp_sem.at[0, 1])
        mine = pay_got.at[:, my_y]
        for d in range(1, SIDE):
            remote(mine, mine, dp_sem.at[SIDE, 0], dp_sem.at[SIDE, 1], at[0, d], col).start()
        for k in range(before_lines, N_DP):
            issue(k)
        s_sum, k_sum = lax.fori_loop(SIDE, N_DP, forward, (s_sum, k_sum))
        lane = lax.broadcasted_iota(jnp.int32, (tokens, LANES), 1)
        sums = jnp.where(lane == 0, jnp.sum(s_sum, axis=1, keepdims=True), 0.0)
        sums = jnp.where(lane == 1, jnp.sum(t_acc[...], axis=1, keepdims=True), sums)
        sums = jnp.where(lane == AWAY, SOFT_CAP * jnp.sum(c_acc[...] - k_sum, axis=1, keepdims=True), sums)
        own_col[...] = sums
        tp_got[col] = sums
        tp_sent, tp_came = to_tp(lambda c: own_col, tp_got, 0)
        tp_came()
        total = added(tp_got)
        square[0:tokens] = jnp.where(lane == DOWN, mask_col, total)
        line = jnp.transpose(square[...])[0:few]
        own_row[...] = line
        all_ref[me] = line
        dp_sent, dp_came = to_dp(own_row, all_ref, 2, pl.ds(0, SIDE))
        twin = col + 1 - 2 * lax.rem(col, 2)
        lines = pay_got.at[pl.ds(0, SIDE - 1)]
        whole(lines, dp_sem.at[SIDE, 1])
        mask_came()
        x_got[col] = pay_got[...]

        evens = range(0, N_TP, 2)
        for j in evens[1:]:
            remote(pay_got, x_got.at[col], tp_sem.at[1, 0], tp_sem.at[1, 1], me, mates[j]).start()
        came(0)
        onward(1, True, None)
        onward(1, False, 0)

        count = jnp.sum(added(mask_got, slice(1)), axis=1, keepdims=True)
        inv_s, inv_t, weight = 1.0 / total[:, 0:1], 1.0 / total[:, 1:2], mask_col / count
        dx[...] = jnp.zeros((tokens, dim), F32)

        def backward(i, _):
            slots = next_tiles(i)
            total = dx[...]
            for c in range(per):
                ratio, stu = student(slots[c])
                tea = sends[aligned((i - N_DP) * tokens, tokens, tokens), pl.ds(c * sub, sub)]
                diff = (stu * inv_s - tea * inv_t) * weight
                g = (diff * (1.0 - ratio * ratio)).astype(BF16)
                total = total + jnp.dot(g, tabs[slots[c]], preferred_element_type=F32)
            dx[...] = total
            return 0

        lax.fori_loop(N_DP, 2 * N_DP, backward, 0)
        came(1)
        onward(2, True, 0)
        onward(1, False, 1)
        whole(x_got.at[pl.ds(0, SIDE - 1)], tp_sem.at[1, 1])
        for j in evens:
            remote(x_got.at[mates[j]], x_got.at[mates[j]], tp_sem.at[SIDE, 0], tp_sem.at[SIDE, 1], me, twin).start()

        rs_got[col] = dx[my_few]
        rs_sent, rs_came = to_tp(lambda c: dx.at[aligned(c * few, few, few)], rs_got, 2)
        rs_came()
        my_x = added(rs_got)
        my_n = n_buf[my_few]
        grad_n = my_x * w_ref[...]
        my_h = inv_buf[my_few, 0:1] * (grad_n - my_n * jnp.mean(grad_n * my_n, axis=1, keepdims=True))
        ag_own[...] = jnp.zeros((2 * few, dim), F32)
        ag_own[0:few] = my_h
        ag_own[few:few + 1] = jnp.sum(my_x * my_n, axis=0, keepdims=True)
        ag_got[col] = ag_own[...]
        ag_sent, ag_came = to_tp(lambda c: ag_own, ag_got, DOWN)
        ag_came()
        gh_ref[...] = jnp.concatenate([ag_got[j, 0:few] for j in range(N_TP)], axis=0)
        line = added(ag_got, slice(few, few + 1))
        gn_own[0:1] = line
        gn_got[me, 0:1] = line
        gn_sent, gn_came = to_dp(gn_own, gn_got, DOWN, pl.ds(0, 1))

        came(2)
        onward(DOWN, True, 0, 1)
        onward(2, True, 1)
        whole(x_got.at[pl.ds(0, SIDE)], tp_sem.at[SIDE, 1])

        def widen(d, _):
            rows = jnp.concatenate([x_got[j, lax.div(d, SIDE), lax.rem(d, SIDE)] for j in range(N_TP)], axis=0)
            x_out[aligned(d * tokens, tokens, tokens)] = (rows * w_ref[...]).astype(BF16)
            return 0

        lax.fori_loop(0, N_DP, widen, 0)
        dp_came()
        row = lax.broadcasted_iota(jnp.int32, (few, LANES), 0)
        lanes = lax.broadcasted_iota(jnp.int32, (few, LANES), 1)
        for d in range(N_DP):
            block = all_ref[d]
            safe = jnp.where((row < AWAY) & (lanes < tokens), block, 1.0)
            rel[d * few:(d + 1) * few] = jnp.where(row < AWAY, 1.0 / safe, block / count)
        for k, (dz, dy) in enumerate(OFFSETS):
            square[k * few:(k + 1) * few] = rel[aligned(at[-dz, -dy] * few, few, few)]
        coef_ref[...] = jnp.transpose(square[...])

        own_tab.wait()
        whole(got_soon.at[pl.ds(0, N_DP - 1)], hop_in.at[SIDE])
        whole(sends.at[pl.ds(0, len(JOBS) * half)], hop_out.at[0])

        def block(b, _):
            grad_block(at, got_soon, x_out, tab_out[aligned(b * sub, sub)], coef_ref, sends, g_buf, blocks_ref, b)
            return 0

        lax.fori_loop(0, 2, block, 0)
        gn_came()
        gg_ref[...] = added(gn_got, slice(1))
        whole(got_late.at[pl.ds(0, N_DP - 1)], hop_in.at[SIDE + 1])
        whole(stage, hop_out.at[1])
        for ref, sem in (*mask_sent, *tp_sent, *dp_sent, *rs_sent, *ag_sent, *gn_sent):
            whole(ref, sem)
        whole(pay_got.at[0, pl.ds(0, SIDE - 1)], dp_sem.at[0, 0])
        whole(lines, dp_sem.at[SIDE, 0])
        whole(x_got.at[pl.ds(0, SIDE - 1)], tp_sem.at[1, 0])
        whole(x_got.at[pl.ds(0, SIDE)], tp_sem.at[SIDE, 0])

    dma = pltpu.SemaphoreType.DMA
    wide, flat = (tokens, dim), (few, LANES)
    return pl.pallas_call(
        kern,
        out_shape=tuple(jax.ShapeDtypeStruct(shape, kind) for shape, kind in (
            ((N_DP, tokens, part // 2), F32), ((2, sub, dim), F32), ((N_DP * tokens, dim), BF16), ((part, dim), BF16), ((LANES, LANES), F32), ((N_DP, *flat), F32), (wide, F32),
            ((1, dim), F32))),
        in_specs=[HB] * 5, out_specs=(VM,) * 8,
        scratch_shapes=[pltpu.VMEM(shape, kind) for shape, kind in (
            (wide, BF16), ((dim // LANES, LANES), F32), ((1, tokens), F32), ((1, dim), F32), ((ring * tokens, part), BF16), ((N_DP * tokens, part), F32),
            ((len(MIDDLE), half, part), F32), ((N_DP, tokens, part // 2), F32), ((N_DP * tokens, sub), BF16), ((tokens, LANES), F32), ((tokens, LANES), F32),
            ((depth, sub, dim), BF16), (wide, F32), (wide, BF16), ((tokens, LANES), F32), ((LANES, LANES), F32), ((few, dim), F32),
            ((SIDE, SIDE, few, dim), F32), (flat, F32), ((N_DP, *flat), F32), ((N_TP, SIDE, SIDE, few, dim), F32), ((N_TP, tokens, LANES), F32),
            ((tokens, LANES), F32), (flat, F32), ((LANES, LANES), F32), (wide, F32), ((N_TP, few, dim), F32), ((2 * few, dim), F32),
            ((N_TP, 2 * few, dim), F32), ((few, dim), F32), ((N_DP, few, dim), F32))] + [
            dma((ring,)), dma((depth,)), dma((5,)), dma((2,)), dma((SIDE + 2,)), dma((SIDE + 1, 2)), dma((SIDE + 1, 2))],
        compiler_params=pltpu.CompilerParams(collective_id=0, has_side_effects=True, vmem_limit_bytes=L_FRONT * MIB),
        cost_estimate=pl.CostEstimate(flops=3 * 10 ** 9, bytes_accessed=100 * MIB, transcendentals=0), name='front')(
            *(pltpu.with_memory_space_constraint(a, pltpu.HBM) for a in (hidden, gain_row, mask_row, teacher, table)))


def finish(teas, x_all, tab_part, coef):
    n, tokens, late = teas.shape
    dim = x_all.shape[1]
    span = late // 2

    def kern(tea_ref, x_ref, tab_ref, coef_ref, out_ref, z_buf, g_buf):
        at = peers()[1]

        def block(b, _):
            grad_block(at, tea_ref, x_ref, tab_ref[aligned(late + b * span, span)], coef_ref, z_buf, g_buf, out_ref, b)
            return 0

        lax.fori_loop(0, 2, block, 0)

    return pl.pallas_call(kern, out_shape=jax.ShapeDtypeStruct((2, span, dim), F32), in_specs=[VM] * 4, out_specs=VM,
        scratch_shapes=[pltpu.VMEM((n * tokens, span), F32), pltpu.VMEM((n * tokens, span), BF16)], name='finish',
        compiler_params=pltpu.CompilerParams(vmem_limit_bytes=22 * MIB),
        cost_estimate=pl.CostEstimate(flops=10 ** 9, bytes_accessed=8 * MIB, transcendentals=0))(teas, x_all, tab_part, coef)


def place(table, pieces, vocab):
    arrays = [p[0] for p in pieces]
    n = len(arrays)
    dim = arrays[0].shape[1]
    rows = vocab // N_DP
    quarter = rows // SIDE
    cut = 256
    chunks = []
    for i, (array, dz, dy, kind, start) in enumerate(pieces):
        r = 0
        while r < array.shape[0]:
            row = start + r
            size = min(cut, array.shape[0] - r, quarter - row % quarter)
            chunks.append((i, r, size, dz, dy, row + (row // quarter + kind) * quarter))
            r += size

    def kern(*refs):
        dst, buf, sem = refs[-DOWN:]
        at = peers()[1]
        reads, writes = [], []
        for k, (i, r, size, dz, dy, first) in enumerate(chunks):
            held = buf.at[k, pl.ds(0, size)]
            there = aligned(at[dz, dy] * rows + first, size, 8)
            reads.append(pltpu.make_async_copy(refs[i].at[pl.ds(r, size)], held, sem.at[0, k]))
            writes.append(pltpu.make_async_copy(held, dst.at[there], sem.at[1, k]))
        for cp in reads:
            cp.start()
        for read, write in zip(reads, writes):
            read.wait()
            write.start()
        for cp in writes:
            cp.wait()

    args = arrays if table is None else [*arrays, table]
    size = len(chunks) * cut * dim
    return pl.pallas_call(kern, out_shape=jax.ShapeDtypeStruct((vocab, dim), F32), in_specs=[pl.BlockSpec(memory_space=pl.ANY)] * n + [HB] * (len(args) - n),
        out_specs=HB, scratch_shapes=[pltpu.VMEM((len(chunks), cut, dim), F32), pltpu.SemaphoreType.DMA((2, len(chunks)))],
        input_output_aliases={} if table is None else {n: 0}, name='place', compiler_params=pltpu.CompilerParams(vmem_limit_bytes=4 * size + MIB),
        cost_estimate=pl.CostEstimate(flops=10 * MIB, bytes_accessed=8 * size, transcendentals=0))(*args)


def gather(first, rest, vocab):
    quarter = first[0].shape[0]
    sets, ways = range(2), (UP, DOWN)
    table, event = None, 0

    def send(pair, axis, step):
        out = []
        for k in sets:
            dz, dy = (step, 0) if axis == k else (0, step)
            out.append(lax.ppermute(pair[k], 'dp', [(d, shift(d, dz, dy)) for d in range(N_DP)]))
        return out

    def put(pair, a, b, start=0):
        return [(pair[k], *((b, a) if k else (a, b)), k, start) for k in sets]

    def settle(*pieces):
        nonlocal table
        table = place(table, [p for ps in pieces for p in ps], vocab)

    def wait(*pairs):
        nonlocal table, event
        event += 1
        table, *flat = lax.optimization_barrier((table, *(x for pair in pairs for x in pair)))
        return [flat[2 * i:2 * i + 2] for i in range(len(pairs))]

    def join(one, other):
        return [jnp.concatenate(pair) for pair in zip(one, other)]

    own = [first]
    low, high = ([send(own[0], 0, way)] for way in ways)
    later = rest()
    event = 1
    own.append([later[:quarter], later[quarter:]])
    low.append(send(own[1], 0, UP))
    high.append(send(own[1], 0, DOWN))
    whole = join(*own)
    side = {way: send(whole, 1, way) for way in ways}
    settle(put(own[0], 0, 0, 0), put(own[1], 0, 0, quarter))

    low[0], high[0] = wait(low[0], high[0])
    far_low = send(low[0], 0, UP)
    settle(put(low[0], DOWN, 0, 0), put(high[0], UP, 0, 0))

    low[1], high[1] = wait(low[1], high[1])
    far_high = send(high[1], 0, DOWN)
    low_whole, high_whole = join(*low), join(*high)
    low_side = {way: send(low_whole, 1, way) for way in ways}
    settle(put(low[1], DOWN, 0, quarter), put(high[1], UP, 0, quarter))

    side[UP], side[DOWN], high_whole = wait(side[UP], side[DOWN], high_whole)
    high_side = {way: send(high_whole, 1, way) for way in ways}
    side_far = send(side[UP], 1, UP)
    settle(put(side[UP], 0, DOWN))
    settle(put(side[DOWN], 0, UP))

    far_low, far_high = wait(far_low, far_high)
    far_side = {(c, way): send(pair, 1, way) for way in ways for c, pair in enumerate((far_low, far_high))}
    settle(put(far_low, AWAY, 0, 0), put(far_high, AWAY, 0, quarter))

    low_side[UP], low_side[DOWN] = wait(low_side[UP], low_side[DOWN])
    low_far = send(low_side[DOWN], 1, DOWN)
    settle(put(low_side[UP], DOWN, DOWN))
    settle(put(low_side[DOWN], DOWN, UP))

    high_side[UP], high_side[DOWN] = wait(high_side[UP], high_side[DOWN])
    high_far = [send([x[:quarter] for x in high_side[UP]], 1, UP), send([x[quarter:] for x in high_side[DOWN]], 1, DOWN)]
    settle(put(high_side[UP], UP, DOWN))
    settle(put(high_side[DOWN], UP, UP))

    far_side[0, DOWN], far_side[1, DOWN], side_far = wait(far_side[0, DOWN], far_side[1, DOWN], side_far)
    ends = slice(0, quarter - LAST), slice(quarter - LAST, quarter)
    last_down = [send([x[end] for x in far_side[1, DOWN]], 1, DOWN) for end in ends]
    settle(put(far_side[0, DOWN], AWAY, UP, 0), put(far_side[1, DOWN], AWAY, UP, quarter))
    settle(put(side_far, 0, AWAY))

    far_side[0, UP], = wait(far_side[0, UP])
    last_up = [send([x[end] for x in far_side[0, UP]], 1, UP) for end in ends]
    settle(put(far_side[0, UP], AWAY, DOWN, 0))

    far_side[1, UP], low_far = wait(far_side[1, UP], low_far)
    settle(put(far_side[1, UP], AWAY, DOWN, quarter))
    settle(put(low_far, DOWN, AWAY))

    high_far = wait(*high_far)
    settle(put(high_far[0], UP, AWAY, 0), put(high_far[1], UP, AWAY, quarter))
    for up, down, end in zip(last_up, last_down, ends):
        up, down = wait(up, down)
        settle(put(up, AWAY, AWAY, end.start), put(down, AWAY, AWAY, quarter + end.start))
    return table


def solution(mesh):
    def local_step(hid_rows, w_final, tab_rows, tea_rows, mask_rows):
        tokens = hid_rows.shape[0]
        late, soon, x_all, tab_part, coef, stats, grad_h, gain_line = front(hid_rows, w_final.reshape(-1, LANES), mask_rows[None], tea_rows, tab_rows)
        coef, *first = lax.optimization_barrier((coef, soon[0], soon[1]))
        table = gather(first, lambda: finish(late, x_all, tab_part, coef).reshape(-1, x_all.shape[1]), tab_rows.shape[0])
        s_sum, t_sum, k_sum, masks = (stats[:, i, :tokens] for i in range(SIDE))
        all_kl = k_sum / t_sum + jnp.log(s_sum) - jnp.log(t_sum)
        loss_val = jnp.sum(masks * all_kl) / jnp.sum(masks)
        return loss_val, grad_h.astype(BF16), gain_line[0], table

    return jax.shard_map(local_step, mesh=mesh, in_specs=(P('dp', None), P(None), P('tp', None), P('dp', 'tp'), P('dp')), out_specs=(P(), P('dp', None), P(None), P('tp', None)), check_vma=False)
```
